32 devices in a mesh: rep: 4 (over x, y), dp: 8 (over z, core).
Axes of the slice: x: 2, y: 2, z: 4, core: 2. Of those that a mesh axis runs over, the one named last changes fastest.
Arguments:
- x: bfloat16 [32, 2048, 1024], P(('rep', 'dp')), parts along dimension 0
- dy: bfloat16 [32, 2048, 1024], P(('rep', 'dp')), parts along dimension 0
- w_gate: bfloat16 [2, 1024, 3200], replicated
- w_up: bfloat16 [2, 1024, 3200], replicated
- w_down: bfloat16 [2, 3200, 1024], replicated
- m_w_gate: float32 [2, 1024, 3200], replicated
- m_w_up: float32 [2, 1024, 3200], replicated
- m_w_down: float32 [2, 3200, 1024], replicated
- v_w_gate: float32 [2, 1024, 3200], replicated
- v_w_up: float32 [2, 1024, 3200], replicated
- v_w_down: float32 [2, 3200, 1024], replicated
Outputs:
- output 1: bfloat16 [8, 1024, 3200], P('rep'), parts along dimension 0
- output 2: bfloat16 [8, 1024, 3200], P('rep'), parts along dimension 0
- output 3: bfloat16 [8, 3200, 1024], P('rep'), parts along dimension 0
- output 4: float32 [8, 1024, 3200], P('rep'), parts along dimension 0
- output 5: float32 [8, 1024, 3200], P('rep'), parts along dimension 0
- output 6: float32 [8, 3200, 1024], P('rep'), parts along dimension 0
- output 7: float32 [8, 1024, 3200], P('rep'), parts along dimension 0
- output 8: float32 [8, 1024, 3200], P('rep'), parts along dimension 0
- output 9: float32 [8, 3200, 1024], P('rep'), parts along dimension 0
There are 4 independent parts. The reference program is written for one: setup_inputs(seed, part) draws one part's arguments, and reference() takes and returns one part's arrays. A program takes and returns all parts, laid end to end along the dimension named above; an argument that names none is the same for every part.
All inputs are finite; a program needn't handle non-finite values.
Results may differ from the reference program's by a relative error of at most 0.022.
Values are sent between devices in bfloat16 or wider.
A program may use at most 2.75 GiB of HBM per device.

```python
import jax
import jax.numpy as jnp
from jax import lax

SEQUENCES = 8
TOKENS = 2048
D = 1024
FF = 3200
LAYERS = 2
NAMES = ("w_gate", "w_up", "w_down")
SHAPES = {"w_gate": (LAYERS, D, FF), "w_up": (LAYERS, D, FF), "w_down": (LAYERS, FF, D)}


def bump(key, n, height):
    away = (jnp.arange(n, dtype=jnp.int32) - jax.random.randint(key, (), 0, n, jnp.int32)) % n
    return jnp.where(away < n // 8, height, 1.0)


def together(key, own, strength):
    shared = jax.random.normal(key, own.shape[1:], jnp.float32)
    return (own + strength * shared) * lax.rsqrt(1 + strength * strength)


def setup_inputs(seed: int = 0, part: int = 0) -> dict:
    kx, kdy, ka, kb, kz, kf, kh, kl, *keys = jax.random.split(jax.random.key(seed), 8 + 3 * len(NAMES))
    kx, kdy, ka, kb = (jax.random.fold_in(k, part) for k in (kx, kdy, ka, kb))
    kw, km, kv = (keys[i::3] for i in range(3))
    shape = (SEQUENCES, TOKENS, D)
    much_x, much_dy = jax.random.uniform(kz, (2,), jnp.float32, 0.0, 1.0)
    loud = 2.0 ** jax.random.uniform(jax.random.fold_in(kz, 1), (), jnp.float32, -1.0, 2.0)
    layers = 2.0 ** jax.random.uniform(kl, (LAYERS, 1, 1), jnp.float32, -1.0, 1.0)
    x = together(ka, jax.random.normal(kx, shape, jnp.float32), much_x) * bump(kf, D, 4.0)
    dy = together(kb, jax.random.normal(kdy, shape, jnp.float32), much_dy)
    drawn = {"x": x.astype(jnp.bfloat16), "dy": (loud * dy * (SEQUENCES * TOKENS) ** -0.5).astype(jnp.bfloat16)}
    for key, name in zip(kw, NAMES, strict=True):
        w = jax.random.normal(key, SHAPES[name], jnp.float32) * SHAPES[name][1] ** -0.5
        drawn[name] = (w * {"w_gate": 1.0, "w_up": bump(kh, FF, 4.0), "w_down": layers}[name]).astype(jnp.bfloat16)
    for key, name in zip(km, NAMES, strict=True):
        drawn[f"m_{name}"] = 0.1 * jax.random.normal(key, SHAPES[name], jnp.float32)
    for key, name in zip(kv, NAMES, strict=True):
        drawn[f"v_{name}"] = jax.random.uniform(key, SHAPES[name], jnp.float32, 0.005, 0.015)
    return drawn


def matmul(a, w):
    return jnp.dot(a, w, preferred_element_type=jnp.float32).astype(jnp.bfloat16)


def normed(h):
    wide = h.astype(jnp.float32)
    scale = lax.rsqrt(jnp.mean(wide**2, -1, keepdims=True) + 1e-6)
    return (wide * scale).astype(jnp.bfloat16)


def layer(h, w):
    a = normed(h)
    gate = jnp.dot(a, w["w_gate"], preferred_element_type=jnp.float32)
    up = jnp.dot(a, w["w_up"], preferred_element_type=jnp.float32)
    return h + matmul((jax.nn.silu(gate) * up).astype(jnp.bfloat16), w["w_down"])


def adamw(w, m, v, g):
    m = 0.9 * m + 0.1 * g
    v = 0.95 * v + 0.05 * g * g
    step = m * lax.rsqrt(v + 1e-8) + 0.1 * w
    return (w - 0.02 * step).astype(jnp.bfloat16), m, v


def stack(weights, h):
    return lax.scan(lambda h, w: (layer(h, w), None), h, weights)[0]


def reference(x, dy, w_gate, w_up, w_down, m_w_gate, m_w_up, m_w_down, v_w_gate, v_w_up, v_w_down):
    weights = dict(zip(NAMES, (w_gate, w_up, w_down), strict=True))

    def take(so_far, sequence):
        h, by_y = sequence
        _, back = jax.vjp(lambda w: stack(w, h), weights)
        return jax.tree.map(lambda total, term: total + term.astype(jnp.float32), so_far, back(by_y)[0]), None

    none_yet = {name: jnp.zeros(w.shape, jnp.float32) for name, w in weights.items()}
    by_weights, _ = lax.scan(take, none_yet, (x, dy))
    gradients = [by_weights[name].astype(jnp.bfloat16).astype(jnp.float32) for name in NAMES]
    new = [
        adamw(w.astype(jnp.float32), m, v, g)
        for w, m, v, g in zip((w_gate, w_up, w_down), (m_w_gate, m_w_up, m_w_down), (v_w_gate, v_w_up, v_w_down), gradients, strict=True)
    ]
    return tuple(one[which] for which in range(3) for one in new)
```

```python
import functools

import jax
import jax.numpy as jnp
from jax import lax
from jax.experimental import pallas as pl
from jax.experimental.pallas import tpu as pltpu
from jax.sharding import PartitionSpec as P

BF16, F32 = jnp.bfloat16, jnp.float32
MESH = pl.DeviceIdType.MESH
VMEM_LIMIT = 66_000_000
BLOCKS = 5
ALL = 6 * BLOCKS
SUMMED = 26
UNITS = 5
FIRST = 8
SLOTS, SEND_SLOTS, LOAD_SLOTS = 16, 8, 4
NN = (((1,), (0,)), ((), ()))
NT = (((1,), (1,)), ((), ()))


def dot(a, b, dims=NN):
    return lax.dot_general(a, b, dims, preferred_element_type=F32)


def scale_of(wide):
    return lax.rsqrt(jnp.mean(wide * wide, -1, keepdims=True) + 1e-6)


def cuts(n, width):
    starts = list(range(0, n - width + 1, width))
    return [(s, (starts[i + 1] if i + 1 < len(starts) else n) - s) for i, s in enumerate(starts)]


def forward_kernel(width, x_ref, wg_hbm, wu_hbm, wd_hbm, a0_ref, h1_ref, a1_ref, wg, wu, wd, p, sems):
    first = pl.program_id(0) == 0
    pieces = cuts(wg.shape[1], width)

    def loads(i):
        s, n = pieces[i]
        return (
            pltpu.make_async_copy(wg_hbm.at[0, :, pl.ds(s, n)], wg.at[:, pl.ds(s, n)], sems.at[0, i]),
            pltpu.make_async_copy(wu_hbm.at[0, :, pl.ds(s, n)], wu.at[:, pl.ds(s, n)], sems.at[1, i]),
            pltpu.make_async_copy(wd_hbm.at[0, pl.ds(s, n), :], wd.at[pl.ds(s, n), :], sems.at[2, i]),
        )

    @pl.when(first)
    def _():
        for i in range(len(pieces)):
            for c in loads(i)[:2]:
                c.start()
        for i in range(len(pieces)):
            loads(i)[2].start()

    wide = x_ref[...].astype(F32)
    a = (wide * scale_of(wide)).astype(BF16)
    a0_ref[...] = a
    for i, (s, n) in enumerate(pieces):

        @pl.when(first)
        def _(i=i):
            for c in loads(i)[:2]:
                c.wait()

        gate = dot(a, wg[:, s : s + n])
        up = dot(a, wu[:, s : s + n])
        p[:, s : s + n] = (gate * (0.5 * jnp.tanh(0.5 * gate) + 0.5) * up).astype(BF16)

    @pl.when(first)
    def _():
        for i in range(len(pieces)):
            loads(i)[2].wait()

    h1 = (wide + dot(p[...], wd[...]).astype(BF16).astype(F32)).astype(BF16)
    h1_ref[...] = h1
    wide1 = h1.astype(F32)
    a1_ref[...] = (wide1 * scale_of(wide1)).astype(BF16)


def forward(x, wg, wu, wd):
    t, d = x.shape
    ff = wg.shape[2]
    tile = min(t, 512)
    width = min(ff, 768)
    rows = pl.BlockSpec((tile, d), lambda i: (i, 0))
    anywhere = pl.BlockSpec(memory_space=pl.ANY)
    return pl.pallas_call(
        functools.partial(forward_kernel, width),
        grid=(t // tile,),
        out_shape=[jax.ShapeDtypeStruct((t, d), BF16)] * 3,
        in_specs=[rows, anywhere, anywhere, anywhere],
        out_specs=[rows] * 3,
        scratch_shapes=[
            pltpu.VMEM((d, ff), BF16),
            pltpu.VMEM((d, ff), BF16),
            pltpu.VMEM((ff, d), BF16),
            pltpu.VMEM((tile, ff), BF16),
            pltpu.SemaphoreType.DMA((3, len(cuts(ff, width)))),
        ],
        compiler_params=pltpu.CompilerParams(vmem_limit_bytes=VMEM_LIMIT, dimension_semantics=("arbitrary",)),
        cost_estimate=pl.CostEstimate(flops=6 * t * d * ff, bytes_accessed=6 * d * ff + 8 * t * d, transcendentals=t * ff),
        name="forward",
    )(x, wg, wu, wd)


BLOCK_STEPS, LOW_STEPS = 7, 5
TURN = BLOCKS * BLOCK_STEPS
STEPS = TURN + 1 + BLOCKS * LOW_STEPS


def step_of(s):
    low = s - (TURN + 1)
    block = jnp.where(s < TURN, s // BLOCK_STEPS, jnp.where(s == TURN, BLOCKS, BLOCKS + low // LOW_STEPS))
    kind = jnp.where(s < TURN, s % BLOCK_STEPS, jnp.where(s == TURN, 7, low % LOW_STEPS))
    return block, kind


def backward_kernel(
    a1_hbm, a0_hbm, h1_hbm, dy_hbm, wg_hbm, wu_hbm, wd_hbm,
    g_hbm, left_hbm, mine_hbm, theirs_hbm,
    ad, pgu, wgb, wub, wdb, wgt, wut, dat, stage, mb, xb, sb, ra, rb, tot,
    in_sem, w_sem, own_sem, give_sem, get_sem, left_sem, load_sem, s_sem, ra_sem, rb_sem, tot_sem, down_sem, up_sem, keep_sem, pass_sem, partner_sem,
):
    me = lax.axis_index("dp")
    z, core = me // 2, me % 2
    partner = me + 1 - 2 * core
    t, d = ad.shape[1:]
    f = stage.shape[1]
    half, r = f // 2, f // 2 // UNITS
    units = SUMMED * UNITS
    sub = dat.shape[2]

    def remote(src, dst, send, recv, device):
        return pltpu.make_async_remote_copy(src_ref=src, dst_ref=dst, send_sem=send, recv_sem=recv, device_id={"dp": device}, device_id_type=MESH)

    barrier = pltpu.get_barrier_semaphore()
    pl.semaphore_signal(barrier, inc=1, device_id={"dp": partner}, device_id_type=MESH)

    @pl.when(z > 0)
    def _():
        pl.semaphore_signal(barrier, inc=1, device_id={"dp": me - 2}, device_id_type=MESH)

    @pl.when(z < 3)
    def _():
        pl.semaphore_signal(barrier, inc=1, device_id={"dp": me + 2}, device_id_type=MESH)

    pl.semaphore_wait(barrier, 3 - z // 3 - (3 - z) // 3)

    def weights(block):
        layer, j, slot = 1 - block // BLOCKS, block % BLOCKS, block % 2
        at = pl.ds(pl.multiple_of(j * f, f), f)
        return (
            pltpu.make_async_copy(wg_hbm.at[layer, :, at], wgb.at[slot], w_sem.at[slot, 0]),
            pltpu.make_async_copy(wu_hbm.at[layer, :, at], wub.at[slot], w_sem.at[slot, 1]),
            pltpu.make_async_copy(wd_hbm.at[layer, at, :], wdb.at[slot], w_sem.at[slot, 2]),
        )

    load_dy = pltpu.make_async_copy(dy_hbm, ad.at[0], in_sem.at[0])
    load_a1 = pltpu.make_async_copy(a1_hbm, ad.at[1], in_sem.at[1])
    load_h1 = pltpu.make_async_copy(h1_hbm, ad.at[1], in_sem.at[2])
    load_a0 = pltpu.make_async_copy(a0_hbm, ad.at[1], in_sem.at[3])

    def hidden(block, kind):
        slot = block % 2

        @pl.when(kind == 0)
        def _():
            @pl.when(block == 0)
            def _():
                load_dy.wait()
                load_a1.wait()

            @pl.when(block == BLOCKS)
            def _():
                load_a0.wait()

            for c in weights(block):
                c.wait()

            @pl.when(block + 1 < 2 * BLOCKS)
            def _():
                for c in weights(block + 1):
                    c.start()

            wgt[...] = wgb[slot].T
            wut[...] = wub[slot].T

        for i in range(t // 2 // sub):
            at = pl.ds(pl.multiple_of(kind * (t // 2) + i * sub, sub), sub)
            gate = dot(wgt[...], ad[1, at, :], NT)
            up = dot(wut[...], ad[1, at, :], NT)
            dp = dot(wdb[slot], ad[0, at, :], NT).astype(BF16).astype(F32)
            sig = 0.5 * jnp.tanh(0.5 * gate) + 0.5
            silu = gate * sig
            pgu[0, :, at] = (silu * up).astype(BF16)
            pgu[1, :, at] = (dp * up * (sig + silu * (1.0 - sig))).astype(BF16)
            pgu[2, :, at] = (dp * silu).astype(BF16)

    def gradient(block, kind):
        which = kind - 2
        slot = (3 * block + which) % 2
        rhs = jnp.minimum(which, 1)
        lhs = pgu[which]
        for i in range(2):
            cols = slice(i * (d // 2), (i + 1) * (d // 2))
            stage[slot, :, cols] = dot(lhs, ad[rhs, :, cols]).astype(BF16)

    def to_input(block, kind):
        slot = block % 2

        @pl.when((block == BLOCKS - 1) & (kind == 5))
        def _():
            load_h1.start()

        for i in range(t // 2 // sub):
            tile = (kind - 5) * (t // 2 // sub) + i
            at = pl.ds(pl.multiple_of(tile * sub, sub), sub)
            dat[tile] += dot(wgb[slot], pgu[1, :, at]) + dot(wub[slot], pgu[2, :, at])

    def turn():
        load_h1.wait()

        def body(i, _):
            at = pl.ds(pl.multiple_of(i * sub, sub), sub)
            da = dat[i].T.astype(BF16).astype(F32)
            wide = ad[1, at, :].astype(F32)
            scale = scale_of(wide)
            inner = jnp.sum(da * wide, -1, keepdims=True) * (scale * scale * scale) * (1.0 / d)
            through = (da * scale - wide * inner).astype(BF16).astype(F32)
            ad[0, at, :] = (ad[0, at, :].astype(F32) + through).astype(BF16)
            return 0

        lax.fori_loop(0, t // sub, body, 0)
        load_a0.start()

    def rows(slot, c):
        return stage.at[slot, pl.ds(pl.multiple_of(c * half, half), half), :]

    def piece_copies(q):
        slot = q % 2
        own = pltpu.make_async_copy(rows(slot, core), mine_hbm.at[q], own_sem.at[q])
        give = remote(rows(slot, 1 - core), theirs_hbm.at[q], give_sem.at[slot], get_sem.at[q], partner)
        return own, give

    def left_copy(q):
        return pltpu.make_async_copy(stage.at[q % 2], left_hbm.at[q - SUMMED], left_sem.at[q % 2])

    def send_stage(q):
        @pl.when(q < SUMMED)
        def _():
            own, give = piece_copies(q)
            own.start()
            give.start()

        @pl.when(q >= SUMMED)
        def _():
            left_copy(q).start()

    def wait_stage(q):
        @pl.when(q < SUMMED)
        def _():
            own, give = piece_copies(q)
            own.wait()
            give.wait_send()

        @pl.when(q >= SUMMED)
        def _():
            left_copy(q).wait()

    is0, is1, is2, is3 = z == 0, z == 1, z == 2, z == 3
    sum_lag = jnp.where(is1, 4, jnp.where(is2, 2, 0))
    tot_lag = jnp.where(is1, 4, jnp.where(is3, 10, 7))
    free_lag = tot_lag + jnp.where(is3, 3, 4)

    def load_copies(k):
        q, at, slot = k // UNITS, pl.ds(pl.multiple_of((k % UNITS) * r, r), r), k % LOAD_SLOTS
        return (
            pltpu.make_async_copy(mine_hbm.at[q, at, :], mb.at[slot], load_sem.at[slot, 0]),
            pltpu.make_async_copy(theirs_hbm.at[q, at, :], xb.at[slot], load_sem.at[slot, 1]),
        )

    def s_copy_edge(k):
        return remote(sb.at[k % SEND_SLOTS], ra.at[k % SLOTS], s_sem.at[k % SEND_SLOTS], ra_sem.at[k % SLOTS], me + 2 - 4 * (z // 3))

    def s_copy_inner(k):
        return remote(sb.at[k % SEND_SLOTS], rb.at[k % SLOTS], s_sem.at[k % SEND_SLOTS], rb_sem.at[k % SLOTS], me - 2)

    def tot_down(k):
        return remote(tot.at[k % SLOTS], tot.at[k % SLOTS], down_sem.at[k % SLOTS], tot_sem.at[k % SLOTS], me - 2)

    def tot_up(k):
        return remote(tot.at[k % SLOTS], tot.at[k % SLOTS], up_sem.at[k % SLOTS], tot_sem.at[k % SLOTS], me + 2)

    def out_copies(k):
        q, at, slot = k // UNITS, pl.ds(pl.multiple_of(core * half + (k % UNITS) * r, r), r), k % SLOTS
        return (
            pltpu.make_async_copy(tot.at[slot], g_hbm.at[q, at, :], keep_sem.at[slot]),
            remote(tot.at[slot], g_hbm.at[q, at, :], pass_sem.at[slot], partner_sem, partner),
        )

    def inside(k):
        return (k >= 0) & (k < units)

    def free(k):
        @pl.when(inside(k))
        def _():
            keep, give = out_copies(k)
            keep.wait()
            give.wait_send()

            @pl.when(is1)
            def _():
                tot_down(k).wait_send()

            @pl.when(is1 | is2)
            def _():
                tot_up(k).wait_send()

    def add(k):
        @pl.when(inside(k))
        def _():
            for c in load_copies(k):
                c.wait()
            slot = k % LOAD_SLOTS
            both = mb[slot].astype(F32) + xb[slot].astype(F32)

            @pl.when((is0 | is3) & (k >= SEND_SLOTS))
            def _():
                s_copy_edge(k - SEND_SLOTS).wait_send()

            @pl.when(is2 & (k >= SEND_SLOTS))
            def _():
                s_copy_inner(k - SEND_SLOTS).wait_send()

            @pl.when(is0 | is3)
            def _():
                sb[k % SEND_SLOTS] = both.astype(BF16)

            @pl.when(is2)
            def _():
                s_copy_edge(k).wait_recv()
                sb[k % SEND_SLOTS] = (both + ra[k % SLOTS].astype(F32)).astype(BF16)

            @pl.when(is1)
            def _():
                s_copy_edge(k).wait_recv()
                s_copy_inner(k).wait_recv()
                tot[k % SLOTS] = (both + ra[k % SLOTS].astype(F32) + rb[k % SLOTS].astype(F32)).astype(BF16)

    def arrive(k):
        @pl.when(inside(k) & (z != 1))
        def _():
            tot_down(k).wait_recv()

    def send(k_sum, k_tot):
        @pl.when(inside(k_sum) & (is0 | is3))
        def _():
            s_copy_edge(k_sum).start()

        @pl.when(inside(k_sum) & is2)
        def _():
            s_copy_inner(k_sum).start()

        @pl.when(inside(k_tot))
        def _():
            @pl.when(is1)
            def _():
                tot_down(k_tot).start()

            @pl.when(is1 | is2)
            def _():
                tot_up(k_tot).start()

            for c in out_copies(k_tot):
                c.start()

    def load(k):
        @pl.when(inside(k))
        def _():
            @pl.when(k % UNITS == 0)
            def _():
                piece_copies(k // UNITS)[1].wait_recv()

            for c in load_copies(k):
                c.start()

    load_dy.start()
    load_a1.start()
    for c in weights(0):
        c.start()
    dat[...] = jnp.zeros_like(dat)

    def tick(i, _):
        step = i // 2
        works = i % 2 == 0

        @pl.when((step >= 1) & (step <= STEPS))
        def _():
            block, kind = step_of(step - 1)
            q = 3 * block + kind - 2

            @pl.when((kind >= 2) & (kind <= 4) & works)
            def _():
                send_stage(q)

            @pl.when((kind >= 2) & (kind <= 4) & (i % 2 == 1))
            def _():
                wait_stage(q)

        now = i - FIRST
        free(now - free_lag)
        add(now - sum_lag)
        arrive(now - tot_lag)
        send(now - sum_lag, now - tot_lag)
        load(now - sum_lag + 1)

        @pl.when(works & (step < STEPS))
        def _():
            block, kind = step_of(step)

            @pl.when(kind <= 1)
            def _():
                hidden(block, kind)

            @pl.when((kind >= 2) & (kind <= 4))
            def _():
                gradient(block, kind)

            @pl.when((kind == 5) | (kind == 6))
            def _():
                to_input(block, kind)

            @pl.when(kind == 7)
            def _():
                turn()

        return 0

    lax.fori_loop(0, max(FIRST + units + 14, 2 * STEPS + 2), tick, 0)

    for k in range(units - SEND_SLOTS, units):

        @pl.when(is0 | is3)
        def _(k=k):
            s_copy_edge(k).wait_send()

        @pl.when(is2)
        def _(k=k):
            s_copy_inner(k).wait_send()

    pltpu.make_async_copy(theirs_hbm, theirs_hbm, partner_sem).wait()


def backward(a1, a0, h1, dy, wg, wu, wd):
    t, d = a1.shape
    ff = wg.shape[2]
    f = ff // BLOCKS
    r = f // 2 // UNITS
    sub = t // 4
    anywhere = pl.BlockSpec(memory_space=pl.ANY)
    dma = pltpu.SemaphoreType.DMA
    return pl.pallas_call(
        backward_kernel,
        out_shape=[
            jax.ShapeDtypeStruct((SUMMED, f, d), BF16),
            jax.ShapeDtypeStruct((ALL - SUMMED, f, d), BF16),
            jax.ShapeDtypeStruct((SUMMED, f // 2, d), BF16),
            jax.ShapeDtypeStruct((SUMMED, f // 2, d), BF16),
        ],
        in_specs=[anywhere] * 7,
        out_specs=[anywhere] * 4,
        scratch_shapes=[
            pltpu.VMEM((2, t, d), BF16),
            pltpu.VMEM((3, f, t), BF16),
            pltpu.VMEM((2, d, f), BF16),
            pltpu.VMEM((2, d, f), BF16),
            pltpu.VMEM((2, f, d), BF16),
            pltpu.VMEM((f, d), BF16),
            pltpu.VMEM((f, d), BF16),
            pltpu.VMEM((4, d, sub), F32),
            pltpu.VMEM((2, f, d), BF16),
            pltpu.VMEM((LOAD_SLOTS, r, d), BF16),
            pltpu.VMEM((LOAD_SLOTS, r, d), BF16),
            pltpu.VMEM((SEND_SLOTS, r, d), BF16),
            pltpu.VMEM((SLOTS, r, d), BF16),
            pltpu.VMEM((SLOTS, r, d), BF16),
            pltpu.VMEM((SLOTS, r, d), BF16),
            dma((4,)),
            dma((2, 3)),
            dma((SUMMED,)),
            dma((2,)),
            dma((SUMMED,)),
            dma((2,)),
            dma((LOAD_SLOTS, 2)),
            dma((SEND_SLOTS,)),
            dma((SLOTS,)),
            dma((SLOTS,)),
            dma((SLOTS,)),
            dma((SLOTS,)),
            dma((SLOTS,)),
            dma((SLOTS,)),
            dma((SLOTS,)),
            dma,
        ],
        compiler_params=pltpu.CompilerParams(collective_id=0, has_side_effects=True, vmem_limit_bytes=VMEM_LIMIT),
        cost_estimate=pl.CostEstimate(flops=2 * 15 * t * d * ff, bytes_accessed=100 * d * ff, transcendentals=2 * t * ff),
        name="backward",
    )(a1, a0, h1, dy, wg, wu, wd)


def adamw_kernel(turned, n_old, w_ref, m_ref, v_ref, g_ref, *rest):
    w_out, m_out, v_out = rest[n_old:]
    g = g_ref[0].astype(F32)
    if turned:
        g = g.T
    m = 0.9 * m_ref[0] + 0.1 * g
    v = 0.95 * v_ref[0] + 0.05 * g * g
    w = w_ref[0].astype(F32)
    w_out[0] = (w - 0.02 * (m * lax.rsqrt(v + 1e-8) + 0.1 * w)).astype(BF16)
    m_out[0] = m
    v_out[0] = v


def adamw(which, blocks, first, g, w, m, v, old=()):
    low, high = blocks
    turned = which > 0
    d = min(w.shape[1], w.shape[2])
    f = max(w.shape[1], w.shape[2]) // BLOCKS

    def place(i, s):
        b = low + i
        layer, j = 1 - b // BLOCKS, b % BLOCKS
        return (layer, s, j) if turned else (layer, 2 * j + s, 0)

    if turned:
        spec = pl.BlockSpec((1, d // 2, f), place)
        g_spec = pl.BlockSpec((1, f, d // 2), lambda i, s: (3 * (low + i) + which - first, 0, s))
    else:
        spec = pl.BlockSpec((1, f // 2, d), place)
        g_spec = pl.BlockSpec((1, f // 2, d), lambda i, s: (3 * (low + i) + which - first, s, 0))
    n = (high - low) * d * f
    return pl.pallas_call(
        functools.partial(adamw_kernel, turned, len(old)),
        grid=(high - low, 2),
        out_shape=[jax.ShapeDtypeStruct(w.shape, BF16), jax.ShapeDtypeStruct(w.shape, F32), jax.ShapeDtypeStruct(w.shape, F32)],
        in_specs=[spec, spec, spec, g_spec] + [pl.BlockSpec(memory_space=pl.ANY)] * len(old),
        out_specs=[spec] * 3,
        input_output_aliases={4 + i: i for i in range(len(old))},
        compiler_params=pltpu.CompilerParams(vmem_limit_bytes=VMEM_LIMIT, dimension_semantics=("arbitrary", "arbitrary")),
        cost_estimate=pl.CostEstimate(flops=2000 * n, bytes_accessed=22 * n, transcendentals=n),
        name=f"adamw_{which}",
    )(w, m, v, g, *old)


def solution(mesh):
    def step(x, dy, *arrays):
        w, m, v = (arrays[i : i + 3] for i in (0, 3, 6))
        wg, wu, wd = w
        a0, h1, a1 = forward(x[0], wg, wu, wd)
        g, left, _, _ = backward(a1, a0, h1, dy[0], wg, wu, wd)
        left = lax.psum(left, "dp")
        new = []
        for name, which in ((0, 1), (1, 2), (2, 0)):
            done = (SUMMED - which + 2) // 3
            first = adamw(which, (0, done), 0, g, w[name], m[name], v[name])
            new.append((done, which, name, first))
        out = [adamw(which, (done, 2 * BLOCKS), SUMMED, left, w[name], m[name], v[name], first) for done, which, name, first in new]
        return tuple(one[kind] for kind in range(3) for one in out)

    return jax.shard_map(
        step,
        mesh=mesh,
        in_specs=(P(("rep", "dp"), None, None),) * 2 + (P(None, None, None),) * 9,
        out_specs=(P("rep", None, None),) * 9,
        check_vma=False,
    )
```

```python
import functools

import jax
import jax.numpy as jnp
from jax import lax
from jax.experimental import pallas as pl
from jax.experimental.pallas import tpu as pltpu
from jax.sharding import PartitionSpec as P

BF16, F32 = jnp.bfloat16, jnp.float32
MESH = pl.DeviceIdType.MESH
VMEM_LIMIT = 66_000_000
BLOCKS = 5
ALL = 6 * BLOCKS
SUMMED = 26
UNITS = 5
FIRST = 8
SLOTS, SEND_SLOTS, LOAD_SLOTS = 16, 8, 4
NN = (((1,), (0,)), ((), ()))
NT = (((1,), (1,)), ((), ()))


def dot(a, b, dims=NN):
    return lax.dot_general(a, b, dims, preferred_element_type=F32)


def scale_of(wide):
    return lax.rsqrt(jnp.mean(wide * wide, -1, keepdims=True) + 1e-6)


def cuts(n, width):
    starts = list(range(0, n - width + 1, width))
    return [(s, (starts[i + 1] if i + 1 < len(starts) else n) - s) for i, s in enumerate(starts)]


def forward_kernel(width, x_ref, wg_hbm, wu_hbm, wd_hbm, a0_ref, h1_ref, a1_ref, wg, wu, wd, p, sems):
    first = pl.program_id(0) == 0
    pieces = cuts(wg.shape[1], width)

    def loads(i):
        s, n = pieces[i]
        return (
            pltpu.make_async_copy(wg_hbm.at[0, :, pl.ds(s, n)], wg.at[:, pl.ds(s, n)], sems.at[0, i]),
            pltpu.make_async_copy(wu_hbm.at[0, :, pl.ds(s, n)], wu.at[:, pl.ds(s, n)], sems.at[1, i]),
            pltpu.make_async_copy(wd_hbm.at[0, pl.ds(s, n), :], wd.at[pl.ds(s, n), :], sems.at[2, i]),
        )

    @pl.when(first)
    def _():
        for i in range(len(pieces)):
            for c in loads(i)[:2]:
                c.start()
        for i in range(len(pieces)):
            loads(i)[2].start()

    def product(s, n, gate, up):
        p[:, s : s + n] = (gate * (0.5 * jnp.tanh(0.5 * gate) + 0.5) * up).astype(BF16)

    wide = x_ref[...].astype(F32)
    a = (wide * scale_of(wide)).astype(BF16)
    a0_ref[...] = a
    ready = None
    for i, (s, n) in enumerate(pieces):

        @pl.when(first)
        def _(i=i):
            for c in loads(i)[:2]:
                c.wait()

        gate = dot(a, wg[:, s : s + n])
        up = dot(a, wu[:, s : s + n])
        if ready is not None:
            product(*ready)
        ready = (s, n, gate, up)

    @pl.when(first)
    def _():
        for i in range(len(pieces)):
            loads(i)[2].wait()

    last = pieces[-1][0]
    down = dot(p[:, :last], wd[:last, :])
    product(*ready)
    down += dot(p[:, last:], wd[last:, :])
    h1 = (wide + down.astype(BF16).astype(F32)).astype(BF16)
    h1_ref[...] = h1
    wide1 = h1.astype(F32)
    a1_ref[...] = (wide1 * scale_of(wide1)).astype(BF16)


def forward(x, wg, wu, wd):
    t, d = x.shape
    ff = wg.shape[2]
    tile = min(t, 512)
    width = min(ff, 768)
    rows = pl.BlockSpec((tile, d), lambda i: (i, 0))
    anywhere = pl.BlockSpec(memory_space=pl.ANY)
    return pl.pallas_call(
        functools.partial(forward_kernel, width),
        grid=(t // tile,),
        out_shape=[jax.ShapeDtypeStruct((t, d), BF16)] * 3,
        in_specs=[rows, anywhere, anywhere, anywhere],
        out_specs=[rows] * 3,
        scratch_shapes=[
            pltpu.VMEM((d, ff), BF16),
            pltpu.VMEM((d, ff), BF16),
            pltpu.VMEM((ff, d), BF16),
            pltpu.VMEM((tile, ff), BF16),
            pltpu.SemaphoreType.DMA((3, len(cuts(ff, width)))),
        ],
        compiler_params=pltpu.CompilerParams(vmem_limit_bytes=VMEM_LIMIT, dimension_semantics=("arbitrary",)),
        cost_estimate=pl.CostEstimate(flops=6 * t * d * ff, bytes_accessed=6 * d * ff + 8 * t * d, transcendentals=t * ff),
        name="forward",
    )(x, wg, wu, wd)


BLOCK_STEPS, LOW_STEPS = 7, 5
TURN = BLOCKS * BLOCK_STEPS
STEPS = TURN + 1 + BLOCKS * LOW_STEPS


def step_of(s):
    low = s - (TURN + 1)
    block = jnp.where(s < TURN, s // BLOCK_STEPS, jnp.where(s == TURN, BLOCKS, BLOCKS + low // LOW_STEPS))
    kind = jnp.where(s < TURN, s % BLOCK_STEPS, jnp.where(s == TURN, 7, low % LOW_STEPS))
    return block, kind


def backward_kernel(
    a1_hbm, a0_hbm, h1_hbm, dy_hbm, wg_hbm, wu_hbm, wd_hbm,
    g_hbm, left_hbm, mine_hbm, theirs_hbm,
    ad, pgu, wgb, wub, wdb, wgt, wut, dat, stage, mb, xb, sb, ra, rb, tot,
    in_sem, w_sem, own_sem, give_sem, get_sem, left_sem, load_sem, s_sem, ra_sem, rb_sem, tot_sem, down_sem, up_sem, keep_sem, pass_sem, partner_sem,
):
    me = lax.axis_index("dp")
    z, core = me // 2, me % 2
    partner = me + 1 - 2 * core
    t, d = ad.shape[1:]
    f = stage.shape[1]
    half, r = f // 2, f // 2 // UNITS
    units = SUMMED * UNITS
    sub = dat.shape[2]

    def remote(src, dst, send, recv, device):
        return pltpu.make_async_remote_copy(src_ref=src, dst_ref=dst, send_sem=send, recv_sem=recv, device_id={"dp": device}, device_id_type=MESH)

    def weights(block):
        layer, j, slot = 1 - block // BLOCKS, block % BLOCKS, block % 2
        at = pl.ds(pl.multiple_of(j * f, f), f)
        return (
            pltpu.make_async_copy(wg_hbm.at[layer, :, at], wgb.at[slot], w_sem.at[slot, 0]),
            pltpu.make_async_copy(wu_hbm.at[layer, :, at], wub.at[slot], w_sem.at[slot, 1]),
            pltpu.make_async_copy(wd_hbm.at[layer, at, :], wdb.at[slot], w_sem.at[slot, 2]),
        )

    load_dy = pltpu.make_async_copy(dy_hbm, ad.at[0], in_sem.at[0])
    load_a1 = pltpu.make_async_copy(a1_hbm, ad.at[1], in_sem.at[1])
    load_h1 = pltpu.make_async_copy(h1_hbm, ad.at[1], in_sem.at[2])
    load_a0 = pltpu.make_async_copy(a0_hbm, ad.at[1], in_sem.at[3])

    load_a1.start()
    for c in weights(0):
        c.start()
    load_dy.start()
    dat[...] = jnp.zeros_like(dat)

    barrier = pltpu.get_barrier_semaphore()
    pl.semaphore_signal(barrier, inc=1, device_id={"dp": partner}, device_id_type=MESH)

    @pl.when(z > 0)
    def _():
        pl.semaphore_signal(barrier, inc=1, device_id={"dp": me - 2}, device_id_type=MESH)

    @pl.when(z < 3)
    def _():
        pl.semaphore_signal(barrier, inc=1, device_id={"dp": me + 2}, device_id_type=MESH)

    pl.semaphore_wait(barrier, 3 - z // 3 - (3 - z) // 3)

    def hidden(block, kind):
        slot = block % 2

        @pl.when(kind == 0)
        def _():
            @pl.when(block == 0)
            def _():
                load_dy.wait()
                load_a1.wait()

            @pl.when(block == BLOCKS)
            def _():
                load_a0.wait()

            for c in weights(block):
                c.wait()

            @pl.when(block + 1 < 2 * BLOCKS)
            def _():
                for c in weights(block + 1):
                    c.start()

            wgt[...] = wgb[slot].T
            wut[...] = wub[slot].T

        for i in range(t // 2 // sub):
            at = pl.ds(pl.multiple_of(kind * (t // 2) + i * sub, sub), sub)
            gate = dot(wgt[...], ad[1, at, :], NT)
            up = dot(wut[...], ad[1, at, :], NT)
            dp = dot(wdb[slot], ad[0, at, :], NT).astype(BF16).astype(F32)
            sig = 0.5 * jnp.tanh(0.5 * gate) + 0.5
            silu = gate * sig
            pgu[0, :, at] = (silu * up).astype(BF16)
            pgu[1, :, at] = (dp * up * (sig + silu * (1.0 - sig))).astype(BF16)
            pgu[2, :, at] = (dp * silu).astype(BF16)

    def gradient(block, kind):
        which = kind - 2
        slot = (3 * block + which) % 2
        rhs = jnp.minimum(which, 1)
        lhs = pgu[which]
        for i in range(2):
            cols = slice(i * (d // 2), (i + 1) * (d // 2))
            stage[slot, :, cols] = dot(lhs, ad[rhs, :, cols]).astype(BF16)

    def to_input(block, kind):
        slot = block % 2

        @pl.when((block == BLOCKS - 1) & (kind == 5))
        def _():
            load_h1.start()

        for i in range(t // 2 // sub):
            tile = (kind - 5) * (t // 2 // sub) + i
            at = pl.ds(pl.multiple_of(tile * sub, sub), sub)
            dat[tile] += dot(wgb[slot], pgu[1, :, at]) + dot(wub[slot], pgu[2, :, at])

    def turn():
        load_h1.wait()

        def body(i, _):
            at = pl.ds(pl.multiple_of(i * sub, sub), sub)
            da = dat[i].T.astype(BF16).astype(F32)
            wide = ad[1, at, :].astype(F32)
            scale = scale_of(wide)
            inner = jnp.sum(da * wide, -1, keepdims=True) * (scale * scale * scale) * (1.0 / d)
            through = (da * scale - wide * inner).astype(BF16).astype(F32)
            ad[0, at, :] = (ad[0, at, :].astype(F32) + through).astype(BF16)
            return 0

        lax.fori_loop(0, t // sub, body, 0)
        load_a0.start()

    def rows(slot, c):
        return stage.at[slot, pl.ds(pl.multiple_of(c * half, half), half), :]

    def piece_copies(q):
        slot = q % 2
        own = pltpu.make_async_copy(rows(slot, core), mine_hbm.at[q], own_sem.at[q])
        give = remote(rows(slot, 1 - core), theirs_hbm.at[q], give_sem.at[slot], get_sem.at[q], partner)
        return own, give

    def left_copy(q):
        return pltpu.make_async_copy(stage.at[q % 2], left_hbm.at[q - SUMMED], left_sem.at[q % 2])

    def send_stage(q):
        @pl.when(q < SUMMED)
        def _():
            own, give = piece_copies(q)
            own.start()
            give.start()

        @pl.when(q >= SUMMED)
        def _():
            left_copy(q).start()

    def wait_stage(q):
        @pl.when(q < SUMMED)
        def _():
            own, give = piece_copies(q)
            own.wait()
            give.wait_send()

        @pl.when(q >= SUMMED)
        def _():
            left_copy(q).wait()

    is0, is1, is2, is3 = z == 0, z == 1, z == 2, z == 3
    sum_lag = jnp.where(is1, 4, jnp.where(is2, 2, 0))
    tot_lag = jnp.where(is1, 4, jnp.where(is3, 10, 7))
    free_lag = tot_lag + jnp.where(is3, 3, 4)

    def load_copies(k):
        q, at, slot = k // UNITS, pl.ds(pl.multiple_of((k % UNITS) * r, r), r), k % LOAD_SLOTS
        return (
            pltpu.make_async_copy(mine_hbm.at[q, at, :], mb.at[slot], load_sem.at[slot, 0]),
            pltpu.make_async_copy(theirs_hbm.at[q, at, :], xb.at[slot], load_sem.at[slot, 1]),
        )

    def s_copy_edge(k):
        return remote(sb.at[k % SEND_SLOTS], ra.at[k % SLOTS], s_sem.at[k % SEND_SLOTS], ra_sem.at[k % SLOTS], me + 2 - 4 * (z // 3))

    def s_copy_inner(k):
        return remote(sb.at[k % SEND_SLOTS], rb.at[k % SLOTS], s_sem.at[k % SEND_SLOTS], rb_sem.at[k % SLOTS], me - 2)

    def tot_down(k):
        return remote(tot.at[k % SLOTS], tot.at[k % SLOTS], down_sem.at[k % SLOTS], tot_sem.at[k % SLOTS], me - 2)

    def tot_up(k):
        return remote(tot.at[k % SLOTS], tot.at[k % SLOTS], up_sem.at[k % SLOTS], tot_sem.at[k % SLOTS], me + 2)

    def out_copies(k):
        q, at, slot = k // UNITS, pl.ds(pl.multiple_of(core * half + (k % UNITS) * r, r), r), k % SLOTS
        return (
            pltpu.make_async_copy(tot.at[slot], g_hbm.at[q, at, :], keep_sem.at[slot]),
            remote(tot.at[slot], g_hbm.at[q, at, :], pass_sem.at[slot], partner_sem, partner),
        )

    def inside(k):
        return (k >= 0) & (k < units)

    def free(k):
        @pl.when(inside(k))
        def _():
            keep, give = out_copies(k)
            keep.wait()
            give.wait_send()

            @pl.when(is1)
            def _():
                tot_down(k).wait_send()

            @pl.when(is1 | is2)
            def _():
                tot_up(k).wait_send()

    def add(k):
        @pl.when(inside(k))
        def _():
            for c in load_copies(k):
                c.wait()
            slot = k % LOAD_SLOTS
            both = mb[slot].astype(F32) + xb[slot].astype(F32)

            @pl.when((is0 | is3) & (k >= SEND_SLOTS))
            def _():
                s_copy_edge(k - SEND_SLOTS).wait_send()

            @pl.when(is2 & (k >= SEND_SLOTS))
            def _():
                s_copy_inner(k - SEND_SLOTS).wait_send()

            @pl.when(is0 | is3)
            def _():
                sb[k % SEND_SLOTS] = both.astype(BF16)

            @pl.when(is2)
            def _():
                s_copy_edge(k).wait_recv()
                sb[k % SEND_SLOTS] = (both + ra[k % SLOTS].astype(F32)).astype(BF16)

            @pl.when(is1)
            def _():
                s_copy_edge(k).wait_recv()
                s_copy_inner(k).wait_recv()
                tot[k % SLOTS] = (both + ra[k % SLOTS].astype(F32) + rb[k % SLOTS].astype(F32)).astype(BF16)

    def arrive(k):
        @pl.when(inside(k) & (z != 1))
        def _():
            tot_down(k).wait_recv()

    def send(k_sum, k_tot):
        @pl.when(inside(k_sum) & (is0 | is3))
        def _():
            s_copy_edge(k_sum).start()

        @pl.when(inside(k_sum) & is2)
        def _():
            s_copy_inner(k_sum).start()

        @pl.when(inside(k_tot))
        def _():
            @pl.when(is1)
            def _():
                tot_down(k_tot).start()

            @pl.when(is1 | is2)
            def _():
                tot_up(k_tot).start()

            for c in out_copies(k_tot):
                c.start()

    def load(k):
        @pl.when(inside(k))
        def _():
            @pl.when(k % UNITS == 0)
            def _():
                piece_copies(k // UNITS)[1].wait_recv()

            for c in load_copies(k):
                c.start()


    def tick(i, _):
        step = i // 2
        works = i % 2 == 0

        @pl.when((step >= 1) & (step <= STEPS))
        def _():
            block, kind = step_of(step - 1)
            q = 3 * block + kind - 2

            @pl.when((kind >= 2) & (kind <= 4) & works)
            def _():
                send_stage(q)

            @pl.when((kind >= 2) & (kind <= 4) & (i % 2 == 1))
            def _():
                wait_stage(q)

        now = i - FIRST
        free(now - free_lag)
        add(now - sum_lag)
        arrive(now - tot_lag)
        send(now - sum_lag, now - tot_lag)
        load(now - sum_lag + 1)

        @pl.when(works & (step < STEPS))
        def _():
            block, kind = step_of(step)

            @pl.when(kind <= 1)
            def _():
                hidden(block, kind)

            @pl.when((kind >= 2) & (kind <= 4))
            def _():
                gradient(block, kind)

            @pl.when((kind == 5) | (kind == 6))
            def _():
                to_input(block, kind)

            @pl.when(kind == 7)
            def _():
                turn()

        return 0

    lax.fori_loop(0, max(FIRST + units + 14, 2 * STEPS + 2), tick, 0)

    for k in range(units - SEND_SLOTS, units):

        @pl.when(is0 | is3)
        def _(k=k):
            s_copy_edge(k).wait_send()

        @pl.when(is2)
        def _(k=k):
            s_copy_inner(k).wait_send()

    pltpu.make_async_copy(theirs_hbm, theirs_hbm, partner_sem).wait()


def backward(a1, a0, h1, dy, wg, wu, wd):
    t, d = a1.shape
    ff = wg.shape[2]
    f = ff // BLOCKS
    r = f // 2 // UNITS
    sub = t // 4
    anywhere = pl.BlockSpec(memory_space=pl.ANY)
    dma = pltpu.SemaphoreType.DMA
    return pl.pallas_call(
        backward_kernel,
        out_shape=[
            jax.ShapeDtypeStruct((SUMMED, f, d), BF16),
            jax.ShapeDtypeStruct((ALL - SUMMED, f, d), BF16),
            jax.ShapeDtypeStruct((SUMMED, f // 2, d), BF16),
            jax.ShapeDtypeStruct((SUMMED, f // 2, d), BF16),
        ],
        in_specs=[anywhere] * 7,
        out_specs=[anywhere] * 4,
        scratch_shapes=[
            pltpu.VMEM((2, t, d), BF16),
            pltpu.VMEM((3, f, t), BF16),
            pltpu.VMEM((2, d, f), BF16),
            pltpu.VMEM((2, d, f), BF16),
            pltpu.VMEM((2, f, d), BF16),
            pltpu.VMEM((f, d), BF16),
            pltpu.VMEM((f, d), BF16),
            pltpu.VMEM((4, d, sub), F32),
            pltpu.VMEM((2, f, d), BF16),
            pltpu.VMEM((LOAD_SLOTS, r, d), BF16),
            pltpu.VMEM((LOAD_SLOTS, r, d), BF16),
            pltpu.VMEM((SEND_SLOTS, r, d), BF16),
            pltpu.VMEM((SLOTS, r, d), BF16),
            pltpu.VMEM((SLOTS, r, d), BF16),
            pltpu.VMEM((SLOTS, r, d), BF16),
            dma((4,)),
            dma((2, 3)),
            dma((SUMMED,)),
            dma((2,)),
            dma((SUMMED,)),
            dma((2,)),
            dma((LOAD_SLOTS, 2)),
            dma((SEND_SLOTS,)),
            dma((SLOTS,)),
            dma((SLOTS,)),
            dma((SLOTS,)),
            dma((SLOTS,)),
            dma((SLOTS,)),
            dma((SLOTS,)),
            dma((SLOTS,)),
            dma,
        ],
        compiler_params=pltpu.CompilerParams(collective_id=0, has_side_effects=True, vmem_limit_bytes=VMEM_LIMIT),
        cost_estimate=pl.CostEstimate(flops=2 * 15 * t * d * ff, bytes_accessed=100 * d * ff, transcendentals=2 * t * ff),
        name="backward",
    )(a1, a0, h1, dy, wg, wu, wd)


HALVES = ((1, 0), (1, 1), (2, 0), (2, 1), (0, 0), (0, 1))


def adamw_kernel(rounds, first, n_old, *refs):
    arrays = {1: refs[0:3], 2: refs[3:6], 0: refs[6:9]}
    g_hbm = refs[9]
    outs = refs[10 + n_old :][:9]
    outs = {1: outs[0:3], 2: outs[3:6], 0: outs[6:9]}
    wt, mt, vt, gt, wd, md, vd, gd, wt_out, mt_out, vt_out, wd_out, md_out, vd_out, turned, in_sem, out_sem = refs[10 + n_old + 9 :]
    d, f = wt.shape[1] * 2, wt.shape[2]

    def place(b, half):
        which, s = HALVES[half]
        layer, j, q = 1 - b // BLOCKS, b % BLOCKS, 3 * b + which - first
        if which:
            cols = pl.ds(pl.multiple_of(j * f, f), f)
            return which, lambda ref: ref.at[layer, pl.ds(s * (d // 2), d // 2), cols], g_hbm.at[q, :, pl.ds(s * (d // 2), d // 2)]
        rows = pl.ds(pl.multiple_of(j * f + s * (f // 2), f // 2), f // 2)
        return which, lambda ref: ref.at[layer, rows, :], g_hbm.at[q, pl.ds(s * (f // 2), f // 2), :]

    def buffers(half):
        if HALVES[half][0]:
            return [x.at[half] for x in (wt, mt, vt, gt)], [x.at[half] for x in (wt_out, mt_out, vt_out)]
        return [x.at[half - 4] for x in (wd, md, vd, gd)], [x.at[half - 4] for x in (wd_out, md_out, vd_out)]

    def loads(b, half):
        which, at, g = place(b, half)
        sources = [at(x) for x in arrays[which]] + [g]
        return [pltpu.make_async_copy(x, y, in_sem.at[half, i]) for i, (x, y) in enumerate(zip(sources, buffers(half)[0], strict=True))]

    def stores(b, half):
        which, at, _ = place(b, half)
        return [pltpu.make_async_copy(x, at(y), out_sem.at[half, i]) for i, (x, y) in enumerate(zip(buffers(half)[1], outs[which], strict=True))]

    def take(half):
        (w_in, m_in, v_in, g_in), (w_out, m_out, v_out) = buffers(half)
        if HALVES[half][0]:
            turned[...] = g_in[...].T
            g_in = turned

        def body(i, _):
            at = pl.ds(pl.multiple_of(i * 16, 16), 16)
            g = g_in[at, :].astype(F32)
            m = 0.9 * m_in[at, :] + 0.1 * g
            v = 0.95 * v_in[at, :] + 0.05 * g * g
            w = w_in[at, :].astype(F32)
            w_out[at, :] = (w - 0.02 * (m * lax.rsqrt(v + 1e-8) + 0.1 * w)).astype(BF16)
            m_out[at, :] = m
            v_out[at, :] = v
            return 0

        lax.fori_loop(0, w_in.shape[0] // 16, body, 0, unroll=2)

    def start(copies):
        for c in copies:
            c.start()

    def wait(copies):
        for c in copies:
            c.wait()

    starts = {}
    for blocks, halves in rounds:
        for half in halves:
            if half not in starts:
                starts[half] = True
                start(loads(blocks[0], half))
    before = {}
    for n, (blocks, halves) in enumerate(rounds):
        low, high = blocks

        def next_of(half, n=n):
            return next((bs[0] for bs, hs in rounds[n + 1 :] if half in hs), None)

        def one(b, half, low=low, high=high, next_of=next_of):
            wait(loads(b, half))
            if half in before:
                wait(stores(before[half], half))
            elif high - low > 1:

                @pl.when(b > low)
                def _():
                    wait(stores(b - 1, half))

            take(half)
            start(stores(b, half))
            if high - low > 1:

                @pl.when(b + 1 < high)
                def _():
                    start(loads(b + 1, half))

            after = next_of(half)
            if after is not None:
                if high - low > 1:

                    @pl.when(b + 1 == high)
                    def _():
                        start(loads(after, half))

                else:
                    start(loads(after, half))

        def turn(b, _, halves=halves):
            for half in halves:
                one(b, half)
            return 0

        if high - low > 1:
            lax.fori_loop(low, high, turn, 0)
        else:
            turn(low, 0)
        for half in halves:
            before[half] = high - 1
    for half, b in before.items():
        wait(stores(b, half))


def adamw(pieces, first, g, w, m, v, old=()):
    low, high = pieces
    d, ff = w[0].shape[1:]
    f = ff // BLOCKS
    rounds = []
    for b in range(2 * BLOCKS):
        halves = tuple(h for h, (which, _) in enumerate(HALVES) if low <= 3 * b + which < high)
        if not halves:
            continue
        if len(rounds) == 1 and rounds[0][1] == halves:
            rounds[-1] = ((rounds[-1][0][0], b + 1), halves)
        else:
            rounds.append(((b, b + 1), halves))
    anywhere = pl.BlockSpec(memory_space=pl.ANY)
    operands = [x for i in range(3) for x in (w[i], m[i], v[i])]
    n = (high - low) * d * f
    return pl.pallas_call(
        functools.partial(adamw_kernel, tuple(rounds), first, len(old)),
        out_shape=[jax.ShapeDtypeStruct(x.shape, x.dtype) for x in operands],
        in_specs=[anywhere] * (10 + len(old)),
        out_specs=[anywhere] * 9,
        scratch_shapes=[
            pltpu.VMEM((4, d // 2, f), BF16),
            pltpu.VMEM((4, d // 2, f), F32),
            pltpu.VMEM((4, d // 2, f), F32),
            pltpu.VMEM((4, f, d // 2), BF16),
            pltpu.VMEM((2, f // 2, d), BF16),
            pltpu.VMEM((2, f // 2, d), F32),
            pltpu.VMEM((2, f // 2, d), F32),
            pltpu.VMEM((2, f // 2, d), BF16),
            pltpu.VMEM((4, d // 2, f), BF16),
            pltpu.VMEM((4, d // 2, f), F32),
            pltpu.VMEM((4, d // 2, f), F32),
            pltpu.VMEM((2, f // 2, d), BF16),
            pltpu.VMEM((2, f // 2, d), F32),
            pltpu.VMEM((2, f // 2, d), F32),
            pltpu.VMEM((d // 2, f), BF16),
            pltpu.SemaphoreType.DMA((6, 4)),
            pltpu.SemaphoreType.DMA((6, 3)),
        ],
        input_output_aliases={10 + i: i for i in range(len(old))},
        compiler_params=pltpu.CompilerParams(vmem_limit_bytes=VMEM_LIMIT),
        cost_estimate=pl.CostEstimate(flops=2000 * n, bytes_accessed=22 * n, transcendentals=n),
        name="adamw",
    )(*operands, g, *old)


def solution(mesh):
    def step(x, dy, *arrays):
        w, m, v = (arrays[i : i + 3] for i in (0, 3, 6))
        wg, wu, wd = w
        a0, h1, a1 = forward(x[0], wg, wu, wd)
        g, left, _, _ = backward(a1, a0, h1, dy[0], wg, wu, wd)
        left = lax.psum(left, "dp")
        done = adamw((0, SUMMED), 0, g, w, m, v)
        done = adamw((SUMMED, ALL), SUMMED, left, w, m, v, done)
        return tuple(done[3 * i + kind] for kind in range(3) for i in range(3))

    return jax.shard_map(
        step,
        mesh=mesh,
        in_specs=(P(("rep", "dp"), None, None),) * 2 + (P(None, None, None),) * 9,
        out_specs=(P("rep", None, None),) * 9,
        check_vma=False,
    )
```

```python
import functools

import jax
import jax.numpy as jnp
from jax import lax
from jax.experimental import pallas as pl
from jax.experimental.pallas import tpu as pltpu
from jax.sharding import PartitionSpec as P

BF16, F32 = jnp.bfloat16, jnp.float32
MESH = pl.DeviceIdType.MESH
VMEM_LIMIT = 66_000_000
BLOCKS = 5
ALL = 6 * BLOCKS
SUMMED = 26
UNITS = 5
FIRST = 8
SLOTS, SEND_SLOTS, LOAD_SLOTS = 32, 16, 4
NN = (((1,), (0,)), ((), ()))
NT = (((1,), (1,)), ((), ()))


def dot(a, b, dims=NN):
    return lax.dot_general(a, b, dims, preferred_element_type=F32)


def scale_of(wide):
    return lax.rsqrt(jnp.mean(wide * wide, -1, keepdims=True) + 1e-6)


def cuts(n, width):
    starts = list(range(0, n - width + 1, width))
    return [(s, (starts[i + 1] if i + 1 < len(starts) else n) - s) for i, s in enumerate(starts)]


def forward_kernel(width, x_ref, wg_hbm, wu_hbm, wd_hbm, a0_ref, h1_ref, a1_ref, wg, wu, wd, p, sems):
    first = pl.program_id(0) == 0
    pieces = cuts(wg.shape[1], width)

    def loads(i):
        s, n = pieces[i]
        return (
            pltpu.make_async_copy(wg_hbm.at[0, :, pl.ds(s, n)], wg.at[:, pl.ds(s, n)], sems.at[0, i]),
            pltpu.make_async_copy(wu_hbm.at[0, :, pl.ds(s, n)], wu.at[:, pl.ds(s, n)], sems.at[1, i]),
            pltpu.make_async_copy(wd_hbm.at[0, pl.ds(s, n), :], wd.at[pl.ds(s, n), :], sems.at[2, i]),
        )

    @pl.when(first)
    def _():
        for i in range(len(pieces)):
            for c in loads(i)[:2]:
                c.start()
        for i in range(len(pieces)):
            loads(i)[2].start()

    wide = x_ref[...].astype(F32)
    a = (wide * scale_of(wide)).astype(BF16)
    a0_ref[...] = a
    for i, (s, n) in enumerate(pieces):

        @pl.when(first)
        def _(i=i):
            for c in loads(i)[:2]:
                c.wait()

        gate = dot(a, wg[:, s : s + n])
        up = dot(a, wu[:, s : s + n])
        p[:, s : s + n] = (gate * (0.5 * jnp.tanh(0.5 * gate) + 0.5) * up).astype(BF16)

    @pl.when(first)
    def _():
        for i in range(len(pieces)):
            loads(i)[2].wait()

    h1 = (wide + dot(p[...], wd[...]).astype(BF16).astype(F32)).astype(BF16)
    h1_ref[...] = h1
    wide1 = h1.astype(F32)
    a1_ref[...] = (wide1 * scale_of(wide1)).astype(BF16)


def forward(x, wg, wu, wd):
    t, d = x.shape
    ff = wg.shape[2]
    tile = min(t, 512)
    width = min(ff, 768)
    rows = pl.BlockSpec((tile, d), lambda i: (i, 0))
    anywhere = pl.BlockSpec(memory_space=pl.ANY)
    return pl.pallas_call(
        functools.partial(forward_kernel, width),
        grid=(t // tile,),
        out_shape=[jax.ShapeDtypeStruct((t, d), BF16)] * 3,
        in_specs=[rows, anywhere, anywhere, anywhere],
        out_specs=[rows] * 3,
        scratch_shapes=[
            pltpu.VMEM((d, ff), BF16),
            pltpu.VMEM((d, ff), BF16),
            pltpu.VMEM((ff, d), BF16),
            pltpu.VMEM((tile, ff), BF16),
            pltpu.SemaphoreType.DMA((3, len(cuts(ff, width)))),
        ],
        compiler_params=pltpu.CompilerParams(vmem_limit_bytes=VMEM_LIMIT, dimension_semantics=("arbitrary",)),
        cost_estimate=pl.CostEstimate(flops=6 * t * d * ff, bytes_accessed=6 * d * ff + 8 * t * d, transcendentals=t * ff),
        name="forward",
    )(x, wg, wu, wd)


HALF_STEPS, TILES = 5, 4
BLOCK_STEPS, LOW_STEPS = 2 * HALF_STEPS + TILES, 2 * HALF_STEPS
TURN = BLOCKS * BLOCK_STEPS
STEPS = TURN + TILES + BLOCKS * LOW_STEPS


def step_of(s):
    low = s - (TURN + TILES)
    block = jnp.where(s < TURN, s // BLOCK_STEPS, jnp.where(low < 0, BLOCKS, BLOCKS + low // LOW_STEPS))
    place = jnp.where(s < TURN, s % BLOCK_STEPS, jnp.where(low < 0, BLOCK_STEPS + s - TURN, low % LOW_STEPS))
    return block, place


def summed_piece(c):
    full, rest = SUMMED // 3, max(SUMMED % 3, 1)
    late = c - 6 * full
    return tuple(
        jnp.where(late < 0, early, other) for early, other in ((c // 6, full), (c % 6 // 3, late // rest), (c % 3, late % rest))
    )


def place_of(block, half, which):
    full, rest = SUMMED // 3, SUMMED % 3
    return jnp.where(block < full, 6 * block + 3 * half + which, 6 * full + rest * half + which)


def backward_kernel(
    a1_hbm, a0_hbm, h1_hbm, dy_hbm, wg_hbm, wu_hbm, wd_hbm,
    g_hbm, left_hbm, mine_hbm, theirs_hbm,
    ad, pgu, wgb, wub, wdb, wgt, wut, dat, stage, mb, xb, sb, ra, rb, tot,
    in_sem, w_sem, own_sem, give_sem, get_sem, left_sem, load_sem, s_sem, ra_sem, rb_sem, tot_sem, down_sem, up_sem, keep_sem, pass_sem, partner_sem,
):
    me = lax.axis_index("dp")
    z, core = me // 2, me % 2
    partner = me + 1 - 2 * core
    t, d = ad.shape[1:]
    f, fs = wgt.shape[0], stage.shape[1]
    part, r = fs // 2, fs // 2 // UNITS
    units = 2 * SUMMED * UNITS
    sub = dat.shape[2]

    def remote(src, dst, send, recv, device):
        return pltpu.make_async_remote_copy(src_ref=src, dst_ref=dst, send_sem=send, recv_sem=recv, device_id={"dp": device}, device_id_type=MESH)

    def weights(block):
        layer, j, slot = 1 - block // BLOCKS, block % BLOCKS, block % 2
        at = pl.ds(pl.multiple_of(j * f, f), f)
        return (
            pltpu.make_async_copy(wg_hbm.at[layer, :, at], wgb.at[slot], w_sem.at[slot, 0]),
            pltpu.make_async_copy(wu_hbm.at[layer, :, at], wub.at[slot], w_sem.at[slot, 1]),
            pltpu.make_async_copy(wd_hbm.at[layer, at, :], wdb.at[slot], w_sem.at[slot, 2]),
        )

    load_dy = pltpu.make_async_copy(dy_hbm, ad.at[0], in_sem.at[0])
    load_a1 = pltpu.make_async_copy(a1_hbm, ad.at[1], in_sem.at[1])
    load_h1 = pltpu.make_async_copy(h1_hbm, ad.at[1], in_sem.at[2])
    load_a0 = pltpu.make_async_copy(a0_hbm, ad.at[1], in_sem.at[3])

    load_a1.start()
    for c in weights(0):
        c.start()
    load_dy.start()
    dat[...] = jnp.zeros_like(dat)

    barrier = pltpu.get_barrier_semaphore()
    pl.semaphore_signal(barrier, inc=1, device_id={"dp": partner}, device_id_type=MESH)

    @pl.when(z > 0)
    def _():
        pl.semaphore_signal(barrier, inc=1, device_id={"dp": me - 2}, device_id_type=MESH)

    @pl.when(z < 3)
    def _():
        pl.semaphore_signal(barrier, inc=1, device_id={"dp": me + 2}, device_id_type=MESH)

    pl.semaphore_wait(barrier, 3 - z // 3 - (3 - z) // 3)

    def at_half(half):
        return pl.ds(pl.multiple_of(half * fs, fs), fs)

    def hidden(block, half, tokens):
        slot = block % 2

        @pl.when((half == 0) & (tokens == 0))
        def _():
            @pl.when(block == 0)
            def _():
                load_a1.wait()
                load_dy.wait()

            @pl.when(block == BLOCKS)
            def _():
                load_a0.wait()

            for c in weights(block):
                c.wait()

            @pl.when(block + 1 < 2 * BLOCKS)
            def _():
                for c in weights(block + 1):
                    c.start()

            wgt[...] = wgb[slot].T
            wut[...] = wub[slot].T

        units_at = at_half(half)
        for i in range(t // 2 // sub):
            at = pl.ds(pl.multiple_of(tokens * (t // 2) + i * sub, sub), sub)
            gate = dot(wgt[units_at, :], ad[1, at, :], NT)
            up = dot(wut[units_at, :], ad[1, at, :], NT)
            dp = dot(wdb[slot, units_at, :], ad[0, at, :], NT).astype(BF16).astype(F32)
            sig = 0.5 * jnp.tanh(0.5 * gate) + 0.5
            silu = gate * sig
            pgu[0, units_at, at] = (silu * up).astype(BF16)
            pgu[1, units_at, at] = (dp * up * (sig + silu * (1.0 - sig))).astype(BF16)
            pgu[2, units_at, at] = (dp * silu).astype(BF16)

    def gradient(block, half, which):
        rhs = jnp.minimum(which, 1)
        stage[slot_of(half, which)] = dot(pgu[which, at_half(half), :], ad[rhs]).astype(BF16)

    def to_input(block, tile):
        slot = block % 2

        @pl.when((block == BLOCKS - 1) & (tile == 0))
        def _():
            load_h1.start()

        at = pl.ds(pl.multiple_of(tile * sub, sub), sub)
        dat[tile] += dot(wgb[slot], pgu[1, :, at]) + dot(wub[slot], pgu[2, :, at])

    def turn(tile):
        @pl.when(tile == 0)
        def _():
            load_h1.wait()

        at = pl.ds(pl.multiple_of(tile * sub, sub), sub)
        da = dat[tile].T.astype(BF16).astype(F32)
        wide = ad[1, at, :].astype(F32)
        scale = scale_of(wide)
        inner = jnp.sum(da * wide, -1, keepdims=True) * (scale * scale * scale) * (1.0 / d)
        through = (da * scale - wide * inner).astype(BF16).astype(F32)
        ad[0, at, :] = (ad[0, at, :].astype(F32) + through).astype(BF16)

        @pl.when(tile == TILES - 1)
        def _():
            load_a0.start()

    def slot_of(half, which):
        return (half + which) % 2

    def rows(slot, c):
        return stage.at[slot, pl.ds(pl.multiple_of(c * part, part), part), :]

    def give_copy(slot, c):
        return remote(rows(slot, 1 - core), theirs_hbm.at[c], give_sem.at[slot], get_sem.at[c], partner)

    def own_copy(slot, c):
        return pltpu.make_async_copy(rows(slot, core), mine_hbm.at[c], own_sem.at[slot])

    def left_copy(slot, block, half, which):
        return pltpu.make_async_copy(stage.at[slot], left_hbm.at[3 * block + which - SUMMED, at_half(half), :], left_sem.at[slot])

    def stage_copies(block, half, which, go):
        slot, here = slot_of(half, which), 3 * block + which < SUMMED

        @pl.when(here)
        def _():
            c = place_of(block, half, which)
            if go:
                own_copy(slot, c).start()
                give_copy(slot, c).start()
            else:
                own_copy(slot, c).wait()
                give_copy(slot, c).wait_send()

        @pl.when(jnp.logical_not(here))
        def _():
            copy = left_copy(slot, block, half, which)
            if go:
                copy.start()
            else:
                copy.wait()

    is0, is1, is2, is3 = z == 0, z == 1, z == 2, z == 3
    sum_lag = jnp.where(is1, 6, jnp.where(is2, 3, 0))
    tot_lag = jnp.where(is1, 6, jnp.where(is3, 15, 11))
    free_lag = tot_lag + jnp.where(is3, 4, 6)

    def load_copies(k):
        q, at, slot = k // UNITS, pl.ds(pl.multiple_of((k % UNITS) * r, r), r), k % LOAD_SLOTS
        return (
            pltpu.make_async_copy(mine_hbm.at[q, at, :], mb.at[slot], load_sem.at[slot, 0]),
            pltpu.make_async_copy(theirs_hbm.at[q, at, :], xb.at[slot], load_sem.at[slot, 1]),
        )

    def s_copy_edge(k):
        return remote(sb.at[k % SEND_SLOTS], ra.at[k % SLOTS], s_sem.at[k % SEND_SLOTS], ra_sem.at[k % SLOTS], me + 2 - 4 * (z // 3))

    def s_copy_inner(k):
        return remote(sb.at[k % SEND_SLOTS], rb.at[k % SLOTS], s_sem.at[k % SEND_SLOTS], rb_sem.at[k % SLOTS], me - 2)

    def tot_down(k):
        return remote(tot.at[k % SLOTS], tot.at[k % SLOTS], down_sem.at[k % SLOTS], tot_sem.at[k % SLOTS], me - 2)

    def tot_up(k):
        return remote(tot.at[k % SLOTS], tot.at[k % SLOTS], up_sem.at[k % SLOTS], tot_sem.at[k % SLOTS], me + 2)

    def out_copies(k):
        block, half, which = summed_piece(k // UNITS)
        q, at, slot = 3 * block + which, pl.ds(pl.multiple_of(half * fs + core * part + (k % UNITS) * r, r), r), k % SLOTS
        return (
            pltpu.make_async_copy(tot.at[slot], g_hbm.at[q, at, :], keep_sem.at[slot]),
            remote(tot.at[slot], g_hbm.at[q, at, :], pass_sem.at[slot], partner_sem, partner),
        )

    def inside(k):
        return (k >= 0) & (k < units)

    def free(k):
        @pl.when(inside(k))
        def _():
            keep, give = out_copies(k)
            keep.wait()
            give.wait_send()

            @pl.when(is1)
            def _():
                tot_down(k).wait_send()

            @pl.when(is1 | is2)
            def _():
                tot_up(k).wait_send()

    def add(k):
        @pl.when(inside(k))
        def _():
            for c in load_copies(k):
                c.wait()
            slot = k % LOAD_SLOTS
            both = mb[slot].astype(F32) + xb[slot].astype(F32)

            @pl.when((is0 | is3) & (k >= SEND_SLOTS))
            def _():
                s_copy_edge(k - SEND_SLOTS).wait_send()

            @pl.when(is2 & (k >= SEND_SLOTS))
            def _():
                s_copy_inner(k - SEND_SLOTS).wait_send()

            @pl.when(is0 | is3)
            def _():
                sb[k % SEND_SLOTS] = both.astype(BF16)

            @pl.when(is2)
            def _():
                s_copy_edge(k).wait_recv()
                sb[k % SEND_SLOTS] = (both + ra[k % SLOTS].astype(F32)).astype(BF16)

            @pl.when(is1)
            def _():
                s_copy_edge(k).wait_recv()
                s_copy_inner(k).wait_recv()
                tot[k % SLOTS] = (both + ra[k % SLOTS].astype(F32) + rb[k % SLOTS].astype(F32)).astype(BF16)

    def arrive(k):
        @pl.when(inside(k) & (z != 1))
        def _():
            tot_down(k).wait_recv()

    def send(k_sum, k_tot):
        @pl.when(inside(k_sum) & (is0 | is3))
        def _():
            s_copy_edge(k_sum).start()

        @pl.when(inside(k_sum) & is2)
        def _():
            s_copy_inner(k_sum).start()

        @pl.when(inside(k_tot))
        def _():
            @pl.when(is1)
            def _():
                tot_down(k_tot).start()

            @pl.when(is1 | is2)
            def _():
                tot_up(k_tot).start()

            for c in out_copies(k_tot):
                c.start()

    def load(k):
        @pl.when(inside(k))
        def _():
            @pl.when(k % UNITS == 0)
            def _():
                give_copy(0, k // UNITS).wait_recv()

            for c in load_copies(k):
                c.start()


    def tick(i, _):
        step = i // 2
        works = i % 2 == 0

        @pl.when((step >= 1) & (step <= STEPS))
        def _():
            block, place = step_of(step - 1)
            half, kind = place // HALF_STEPS, place % HALF_STEPS
            made = (place < LOW_STEPS) & (kind >= 2)

            @pl.when(made & works)
            def _():
                stage_copies(block, half, kind - 2, True)

            @pl.when(made & (i % 2 == 1))
            def _():
                stage_copies(block, half, kind - 2, False)

        now = i - FIRST
        free(now - free_lag)
        add(now - sum_lag)
        arrive(now - tot_lag)
        send(now - sum_lag, now - tot_lag)
        load(now - sum_lag + 1)

        @pl.when(works & (step < STEPS))
        def _():
            block, place = step_of(step)
            half, kind = place // HALF_STEPS, place % HALF_STEPS

            @pl.when((place < LOW_STEPS) & (kind < 2))
            def _():
                hidden(block, half, kind)

            @pl.when((place < LOW_STEPS) & (kind >= 2))
            def _():
                gradient(block, half, kind - 2)

            @pl.when((place >= LOW_STEPS) & (place < BLOCK_STEPS))
            def _():
                to_input(block, place - LOW_STEPS)

            @pl.when(place >= BLOCK_STEPS)
            def _():
                turn(place - BLOCK_STEPS)

        return 0

    lax.fori_loop(0, max(FIRST + units + 20, 2 * STEPS + 2), tick, 0)

    for k in range(units - SEND_SLOTS, units):

        @pl.when(is0 | is3)
        def _(k=k):
            s_copy_edge(k).wait_send()

        @pl.when(is2)
        def _(k=k):
            s_copy_inner(k).wait_send()

    pltpu.make_async_copy(theirs_hbm, theirs_hbm, partner_sem).wait()


def backward(a1, a0, h1, dy, wg, wu, wd):
    t, d = a1.shape
    ff = wg.shape[2]
    f = ff // BLOCKS
    fs = f // 2
    r = fs // 2 // UNITS
    sub = t // TILES
    anywhere = pl.BlockSpec(memory_space=pl.ANY)
    dma = pltpu.SemaphoreType.DMA
    return pl.pallas_call(
        backward_kernel,
        out_shape=[
            jax.ShapeDtypeStruct((SUMMED, f, d), BF16),
            jax.ShapeDtypeStruct((ALL - SUMMED, f, d), BF16),
            jax.ShapeDtypeStruct((2 * SUMMED, fs // 2, d), BF16),
            jax.ShapeDtypeStruct((2 * SUMMED, fs // 2, d), BF16),
        ],
        in_specs=[anywhere] * 7,
        out_specs=[anywhere] * 4,
        scratch_shapes=[
            pltpu.VMEM((2, t, d), BF16),
            pltpu.VMEM((3, f, t), BF16),
            pltpu.VMEM((2, d, f), BF16),
            pltpu.VMEM((2, d, f), BF16),
            pltpu.VMEM((2, f, d), BF16),
            pltpu.VMEM((f, d), BF16),
            pltpu.VMEM((f, d), BF16),
            pltpu.VMEM((TILES, d, sub), F32),
            pltpu.VMEM((2, fs, d), BF16),
            pltpu.VMEM((LOAD_SLOTS, r, d), BF16),
            pltpu.VMEM((LOAD_SLOTS, r, d), BF16),
            pltpu.VMEM((SEND_SLOTS, r, d), BF16),
            pltpu.VMEM((SLOTS, r, d), BF16),
            pltpu.VMEM((SLOTS, r, d), BF16),
            pltpu.VMEM((SLOTS, r, d), BF16),
            dma((4,)),
            dma((2, 3)),
            dma((2,)),
            dma((2,)),
            dma((2 * SUMMED,)),
            dma((2,)),
            dma((LOAD_SLOTS, 2)),
            dma((SEND_SLOTS,)),
            dma((SLOTS,)),
            dma((SLOTS,)),
            dma((SLOTS,)),
            dma((SLOTS,)),
            dma((SLOTS,)),
            dma((SLOTS,)),
            dma((SLOTS,)),
            dma,
        ],
        compiler_params=pltpu.CompilerParams(collective_id=0, has_side_effects=True, vmem_limit_bytes=VMEM_LIMIT),
        cost_estimate=pl.CostEstimate(flops=2 * 15 * t * d * ff, bytes_accessed=100 * d * ff, transcendentals=2 * t * ff),
        name="backward",
    )(a1, a0, h1, dy, wg, wu, wd)


HALVES = ((1, 0), (1, 1), (2, 0), (2, 1), (0, 0), (0, 1))


def adamw_kernel(rounds, first, n_old, *refs):
    arrays = {1: refs[0:3], 2: refs[3:6], 0: refs[6:9]}
    g_hbm = refs[9]
    outs = refs[10 + n_old :][:9]
    outs = {1: outs[0:3], 2: outs[3:6], 0: outs[6:9]}
    wt, mt, vt, gt, wd, md, vd, gd, wt_out, mt_out, vt_out, wd_out, md_out, vd_out, turned, in_sem, out_sem = refs[10 + n_old + 9 :]
    d, f = wt.shape[1] * 2, wt.shape[2]

    def place(b, half):
        which, s = HALVES[half]
        layer, j, q = 1 - b // BLOCKS, b % BLOCKS, 3 * b + which - first
        if which:
            cols = pl.ds(pl.multiple_of(j * f, f), f)
            return which, lambda ref: ref.at[layer, pl.ds(s * (d // 2), d // 2), cols], g_hbm.at[q, :, pl.ds(s * (d // 2), d // 2)]
        rows = pl.ds(pl.multiple_of(j * f + s * (f // 2), f // 2), f // 2)
        return which, lambda ref: ref.at[layer, rows, :], g_hbm.at[q, pl.ds(s * (f // 2), f // 2), :]

    def buffers(half):
        if HALVES[half][0]:
            return [x.at[half] for x in (wt, mt, vt, gt)], [x.at[half] for x in (wt_out, mt_out, vt_out)]
        return [x.at[half - 4] for x in (wd, md, vd, gd)], [x.at[half - 4] for x in (wd_out, md_out, vd_out)]

    def loads(b, half):
        which, at, g = place(b, half)
        sources = [at(x) for x in arrays[which]] + [g]
        return [pltpu.make_async_copy(x, y, in_sem.at[half, i]) for i, (x, y) in enumerate(zip(sources, buffers(half)[0], strict=True))]

    def stores(b, half):
        which, at, _ = place(b, half)
        return [pltpu.make_async_copy(x, at(y), out_sem.at[half, i]) for i, (x, y) in enumerate(zip(buffers(half)[1], outs[which], strict=True))]

    def take(half):
        (w_in, m_in, v_in, g_in), (w_out, m_out, v_out) = buffers(half)
        if HALVES[half][0]:
            turned[...] = g_in[...].T
            g_in = turned

        def body(i, _):
            at = pl.ds(pl.multiple_of(i * 16, 16), 16)
            g = g_in[at, :].astype(F32)
            m = 0.9 * m_in[at, :] + 0.1 * g
            v = 0.95 * v_in[at, :] + 0.05 * g * g
            w = w_in[at, :].astype(F32)
            w_out[at, :] = (w - 0.02 * (m * lax.rsqrt(v + 1e-8) + 0.1 * w)).astype(BF16)
            m_out[at, :] = m
            v_out[at, :] = v
            return 0

        lax.fori_loop(0, w_in.shape[0] // 16, body, 0, unroll=2)

    def start(copies):
        for c in copies:
            c.start()

    def wait(copies):
        for c in copies:
            c.wait()

    starts = {}
    for blocks, halves in rounds:
        for half in halves:
            if half not in starts:
                starts[half] = True
                start(loads(blocks[0], half))
    before = {}
    for n, (blocks, halves) in enumerate(rounds):
        low, high = blocks

        def next_of(half, n=n):
            return next((bs[0] for bs, hs in rounds[n + 1 :] if half in hs), None)

        def one(b, half, low=low, high=high, next_of=next_of):
            wait(loads(b, half))
            if half in before:
                wait(stores(before[half], half))
            elif high - low > 1:

                @pl.when(b > low)
                def _():
                    wait(stores(b - 1, half))

            take(half)
            start(stores(b, half))
            if high - low > 1:

                @pl.when(b + 1 < high)
                def _():
                    start(loads(b + 1, half))

            after = next_of(half)
            if after is not None:
                if high - low > 1:

                    @pl.when(b + 1 == high)
                    def _():
                        start(loads(after, half))

                else:
                    start(loads(after, half))

        def turn(b, _, halves=halves):
            for half in halves:
                one(b, half)
            return 0

        if high - low > 1:
            lax.fori_loop(low, high, turn, 0)
        else:
            turn(low, 0)
        for half in halves:
            before[half] = high - 1
    for half, b in before.items():
        wait(stores(b, half))


def adamw(pieces, first, g, w, m, v, old=()):
    low, high = pieces
    d, ff = w[0].shape[1:]
    f = ff // BLOCKS
    rounds = []
    for b in range(2 * BLOCKS):
        halves = tuple(h for h, (which, _) in enumerate(HALVES) if low <= 3 * b + which < high)
        if not halves:
            continue
        if len(rounds) == 1 and rounds[0][1] == halves:
            rounds[-1] = ((rounds[-1][0][0], b + 1), halves)
        else:
            rounds.append(((b, b + 1), halves))
    anywhere = pl.BlockSpec(memory_space=pl.ANY)
    operands = [x for i in range(3) for x in (w[i], m[i], v[i])]
    n = (high - low) * d * f
    return pl.pallas_call(
        functools.partial(adamw_kernel, tuple(rounds), first, len(old)),
        out_shape=[jax.ShapeDtypeStruct(x.shape, x.dtype) for x in operands],
        in_specs=[anywhere] * (10 + len(old)),
        out_specs=[anywhere] * 9,
        scratch_shapes=[
            pltpu.VMEM((4, d // 2, f), BF16),
            pltpu.VMEM((4, d // 2, f), F32),
            pltpu.VMEM((4, d // 2, f), F32),
            pltpu.VMEM((4, f, d // 2), BF16),
            pltpu.VMEM((2, f // 2, d), BF16),
            pltpu.VMEM((2, f // 2, d), F32),
            pltpu.VMEM((2, f // 2, d), F32),
            pltpu.VMEM((2, f // 2, d), BF16),
            pltpu.VMEM((4, d // 2, f), BF16),
            pltpu.VMEM((4, d // 2, f), F32),
            pltpu.VMEM((4, d // 2, f), F32),
            pltpu.VMEM((2, f // 2, d), BF16),
            pltpu.VMEM((2, f // 2, d), F32),
            pltpu.VMEM((2, f // 2, d), F32),
            pltpu.VMEM((d // 2, f), BF16),
            pltpu.SemaphoreType.DMA((6, 4)),
            pltpu.SemaphoreType.DMA((6, 3)),
        ],
        input_output_aliases={10 + i: i for i in range(len(old))},
        compiler_params=pltpu.CompilerParams(vmem_limit_bytes=VMEM_LIMIT),
        cost_estimate=pl.CostEstimate(flops=2000 * n, bytes_accessed=22 * n, transcendentals=n),
        name="adamw",
    )(*operands, g, *old)


def solution(mesh):
    def step(x, dy, *arrays):
        w, m, v = (arrays[i : i + 3] for i in (0, 3, 6))
        wg, wu, wd = w
        a0, h1, a1 = forward(x[0], wg, wu, wd)
        g, left, _, _ = backward(a1, a0, h1, dy[0], wg, wu, wd)
        left = lax.psum(left, "dp")
        done = adamw((0, SUMMED), 0, g, w, m, v)
        done = adamw((SUMMED, ALL), SUMMED, left, w, m, v, done)
        return tuple(done[3 * i + kind] for kind in range(3) for i in range(3))

    return jax.shard_map(
        step,
        mesh=mesh,
        in_specs=(P(("rep", "dp"), None, None),) * 2 + (P(None, None, None),) * 9,
        out_specs=(P("rep", None, None),) * 9,
        check_vma=False,
    )
```

```python
import functools

import jax
import jax.numpy as jnp
from jax import lax
from jax.experimental import pallas as pl
from jax.experimental.pallas import tpu as pltpu
from jax.sharding import PartitionSpec as P

BF16, F32 = jnp.bfloat16, jnp.float32
MESH = pl.DeviceIdType.MESH
VMEM_LIMIT = 66_000_000
BLOCKS = 5
ALL = 6 * BLOCKS
SUMMED = 26
UNITS = 2
FIRST = 4
SLOTS, SEND_SLOTS, LOAD_SLOTS = 12, 6, 4
NN = (((1,), (0,)), ((), ()))
NT = (((1,), (1,)), ((), ()))


def dot(a, b, dims=NN):
    return lax.dot_general(a, b, dims, preferred_element_type=F32)


def scale_of(wide):
    return lax.rsqrt(jnp.mean(wide * wide, -1, keepdims=True) + 1e-6)


def cuts(n, width):
    starts = list(range(0, n - width + 1, width))
    return [(s, (starts[i + 1] if i + 1 < len(starts) else n) - s) for i, s in enumerate(starts)]


def forward_kernel(width, x_ref, wg_hbm, wu_hbm, wd_hbm, a0_ref, h1_ref, a1_ref, wg, wu, wd, p, sems):
    first = pl.program_id(0) == 0
    pieces = cuts(wg.shape[1], width)

    def loads(i):
        s, n = pieces[i]
        return (
            pltpu.make_async_copy(wg_hbm.at[0, :, pl.ds(s, n)], wg.at[:, pl.ds(s, n)], sems.at[0, i]),
            pltpu.make_async_copy(wu_hbm.at[0, :, pl.ds(s, n)], wu.at[:, pl.ds(s, n)], sems.at[1, i]),
            pltpu.make_async_copy(wd_hbm.at[0, pl.ds(s, n), :], wd.at[pl.ds(s, n), :], sems.at[2, i]),
        )

    @pl.when(first)
    def _():
        for i in range(len(pieces)):
            for c in loads(i)[:2]:
                c.start()
        for i in range(len(pieces)):
            loads(i)[2].start()

    wide = x_ref[...].astype(F32)
    a = (wide * scale_of(wide)).astype(BF16)
    a0_ref[...] = a
    for i, (s, n) in enumerate(pieces):

        @pl.when(first)
        def _(i=i):
            for c in loads(i)[:2]:
                c.wait()

        gate = dot(a, wg[:, s : s + n])
        up = dot(a, wu[:, s : s + n])
        p[:, s : s + n] = (gate * (0.5 * jnp.tanh(0.5 * gate) + 0.5) * up).astype(BF16)

    @pl.when(first)
    def _():
        for i in range(len(pieces)):
            loads(i)[2].wait()

    h1 = (wide + dot(p[...], wd[...]).astype(BF16).astype(F32)).astype(BF16)
    h1_ref[...] = h1
    wide1 = h1.astype(F32)
    a1_ref[...] = (wide1 * scale_of(wide1)).astype(BF16)


def forward(x, wg, wu, wd):
    t, d = x.shape
    ff = wg.shape[2]
    tile = min(t, 512)
    width = min(ff, 768)
    rows = pl.BlockSpec((tile, d), lambda i: (i, 0))
    anywhere = pl.BlockSpec(memory_space=pl.ANY)
    return pl.pallas_call(
        functools.partial(forward_kernel, width),
        grid=(t // tile,),
        out_shape=[jax.ShapeDtypeStruct((t, d), BF16)] * 3,
        in_specs=[rows, anywhere, anywhere, anywhere],
        out_specs=[rows] * 3,
        scratch_shapes=[
            pltpu.VMEM((d, ff), BF16),
            pltpu.VMEM((d, ff), BF16),
            pltpu.VMEM((ff, d), BF16),
            pltpu.VMEM((tile, ff), BF16),
            pltpu.SemaphoreType.DMA((3, len(cuts(ff, width)))),
        ],
        compiler_params=pltpu.CompilerParams(vmem_limit_bytes=VMEM_LIMIT, dimension_semantics=("arbitrary",)),
        cost_estimate=pl.CostEstimate(flops=6 * t * d * ff, bytes_accessed=6 * d * ff + 8 * t * d, transcendentals=t * ff),
        name="forward",
    )(x, wg, wu, wd)


HALF_STEPS, DA_STEPS, TILES = 4, 2, 4
BLOCK_STEPS, LOW_STEPS = 2 * HALF_STEPS + DA_STEPS, 2 * HALF_STEPS
TURN = BLOCKS * BLOCK_STEPS
STEPS = TURN + DA_STEPS + BLOCKS * LOW_STEPS


def step_of(s):
    low = s - (TURN + DA_STEPS)
    block = jnp.where(s < TURN, s // BLOCK_STEPS, jnp.where(low < 0, BLOCKS, BLOCKS + low // LOW_STEPS))
    place = jnp.where(s < TURN, s % BLOCK_STEPS, jnp.where(low < 0, BLOCK_STEPS + s - TURN, low % LOW_STEPS))
    return block, place


def summed_piece(c):
    full, rest = SUMMED // 3, max(SUMMED % 3, 1)
    late = c - 6 * full
    return tuple(
        jnp.where(late < 0, early, other) for early, other in ((c // 6, full), (c % 6 // 3, late // rest), (c % 3, late % rest))
    )


def place_of(block, half, which):
    full, rest = SUMMED // 3, SUMMED % 3
    return jnp.where(block < full, 6 * block + 3 * half + which, 6 * full + rest * half + which)


def backward_kernel(
    a1_hbm, a0_hbm, h1_hbm, dy_hbm, wg_hbm, wu_hbm, wd_hbm,
    g_hbm, left_hbm, mine_hbm, theirs_hbm,
    ad, pgu, wgb, wub, wdb, wgt, wut, dat, stage, mb, xb, sb, ra, rb, tot,
    in_sem, w_sem, own_sem, give_sem, get_sem, left_sem, load_sem, s_sem, ra_sem, rb_sem, tot_sem, down_sem, up_sem, keep_sem, pass_sem, partner_sem,
):
    me = lax.axis_index("dp")
    z, core = me // 2, me % 2
    partner = me + 1 - 2 * core
    t, d = ad.shape[1:]
    f, fs = wgt.shape[0], stage.shape[1]
    part, r = fs // 2, fs // 2 // UNITS
    units = 2 * SUMMED * UNITS
    sub = dat.shape[2]

    def remote(src, dst, send, recv, device):
        return pltpu.make_async_remote_copy(src_ref=src, dst_ref=dst, send_sem=send, recv_sem=recv, device_id={"dp": device}, device_id_type=MESH)

    def weights(block):
        layer, j, slot = 1 - block // BLOCKS, block % BLOCKS, block % 2
        at = pl.ds(pl.multiple_of(j * f, f), f)
        return (
            pltpu.make_async_copy(wg_hbm.at[layer, :, at], wgb.at[slot], w_sem.at[slot, 0]),
            pltpu.make_async_copy(wu_hbm.at[layer, :, at], wub.at[slot], w_sem.at[slot, 1]),
            pltpu.make_async_copy(wd_hbm.at[layer, at, :], wdb.at[slot], w_sem.at[slot, 2]),
        )

    load_dy = pltpu.make_async_copy(dy_hbm, ad.at[0], in_sem.at[0])
    load_a1 = pltpu.make_async_copy(a1_hbm, ad.at[1], in_sem.at[1])
    load_h1 = pltpu.make_async_copy(h1_hbm, ad.at[1], in_sem.at[2])
    load_a0 = pltpu.make_async_copy(a0_hbm, ad.at[1], in_sem.at[3])

    load_a1.start()
    for c in weights(0):
        c.start()
    load_dy.start()
    dat[...] = jnp.zeros_like(dat)

    barrier = pltpu.get_barrier_semaphore()
    pl.semaphore_signal(barrier, inc=1, device_id={"dp": partner}, device_id_type=MESH)

    @pl.when(z > 0)
    def _():
        pl.semaphore_signal(barrier, inc=1, device_id={"dp": me - 2}, device_id_type=MESH)

    @pl.when(z < 3)
    def _():
        pl.semaphore_signal(barrier, inc=1, device_id={"dp": me + 2}, device_id_type=MESH)

    pl.semaphore_wait(barrier, 3 - z // 3 - (3 - z) // 3)

    def at_half(half):
        return pl.ds(pl.multiple_of(half * fs, fs), fs)

    def hidden(block, half):
        slot = block % 2

        @pl.when(half == 0)
        def _():
            @pl.when(block == 0)
            def _():
                load_a1.wait()
                load_dy.wait()

            @pl.when(block == BLOCKS)
            def _():
                load_a0.wait()

            for c in weights(block):
                c.wait()

            @pl.when(block + 1 < 2 * BLOCKS)
            def _():
                for c in weights(block + 1):
                    c.start()

            wgt[...] = wgb[slot].T
            wut[...] = wub[slot].T

        units_at = at_half(half)
        for i in range(TILES):
            at = pl.ds(i * sub, sub)
            gate = dot(wgt[units_at, :], ad[1, at, :], NT)
            up = dot(wut[units_at, :], ad[1, at, :], NT)
            dp = dot(wdb[slot, units_at, :], ad[0, at, :], NT).astype(BF16).astype(F32)
            sig = 0.5 * jnp.tanh(0.5 * gate) + 0.5
            silu = gate * sig
            pgu[0, units_at, at] = (silu * up).astype(BF16)
            pgu[1, units_at, at] = (dp * up * (sig + silu * (1.0 - sig))).astype(BF16)
            pgu[2, units_at, at] = (dp * silu).astype(BF16)

    def gradient(block, half, which):
        rhs = jnp.minimum(which, 1)
        stage[slot_of(half, which)] = dot(pgu[which, at_half(half), :], ad[rhs]).astype(BF16)

    def to_input(block, step):
        slot = block % 2

        @pl.when((block == BLOCKS - 1) & (step == 0))
        def _():
            load_h1.start()

        for i in range(TILES // DA_STEPS):
            tile = step * (TILES // DA_STEPS) + i
            at = pl.ds(pl.multiple_of(tile * sub, sub), sub)
            dat[tile] += dot(wgb[slot], pgu[1, :, at]) + dot(wub[slot], pgu[2, :, at])

    def turn(step):
        @pl.when(step == 0)
        def _():
            load_h1.wait()

        def body(i, _):
            tile = step * (TILES // DA_STEPS) + i
            at = pl.ds(pl.multiple_of(tile * sub, sub), sub)
            da = dat[tile].T.astype(BF16).astype(F32)
            wide = ad[1, at, :].astype(F32)
            scale = scale_of(wide)
            inner = jnp.sum(da * wide, -1, keepdims=True) * (scale * scale * scale) * (1.0 / d)
            through = (da * scale - wide * inner).astype(BF16).astype(F32)
            ad[0, at, :] = (ad[0, at, :].astype(F32) + through).astype(BF16)
            return 0

        lax.fori_loop(0, TILES // DA_STEPS, body, 0)

        @pl.when(step == DA_STEPS - 1)
        def _():
            load_a0.start()

    def slot_of(half, which):
        return (half + which) % 2

    def rows(slot, c):
        return stage.at[slot, pl.ds(pl.multiple_of(c * part, part), part), :]

    def give_copy(slot, c):
        return remote(rows(slot, 1 - core), theirs_hbm.at[c], give_sem.at[slot], get_sem.at[c], partner)

    def own_copy(slot, c):
        return pltpu.make_async_copy(rows(slot, core), mine_hbm.at[c], own_sem.at[slot])

    def left_copy(slot, block, half, which):
        return pltpu.make_async_copy(stage.at[slot], left_hbm.at[3 * block + which - SUMMED, at_half(half), :], left_sem.at[slot])

    def stage_copies(block, half, which, go):
        slot, here = slot_of(half, which), 3 * block + which < SUMMED

        @pl.when(here)
        def _():
            c = place_of(block, half, which)
            if go:
                own_copy(slot, c).start()
                give_copy(slot, c).start()
            else:
                own_copy(slot, c).wait()
                give_copy(slot, c).wait_send()

        @pl.when(jnp.logical_not(here))
        def _():
            copy = left_copy(slot, block, half, which)
            if go:
                copy.start()
            else:
                copy.wait()

    is0, is1, is2, is3 = z == 0, z == 1, z == 2, z == 3
    sum_lag = jnp.where(is1, 2, jnp.where(is2, 1, 0))
    tot_lag = jnp.where(is1, 2, jnp.where(is3, 9, 6))
    free_lag = tot_lag + jnp.where(is3, 2, 3)

    def load_copies(k):
        q, at, slot = k // UNITS, pl.ds(pl.multiple_of((k % UNITS) * r, r), r), k % LOAD_SLOTS
        return (
            pltpu.make_async_copy(mine_hbm.at[q, at, :], mb.at[slot], load_sem.at[slot, 0]),
            pltpu.make_async_copy(theirs_hbm.at[q, at, :], xb.at[slot], load_sem.at[slot, 1]),
        )

    def s_copy_edge(k):
        return remote(sb.at[k % SEND_SLOTS], ra.at[k % SLOTS], s_sem.at[k % SEND_SLOTS], ra_sem.at[k % SLOTS], me + 2 - 4 * (z // 3))

    def s_copy_inner(k):
        return remote(sb.at[k % SEND_SLOTS], rb.at[k % SLOTS], s_sem.at[k % SEND_SLOTS], rb_sem.at[k % SLOTS], me - 2)

    def tot_down(k):
        return remote(tot.at[k % SLOTS], tot.at[k % SLOTS], down_sem.at[k % SLOTS], tot_sem.at[k % SLOTS], me - 2)

    def tot_up(k):
        return remote(tot.at[k % SLOTS], tot.at[k % SLOTS], up_sem.at[k % SLOTS], tot_sem.at[k % SLOTS], me + 2)

    def out_copies(k):
        block, half, which = summed_piece(k // UNITS)
        q, at, slot = 3 * block + which, pl.ds(pl.multiple_of(half * fs + core * part + (k % UNITS) * r, r), r), k % SLOTS
        return (
            pltpu.make_async_copy(tot.at[slot], g_hbm.at[q, at, :], keep_sem.at[slot]),
            remote(tot.at[slot], g_hbm.at[q, at, :], pass_sem.at[slot], partner_sem, partner),
        )

    def inside(k):
        return (k >= 0) & (k < units)

    def free(k):
        @pl.when(inside(k))
        def _():
            keep, give = out_copies(k)
            keep.wait()
            give.wait_send()

            @pl.when(is1)
            def _():
                tot_down(k).wait_send()

            @pl.when(is1 | is2)
            def _():
                tot_up(k).wait_send()

    def add(k):
        @pl.when(inside(k))
        def _():
            for c in load_copies(k):
                c.wait()
            slot = k % LOAD_SLOTS
            both = mb[slot].astype(F32) + xb[slot].astype(F32)

            @pl.when((is0 | is3) & (k >= SEND_SLOTS))
            def _():
                s_copy_edge(k - SEND_SLOTS).wait_send()

            @pl.when(is2 & (k >= SEND_SLOTS))
            def _():
                s_copy_inner(k - SEND_SLOTS).wait_send()

            @pl.when(is0 | is3)
            def _():
                sb[k % SEND_SLOTS] = both.astype(BF16)

            @pl.when(is2)
            def _():
                s_copy_edge(k).wait_recv()
                sb[k % SEND_SLOTS] = (both + ra[k % SLOTS].astype(F32)).astype(BF16)

            @pl.when(is1)
            def _():
                s_copy_edge(k).wait_recv()
                s_copy_inner(k).wait_recv()
                tot[k % SLOTS] = (both + ra[k % SLOTS].astype(F32) + rb[k % SLOTS].astype(F32)).astype(BF16)

    def arrive(k):
        @pl.when(inside(k) & (z != 1))
        def _():
            tot_down(k).wait_recv()

    def send(k_sum, k_tot):
        @pl.when(inside(k_sum) & (is0 | is3))
        def _():
            s_copy_edge(k_sum).start()

        @pl.when(inside(k_sum) & is2)
        def _():
            s_copy_inner(k_sum).start()

        @pl.when(inside(k_tot))
        def _():
            @pl.when(is1)
            def _():
                tot_down(k_tot).start()

            @pl.when(is1 | is2)
            def _():
                tot_up(k_tot).start()

            for c in out_copies(k_tot):
                c.start()

    def load(k):
        @pl.when(inside(k))
        def _():
            @pl.when(k % UNITS == 0)
            def _():
                give_copy(0, k // UNITS).wait_recv()

            for c in load_copies(k):
                c.start()


    def stage_of(s, go):
        @pl.when((s >= 0) & (s < STEPS))
        def _():
            block, place = step_of(s)
            half, kind = place // HALF_STEPS, place % HALF_STEPS

            @pl.when((place < LOW_STEPS) & (kind >= 1))
            def _():
                stage_copies(block, half, kind - 1, go)

    def tick(i, _):
        stage_of(i - 2, False)
        stage_of(i - 1, True)
        now = i - FIRST
        free(now - free_lag)
        add(now - sum_lag)
        arrive(now - tot_lag)
        send(now - sum_lag, now - tot_lag)
        load(now - sum_lag + 1)

        @pl.when(i < STEPS)
        def _():
            block, place = step_of(i)
            half, kind = place // HALF_STEPS, place % HALF_STEPS

            @pl.when((place < LOW_STEPS) & (kind == 0))
            def _():
                hidden(block, half)

            @pl.when((place < LOW_STEPS) & (kind >= 1))
            def _():
                gradient(block, half, kind - 1)

            @pl.when((place >= LOW_STEPS) & (place < BLOCK_STEPS))
            def _():
                to_input(block, place - LOW_STEPS)

            @pl.when(place >= BLOCK_STEPS)
            def _():
                turn(place - BLOCK_STEPS)

        return 0

    lax.fori_loop(0, max(FIRST + units + 12, STEPS + 2), tick, 0)

    for k in range(units - SEND_SLOTS, units):

        @pl.when(is0 | is3)
        def _(k=k):
            s_copy_edge(k).wait_send()

        @pl.when(is2)
        def _(k=k):
            s_copy_inner(k).wait_send()

    pltpu.make_async_copy(theirs_hbm, theirs_hbm, partner_sem).wait()


def backward(a1, a0, h1, dy, wg, wu, wd):
    t, d = a1.shape
    ff = wg.shape[2]
    f = ff // BLOCKS
    fs = f // 2
    r = fs // 2 // UNITS
    sub = t // TILES
    anywhere = pl.BlockSpec(memory_space=pl.ANY)
    dma = pltpu.SemaphoreType.DMA
    return pl.pallas_call(
        backward_kernel,
        out_shape=[
            jax.ShapeDtypeStruct((SUMMED, f, d), BF16),
            jax.ShapeDtypeStruct((ALL - SUMMED, f, d), BF16),
            jax.ShapeDtypeStruct((2 * SUMMED, fs // 2, d), BF16),
            jax.ShapeDtypeStruct((2 * SUMMED, fs // 2, d), BF16),
        ],
        in_specs=[anywhere] * 7,
        out_specs=[anywhere] * 4,
        scratch_shapes=[
            pltpu.VMEM((2, t, d), BF16),
            pltpu.VMEM((3, f, t), BF16),
            pltpu.VMEM((2, d, f), BF16),
            pltpu.VMEM((2, d, f), BF16),
            pltpu.VMEM((2, f, d), BF16),
            pltpu.VMEM((f, d), BF16),
            pltpu.VMEM((f, d), BF16),
            pltpu.VMEM((TILES, d, sub), F32),
            pltpu.VMEM((2, fs, d), BF16),
            pltpu.VMEM((LOAD_SLOTS, r, d), BF16),
            pltpu.VMEM((LOAD_SLOTS, r, d), BF16),
            pltpu.VMEM((SEND_SLOTS, r, d), BF16),
            pltpu.VMEM((SLOTS, r, d), BF16),
            pltpu.VMEM((SLOTS, r, d), BF16),
            pltpu.VMEM((SLOTS, r, d), BF16),
            dma((4,)),
            dma((2, 3)),
            dma((2,)),
            dma((2,)),
            dma((2 * SUMMED,)),
            dma((2,)),
            dma((LOAD_SLOTS, 2)),
            dma((SEND_SLOTS,)),
            dma((SLOTS,)),
            dma((SLOTS,)),
            dma((SLOTS,)),
            dma((SLOTS,)),
            dma((SLOTS,)),
            dma((SLOTS,)),
            dma((SLOTS,)),
            dma,
        ],
        compiler_params=pltpu.CompilerParams(collective_id=0, has_side_effects=True, vmem_limit_bytes=VMEM_LIMIT),
        cost_estimate=pl.CostEstimate(flops=2 * 15 * t * d * ff, bytes_accessed=100 * d * ff, transcendentals=2 * t * ff),
        name="backward",
    )(a1, a0, h1, dy, wg, wu, wd)


HALVES = ((1, 0), (1, 1), (2, 0), (2, 1), (0, 0), (0, 1))


def adamw_kernel(rounds, first, n_old, *refs):
    arrays = {1: refs[0:3], 2: refs[3:6], 0: refs[6:9]}
    g_hbm = refs[9]
    outs = refs[10 + n_old :][:9]
    outs = {1: outs[0:3], 2: outs[3:6], 0: outs[6:9]}
    wt, mt, vt, gt, wd, md, vd, gd, wt_out, mt_out, vt_out, wd_out, md_out, vd_out, turned, in_sem, out_sem = refs[10 + n_old + 9 :]
    d, f = wt.shape[1] * 2, wt.shape[2]

    def place(b, half):
        which, s = HALVES[half]
        layer, j, q = 1 - b // BLOCKS, b % BLOCKS, 3 * b + which - first
        if which:
            cols = pl.ds(pl.multiple_of(j * f, f), f)
            return which, lambda ref: ref.at[layer, pl.ds(s * (d // 2), d // 2), cols], g_hbm.at[q, :, pl.ds(s * (d // 2), d // 2)]
        rows = pl.ds(pl.multiple_of(j * f + s * (f // 2), f // 2), f // 2)
        return which, lambda ref: ref.at[layer, rows, :], g_hbm.at[q, pl.ds(s * (f // 2), f // 2), :]

    def buffers(half):
        if HALVES[half][0]:
            return [x.at[half] for x in (wt, mt, vt, gt)], [x.at[half] for x in (wt_out, mt_out, vt_out)]
        return [x.at[half - 4] for x in (wd, md, vd, gd)], [x.at[half - 4] for x in (wd_out, md_out, vd_out)]

    def loads(b, half):
        which, at, g = place(b, half)
        sources = [at(x) for x in arrays[which]] + [g]
        return [pltpu.make_async_copy(x, y, in_sem.at[half, i]) for i, (x, y) in enumerate(zip(sources, buffers(half)[0], strict=True))]

    def stores(b, half):
        which, at, _ = place(b, half)
        return [pltpu.make_async_copy(x, at(y), out_sem.at[half, i]) for i, (x, y) in enumerate(zip(buffers(half)[1], outs[which], strict=True))]

    def take(half):
        (w_in, m_in, v_in, g_in), (w_out, m_out, v_out) = buffers(half)
        if HALVES[half][0]:
            turned[...] = g_in[...].T
            g_in = turned

        def body(i, _):
            at = pl.ds(pl.multiple_of(i * 16, 16), 16)
            g = g_in[at, :].astype(F32)
            m = 0.9 * m_in[at, :] + 0.1 * g
            v = 0.95 * v_in[at, :] + 0.05 * g * g
            w = w_in[at, :].astype(F32)
            w_out[at, :] = (w - 0.02 * (m * lax.rsqrt(v + 1e-8) + 0.1 * w)).astype(BF16)
            m_out[at, :] = m
            v_out[at, :] = v
            return 0

        lax.fori_loop(0, w_in.shape[0] // 16, body, 0, unroll=2)

    def start(copies):
        for c in copies:
            c.start()

    def wait(copies):
        for c in copies:
            c.wait()

    starts = {}
    for blocks, halves in rounds:
        for half in halves:
            if half not in starts:
                starts[half] = True
                start(loads(blocks[0], half))
    before = {}
    for n, (blocks, halves) in enumerate(rounds):
        low, high = blocks

        def next_of(half, n=n):
            return next((bs[0] for bs, hs in rounds[n + 1 :] if half in hs), None)

        def one(b, half, low=low, high=high, next_of=next_of):
            wait(loads(b, half))
            if half in before:
                wait(stores(before[half], half))
            elif high - low > 1:

                @pl.when(b > low)
                def _():
                    wait(stores(b - 1, half))

            take(half)
            start(stores(b, half))
            if high - low > 1:

                @pl.when(b + 1 < high)
                def _():
                    start(loads(b + 1, half))

            after = next_of(half)
            if after is not None:
                if high - low > 1:

                    @pl.when(b + 1 == high)
                    def _():
                        start(loads(after, half))

                else:
                    start(loads(after, half))

        def turn(b, _, halves=halves):
            for half in halves:
                one(b, half)
            return 0

        if high - low > 1:
            lax.fori_loop(low, high, turn, 0)
        else:
            turn(low, 0)
        for half in halves:
            before[half] = high - 1
    for half, b in before.items():
        wait(stores(b, half))


def adamw(pieces, first, g, w, m, v, old=()):
    low, high = pieces
    d, ff = w[0].shape[1:]
    f = ff // BLOCKS
    rounds = []
    for b in range(2 * BLOCKS):
        halves = tuple(h for h, (which, _) in enumerate(HALVES) if low <= 3 * b + which < high)
        if not halves:
            continue
        if len(rounds) == 1 and rounds[0][1] == halves:
            rounds[-1] = ((rounds[-1][0][0], b + 1), halves)
        else:
            rounds.append(((b, b + 1), halves))
    anywhere = pl.BlockSpec(memory_space=pl.ANY)
    operands = [x for i in range(3) for x in (w[i], m[i], v[i])]
    n = (high - low) * d * f
    return pl.pallas_call(
        functools.partial(adamw_kernel, tuple(rounds), first, len(old)),
        out_shape=[jax.ShapeDtypeStruct(x.shape, x.dtype) for x in operands],
        in_specs=[anywhere] * (10 + len(old)),
        out_specs=[anywhere] * 9,
        scratch_shapes=[
            pltpu.VMEM((4, d // 2, f), BF16),
            pltpu.VMEM((4, d // 2, f), F32),
            pltpu.VMEM((4, d // 2, f), F32),
            pltpu.VMEM((4, f, d // 2), BF16),
            pltpu.VMEM((2, f // 2, d), BF16),
            pltpu.VMEM((2, f // 2, d), F32),
            pltpu.VMEM((2, f // 2, d), F32),
            pltpu.VMEM((2, f // 2, d), BF16),
            pltpu.VMEM((4, d // 2, f), BF16),
            pltpu.VMEM((4, d // 2, f), F32),
            pltpu.VMEM((4, d // 2, f), F32),
            pltpu.VMEM((2, f // 2, d), BF16),
            pltpu.VMEM((2, f // 2, d), F32),
            pltpu.VMEM((2, f // 2, d), F32),
            pltpu.VMEM((d // 2, f), BF16),
            pltpu.SemaphoreType.DMA((6, 4)),
            pltpu.SemaphoreType.DMA((6, 3)),
        ],
        input_output_aliases={10 + i: i for i in range(len(old))},
        compiler_params=pltpu.CompilerParams(vmem_limit_bytes=VMEM_LIMIT),
        cost_estimate=pl.CostEstimate(flops=2000 * n, bytes_accessed=22 * n, transcendentals=n),
        name="adamw",
    )(*operands, g, *old)


def solution(mesh):
    def step(x, dy, *arrays):
        w, m, v = (arrays[i : i + 3] for i in (0, 3, 6))
        wg, wu, wd = w
        a0, h1, a1 = forward(x[0], wg, wu, wd)
        g, left, _, _ = backward(a1, a0, h1, dy[0], wg, wu, wd)
        left = lax.psum(left, "dp")
        done = adamw((0, SUMMED), 0, g, w, m, v)
        done = adamw((SUMMED, ALL), SUMMED, left, w, m, v, done)
        return tuple(done[3 * i + kind] for kind in range(3) for i in range(3))

    return jax.shard_map(
        step,
        mesh=mesh,
        in_specs=(P(("rep", "dp"), None, None),) * 2 + (P(None, None, None),) * 9,
        out_specs=(P("rep", None, None),) * 9,
        check_vma=False,
    )
```

```python
import functools

import jax
import jax.numpy as jnp
from jax import lax
from jax.experimental import pallas as pl
from jax.experimental.pallas import tpu as pltpu
from jax.sharding import PartitionSpec as P

BF16, F32 = jnp.bfloat16, jnp.float32
MESH = pl.DeviceIdType.MESH
VMEM_LIMIT = 66_000_000
BLOCKS = 5
ALL = 6 * BLOCKS
SUMMED = 26
UNITS = 2
FINE, PIECES = 2, 5
FIRST = 4
SLOTS, SEND_SLOTS, LOAD_SLOTS = 12, 6, 4
NN = (((1,), (0,)), ((), ()))
NT = (((1,), (1,)), ((), ()))


def dot(a, b, dims=NN):
    return lax.dot_general(a, b, dims, preferred_element_type=F32)


def scale_of(wide):
    return lax.rsqrt(jnp.mean(wide * wide, -1, keepdims=True) + 1e-6)


def cuts(n, width):
    starts = list(range(0, n - width + 1, width))
    return [(s, (starts[i + 1] if i + 1 < len(starts) else n) - s) for i, s in enumerate(starts)]


def forward_kernel(width, x_ref, wg_hbm, wu_hbm, wd_hbm, a0_ref, h1_ref, a1_ref, wg, wu, wd, p, sems):
    first = pl.program_id(0) == 0
    pieces = cuts(wg.shape[1], width)

    def loads(i):
        s, n = pieces[i]
        return (
            pltpu.make_async_copy(wg_hbm.at[0, :, pl.ds(s, n)], wg.at[:, pl.ds(s, n)], sems.at[0, i]),
            pltpu.make_async_copy(wu_hbm.at[0, :, pl.ds(s, n)], wu.at[:, pl.ds(s, n)], sems.at[1, i]),
            pltpu.make_async_copy(wd_hbm.at[0, pl.ds(s, n), :], wd.at[pl.ds(s, n), :], sems.at[2, i]),
        )

    @pl.when(first)
    def _():
        for i in range(len(pieces)):
            for c in loads(i)[:2]:
                c.start()
        for i in range(len(pieces)):
            loads(i)[2].start()

    wide = x_ref[...].astype(F32)
    a = (wide * scale_of(wide)).astype(BF16)
    a0_ref[...] = a
    for i, (s, n) in enumerate(pieces):

        @pl.when(first)
        def _(i=i):
            for c in loads(i)[:2]:
                c.wait()

        gate = dot(a, wg[:, s : s + n])
        up = dot(a, wu[:, s : s + n])
        p[:, s : s + n] = (gate * (0.5 * jnp.tanh(0.5 * gate) + 0.5) * up).astype(BF16)

    @pl.when(first)
    def _():
        for i in range(len(pieces)):
            loads(i)[2].wait()

    h1 = (wide + dot(p[...], wd[...]).astype(BF16).astype(F32)).astype(BF16)
    h1_ref[...] = h1
    wide1 = h1.astype(F32)
    a1_ref[...] = (wide1 * scale_of(wide1)).astype(BF16)


def forward(x, wg, wu, wd):
    t, d = x.shape
    ff = wg.shape[2]
    tile = min(t, 1024)
    width = min(ff, 768)
    rows = pl.BlockSpec((tile, d), lambda i: (i, 0))
    anywhere = pl.BlockSpec(memory_space=pl.ANY)
    return pl.pallas_call(
        functools.partial(forward_kernel, width),
        grid=(t // tile,),
        out_shape=[jax.ShapeDtypeStruct((t, d), BF16)] * 3,
        in_specs=[rows, anywhere, anywhere, anywhere],
        out_specs=[rows] * 3,
        scratch_shapes=[
            pltpu.VMEM((d, ff), BF16),
            pltpu.VMEM((d, ff), BF16),
            pltpu.VMEM((ff, d), BF16),
            pltpu.VMEM((tile, ff), BF16),
            pltpu.SemaphoreType.DMA((3, len(cuts(ff, width)))),
        ],
        compiler_params=pltpu.CompilerParams(vmem_limit_bytes=VMEM_LIMIT, dimension_semantics=("arbitrary",)),
        cost_estimate=pl.CostEstimate(flops=6 * t * d * ff, bytes_accessed=6 * d * ff + 8 * t * d, transcendentals=t * ff),
        name="forward",
    )(x, wg, wu, wd)


HALF_STEPS, DA_STEPS, TILES = 4, 2, 4
BLOCK_STEPS, LOW_STEPS = 2 * HALF_STEPS + DA_STEPS, 2 * HALF_STEPS
TURN = BLOCKS * BLOCK_STEPS
STEPS = TURN + DA_STEPS + BLOCKS * LOW_STEPS


def step_of(s):
    low = s - (TURN + DA_STEPS)
    block = jnp.where(s < TURN, s // BLOCK_STEPS, jnp.where(low < 0, BLOCKS, BLOCKS + low // LOW_STEPS))
    place = jnp.where(s < TURN, s % BLOCK_STEPS, jnp.where(low < 0, BLOCK_STEPS + s - TURN, low % LOW_STEPS))
    return block, place


def summed_piece(c):
    full, rest = SUMMED // 3, max(SUMMED % 3, 1)
    late = c - 6 * full
    return tuple(
        jnp.where(late < 0, early, other) for early, other in ((c // 6, full), (c % 6 // 3, late // rest), (c % 3, late % rest))
    )


def place_of(block, half, which):
    full, rest = SUMMED // 3, SUMMED % 3
    return jnp.where(block < full, 6 * block + 3 * half + which, 6 * full + rest * half + which)


def backward_kernel(
    a1_hbm, a0_hbm, h1_hbm, dy_hbm, wg_hbm, wu_hbm, wd_hbm,
    g_hbm, left_hbm, mine_hbm, theirs_hbm,
    ad, pgu, wgb, wub, wdb, wgt, wut, dat, stage, mb, xb, sb, ra, rb, tot, fsb, fra, frb, ftot,
    in_sem, w_sem, own_sem, give_sem, get_sem, left_sem, load_sem, s_sem, ra_sem, rb_sem, tot_sem, down_sem, up_sem, keep_sem, pass_sem, partner_sem,
    fs_sem, fra_sem, frb_sem, ftot_sem, fdown_sem, fup_sem, fkeep_sem, fpass_sem,
):
    me = lax.axis_index("dp")
    z, core = me // 2, me % 2
    partner = me + 1 - 2 * core
    t, d = ad.shape[1:]
    f, fs = wgt.shape[0], stage.shape[1]
    part, r = fs // 2, fs // 2 // UNITS
    units = 2 * SUMMED * UNITS
    coarse = units - FINE
    sub = dat.shape[2]

    def remote(src, dst, send, recv, device):
        return pltpu.make_async_remote_copy(src_ref=src, dst_ref=dst, send_sem=send, recv_sem=recv, device_id={"dp": device}, device_id_type=MESH)

    def weights(block):
        layer, j, slot = 1 - block // BLOCKS, block % BLOCKS, block % 2
        at = pl.ds(pl.multiple_of(j * f, f), f)
        return (
            pltpu.make_async_copy(wg_hbm.at[layer, :, at], wgb.at[slot], w_sem.at[slot, 0]),
            pltpu.make_async_copy(wu_hbm.at[layer, :, at], wub.at[slot], w_sem.at[slot, 1]),
            pltpu.make_async_copy(wd_hbm.at[layer, at, :], wdb.at[slot], w_sem.at[slot, 2]),
        )

    load_dy = pltpu.make_async_copy(dy_hbm, ad.at[0], in_sem.at[0])
    load_a1 = pltpu.make_async_copy(a1_hbm, ad.at[1], in_sem.at[1])
    load_h1 = pltpu.make_async_copy(h1_hbm, ad.at[1], in_sem.at[2])
    load_a0 = pltpu.make_async_copy(a0_hbm, ad.at[1], in_sem.at[3])

    load_a1.start()
    for c in weights(0):
        c.start()
    load_dy.start()
    dat[...] = jnp.zeros_like(dat)

    barrier = pltpu.get_barrier_semaphore()
    pl.semaphore_signal(barrier, inc=1, device_id={"dp": partner}, device_id_type=MESH)

    @pl.when(z > 0)
    def _():
        pl.semaphore_signal(barrier, inc=1, device_id={"dp": me - 2}, device_id_type=MESH)

    @pl.when(z < 3)
    def _():
        pl.semaphore_signal(barrier, inc=1, device_id={"dp": me + 2}, device_id_type=MESH)

    pl.semaphore_wait(barrier, 3 - z // 3 - (3 - z) // 3)

    def at_half(half):
        return pl.ds(pl.multiple_of(half * fs, fs), fs)

    def hidden(block, half):
        slot = block % 2

        @pl.when(half == 0)
        def _():
            @pl.when(block == 0)
            def _():
                load_a1.wait()
                load_dy.wait()

            @pl.when(block == BLOCKS)
            def _():
                load_a0.wait()

            for c in weights(block):
                c.wait()

            @pl.when(block + 1 < 2 * BLOCKS)
            def _():
                for c in weights(block + 1):
                    c.start()

            wgt[...] = wgb[slot].T
            wut[...] = wub[slot].T

        units_at = at_half(half)
        for i in range(TILES):
            at = pl.ds(i * sub, sub)
            gate = dot(wgt[units_at, :], ad[1, at, :], NT)
            up = dot(wut[units_at, :], ad[1, at, :], NT)
            dp = dot(wdb[slot, units_at, :], ad[0, at, :], NT).astype(BF16).astype(F32)
            sig = 0.5 * jnp.tanh(0.5 * gate) + 0.5
            silu = gate * sig
            pgu[0, units_at, at] = (silu * up).astype(BF16)
            pgu[1, units_at, at] = (dp * up * (sig + silu * (1.0 - sig))).astype(BF16)
            pgu[2, units_at, at] = (dp * silu).astype(BF16)

    def gradient(block, half, which):
        rhs = jnp.minimum(which, 1)
        stage[slot_of(half, which)] = dot(pgu[which, at_half(half), :], ad[rhs]).astype(BF16)

    def to_input(block, step):
        slot = block % 2

        @pl.when((block == BLOCKS - 1) & (step == 0))
        def _():
            load_h1.start()

        for i in range(TILES // DA_STEPS):
            tile = step * (TILES // DA_STEPS) + i
            at = pl.ds(pl.multiple_of(tile * sub, sub), sub)
            dat[tile] += dot(wgb[slot], pgu[1, :, at]) + dot(wub[slot], pgu[2, :, at])

    def turn(step):
        @pl.when(step == 0)
        def _():
            load_h1.wait()

        def body(i, _):
            tile = step * (TILES // DA_STEPS) + i
            at = pl.ds(pl.multiple_of(tile * sub, sub), sub)
            da = dat[tile].T.astype(BF16).astype(F32)
            wide = ad[1, at, :].astype(F32)
            scale = scale_of(wide)
            inner = jnp.sum(da * wide, -1, keepdims=True) * (scale * scale * scale) * (1.0 / d)
            through = (da * scale - wide * inner).astype(BF16).astype(F32)
            ad[0, at, :] = (ad[0, at, :].astype(F32) + through).astype(BF16)
            return 0

        lax.fori_loop(0, TILES // DA_STEPS, body, 0)

        @pl.when(step == DA_STEPS - 1)
        def _():
            load_a0.start()

    def slot_of(half, which):
        return (half + which) % 2

    def rows(slot, c):
        return stage.at[slot, pl.ds(pl.multiple_of(c * part, part), part), :]

    def give_copy(slot, c):
        return remote(rows(slot, 1 - core), theirs_hbm.at[c], give_sem.at[slot], get_sem.at[c], partner)

    def own_copy(slot, c):
        return pltpu.make_async_copy(rows(slot, core), mine_hbm.at[c], own_sem.at[slot])

    def left_copy(slot, block, half, which):
        return pltpu.make_async_copy(stage.at[slot], left_hbm.at[3 * block + which - SUMMED, at_half(half), :], left_sem.at[slot])

    def stage_copies(block, half, which, go):
        slot, here = slot_of(half, which), 3 * block + which < SUMMED

        @pl.when(here)
        def _():
            c = place_of(block, half, which)
            if go:
                own_copy(slot, c).start()
                give_copy(slot, c).start()
            else:
                own_copy(slot, c).wait()
                give_copy(slot, c).wait_send()

        @pl.when(jnp.logical_not(here))
        def _():
            copy = left_copy(slot, block, half, which)
            if go:
                copy.start()
            else:
                copy.wait()

    is0, is1, is2, is3 = z == 0, z == 1, z == 2, z == 3
    sum_lag = jnp.where(is1, 2, jnp.where(is2, 1, 0))
    tot_lag = jnp.where(is1, 2, jnp.where(is3, 9, 6))
    free_lag = tot_lag + jnp.where(is3, 2, 3)

    def load_copies(k):
        q, at, slot = k // UNITS, pl.ds(pl.multiple_of((k % UNITS) * r, r), r), k % LOAD_SLOTS
        return (
            pltpu.make_async_copy(mine_hbm.at[q, at, :], mb.at[slot], load_sem.at[slot, 0]),
            pltpu.make_async_copy(theirs_hbm.at[q, at, :], xb.at[slot], load_sem.at[slot, 1]),
        )

    def s_copy_edge(k):
        return remote(sb.at[k % SEND_SLOTS], ra.at[k % SLOTS], s_sem.at[k % SEND_SLOTS], ra_sem.at[k % SLOTS], me + 2 - 4 * (z // 3))

    def s_copy_inner(k):
        return remote(sb.at[k % SEND_SLOTS], rb.at[k % SLOTS], s_sem.at[k % SEND_SLOTS], rb_sem.at[k % SLOTS], me - 2)

    def tot_down(k):
        return remote(tot.at[k % SLOTS], tot.at[k % SLOTS], down_sem.at[k % SLOTS], tot_sem.at[k % SLOTS], me - 2)

    def tot_up(k):
        return remote(tot.at[k % SLOTS], tot.at[k % SLOTS], up_sem.at[k % SLOTS], tot_sem.at[k % SLOTS], me + 2)

    def out_copies(k):
        block, half, which = summed_piece(k // UNITS)
        q, at, slot = 3 * block + which, pl.ds(pl.multiple_of(half * fs + core * part + (k % UNITS) * r, r), r), k % SLOTS
        return (
            pltpu.make_async_copy(tot.at[slot], g_hbm.at[q, at, :], keep_sem.at[slot]),
            remote(tot.at[slot], g_hbm.at[q, at, :], pass_sem.at[slot], partner_sem, partner),
        )

    def inside(k):
        return (k >= 0) & (k < coarse)

    def free(k):
        @pl.when(inside(k))
        def _():
            keep, give = out_copies(k)
            keep.wait()
            give.wait_send()

            @pl.when(is1)
            def _():
                tot_down(k).wait_send()

            @pl.when(is1 | is2)
            def _():
                tot_up(k).wait_send()

    def add(k):
        @pl.when(inside(k))
        def _():
            for c in load_copies(k):
                c.wait()
            slot = k % LOAD_SLOTS
            both = mb[slot].astype(F32) + xb[slot].astype(F32)

            @pl.when((is0 | is3) & (k >= SEND_SLOTS))
            def _():
                s_copy_edge(k - SEND_SLOTS).wait_send()

            @pl.when(is2 & (k >= SEND_SLOTS))
            def _():
                s_copy_inner(k - SEND_SLOTS).wait_send()

            @pl.when(is0 | is3)
            def _():
                sb[k % SEND_SLOTS] = both.astype(BF16)

            @pl.when(is2)
            def _():
                s_copy_edge(k).wait_recv()
                sb[k % SEND_SLOTS] = (both + ra[k % SLOTS].astype(F32)).astype(BF16)

            @pl.when(is1)
            def _():
                s_copy_edge(k).wait_recv()
                s_copy_inner(k).wait_recv()
                tot[k % SLOTS] = (both + ra[k % SLOTS].astype(F32) + rb[k % SLOTS].astype(F32)).astype(BF16)

    def arrive(k):
        @pl.when(inside(k) & (z != 1))
        def _():
            tot_down(k).wait_recv()

    def send(k_sum, k_tot):
        @pl.when(inside(k_sum) & (is0 | is3))
        def _():
            s_copy_edge(k_sum).start()

        @pl.when(inside(k_sum) & is2)
        def _():
            s_copy_inner(k_sum).start()

        @pl.when(inside(k_tot))
        def _():
            @pl.when(is1)
            def _():
                tot_down(k_tot).start()

            @pl.when(is1 | is2)
            def _():
                tot_up(k_tot).start()

            for c in out_copies(k_tot):
                c.start()

    def fine_edge(j):
        return remote(fsb.at[j], fra.at[j], fs_sem.at[j], fra_sem.at[j], me + 2 - 4 * (z // 3))

    def fine_inner(j):
        return remote(fsb.at[j], frb.at[j], fs_sem.at[j], frb_sem.at[j], me - 2)

    def fine_down(j):
        return remote(ftot.at[j], ftot.at[j], fdown_sem.at[j], ftot_sem.at[j], me - 2)

    def fine_up(j):
        return remote(ftot.at[j], ftot.at[j], fup_sem.at[j], ftot_sem.at[j], me + 2)

    def fine_out(j):
        fr = r // PIECES
        k = coarse + j // PIECES
        block, half, which = summed_piece(k // UNITS)
        row = half * fs + core * part + (k % UNITS) * r + (j % PIECES) * fr
        q, at = 3 * block + which, pl.ds(pl.multiple_of(row, fr), fr)
        return (
            pltpu.make_async_copy(ftot.at[j], g_hbm.at[q, at, :], fkeep_sem.at[j]),
            remote(ftot.at[j], g_hbm.at[q, at, :], fpass_sem.at[j], partner_sem, partner),
        )

    def fine_send(j):
        @pl.when(is1)
        def _():
            fine_up(j).start()
            fine_down(j).start()

        @pl.when(is2)
        def _():
            fine_up(j).start()

        for c in fine_out(j):
            c.start()

    def fine_add(k):
        @pl.when((k >= coarse) & (k < units))
        def _():
            for c in load_copies(k):
                c.wait()
            fr, slot = r // PIECES, k % LOAD_SLOTS

            def body(i, _):
                j = (k - coarse) * PIECES + i
                at = pl.ds(pl.multiple_of(i * fr, fr), fr)
                both = mb[slot, at, :].astype(F32) + xb[slot, at, :].astype(F32)

                @pl.when(is0 | is3)
                def _():
                    fsb[j] = both.astype(BF16)
                    fine_edge(j).start()

                @pl.when(is2)
                def _():
                    fine_edge(j).wait_recv()
                    fsb[j] = (both + fra[j].astype(F32)).astype(BF16)
                    fine_inner(j).start()

                @pl.when(is1)
                def _():
                    fine_edge(j).wait_recv()
                    fine_inner(j).wait_recv()
                    ftot[j] = (both + fra[j].astype(F32) + frb[j].astype(F32)).astype(BF16)
                    fine_send(j)

                return 0

            lax.fori_loop(0, PIECES, body, 0)

    def fine_arrive(k):
        @pl.when((k >= coarse) & (k < units) & (z != 1))
        def _():
            def body(i, _):
                j = (k - coarse) * PIECES + i
                fine_down(j).wait_recv()
                fine_send(j)
                return 0

            lax.fori_loop(0, PIECES, body, 0)

    def fine_end():
        def body(j, _):
            keep, give = fine_out(j)
            keep.wait()
            give.wait_send()

            @pl.when(is0 | is3)
            def _():
                fine_edge(j).wait_send()

            @pl.when(is2)
            def _():
                fine_inner(j).wait_send()

            @pl.when(is1)
            def _():
                fine_down(j).wait_send()

            @pl.when(is1 | is2)
            def _():
                fine_up(j).wait_send()

            return 0

        lax.fori_loop(0, FINE * PIECES, body, 0)

    def load(k):
        @pl.when((k >= 0) & (k < units))
        def _():
            @pl.when(k % UNITS == 0)
            def _():
                give_copy(0, k // UNITS).wait_recv()

            for c in load_copies(k):
                c.start()


    def stage_of(s, go):
        @pl.when((s >= 0) & (s < STEPS))
        def _():
            block, place = step_of(s)
            half, kind = place // HALF_STEPS, place % HALF_STEPS

            @pl.when((place < LOW_STEPS) & (kind >= 1))
            def _():
                stage_copies(block, half, kind - 1, go)

    def tick(i, _):
        stage_of(i - 2, False)
        stage_of(i - 1, True)
        now = i - FIRST
        free(now - free_lag)
        add(now - sum_lag)
        arrive(now - tot_lag)
        send(now - sum_lag, now - tot_lag)
        fine_add(now - sum_lag)
        fine_arrive(now - tot_lag)
        load(now - sum_lag + 1)

        @pl.when(i < STEPS)
        def _():
            block, place = step_of(i)
            half, kind = place // HALF_STEPS, place % HALF_STEPS

            @pl.when((place < LOW_STEPS) & (kind == 0))
            def _():
                hidden(block, half)

            @pl.when((place < LOW_STEPS) & (kind >= 1))
            def _():
                gradient(block, half, kind - 1)

            @pl.when((place >= LOW_STEPS) & (place < BLOCK_STEPS))
            def _():
                to_input(block, place - LOW_STEPS)

            @pl.when(place >= BLOCK_STEPS)
            def _():
                turn(place - BLOCK_STEPS)

        return 0

    lax.fori_loop(0, max(FIRST + units + 12, STEPS + 2), tick, 0)

    for k in range(coarse - SEND_SLOTS, coarse):

        @pl.when(is0 | is3)
        def _(k=k):
            s_copy_edge(k).wait_send()

        @pl.when(is2)
        def _(k=k):
            s_copy_inner(k).wait_send()

    fine_end()
    pltpu.make_async_copy(theirs_hbm, theirs_hbm, partner_sem).wait()


def backward(a1, a0, h1, dy, wg, wu, wd):
    t, d = a1.shape
    ff = wg.shape[2]
    f = ff // BLOCKS
    fs = f // 2
    r = fs // 2 // UNITS
    sub = t // TILES
    anywhere = pl.BlockSpec(memory_space=pl.ANY)
    dma = pltpu.SemaphoreType.DMA
    return pl.pallas_call(
        backward_kernel,
        out_shape=[
            jax.ShapeDtypeStruct((SUMMED, f, d), BF16),
            jax.ShapeDtypeStruct((ALL - SUMMED, f, d), BF16),
            jax.ShapeDtypeStruct((2 * SUMMED, fs // 2, d), BF16),
            jax.ShapeDtypeStruct((2 * SUMMED, fs // 2, d), BF16),
        ],
        in_specs=[anywhere] * 7,
        out_specs=[anywhere] * 4,
        scratch_shapes=[
            pltpu.VMEM((2, t, d), BF16),
            pltpu.VMEM((3, f, t), BF16),
            pltpu.VMEM((2, d, f), BF16),
            pltpu.VMEM((2, d, f), BF16),
            pltpu.VMEM((2, f, d), BF16),
            pltpu.VMEM((f, d), BF16),
            pltpu.VMEM((f, d), BF16),
            pltpu.VMEM((TILES, d, sub), F32),
            pltpu.VMEM((2, fs, d), BF16),
            pltpu.VMEM((LOAD_SLOTS, r, d), BF16),
            pltpu.VMEM((LOAD_SLOTS, r, d), BF16),
            pltpu.VMEM((SEND_SLOTS, r, d), BF16),
            pltpu.VMEM((SLOTS, r, d), BF16),
            pltpu.VMEM((SLOTS, r, d), BF16),
            pltpu.VMEM((SLOTS, r, d), BF16),
            *[pltpu.VMEM((FINE * PIECES, r // PIECES, d), BF16)] * 4,
            dma((4,)),
            dma((2, 3)),
            dma((2,)),
            dma((2,)),
            dma((2 * SUMMED,)),
            dma((2,)),
            dma((LOAD_SLOTS, 2)),
            dma((SEND_SLOTS,)),
            dma((SLOTS,)),
            dma((SLOTS,)),
            dma((SLOTS,)),
            dma((SLOTS,)),
            dma((SLOTS,)),
            dma((SLOTS,)),
            dma((SLOTS,)),
            dma,
            *[dma((FINE * PIECES,))] * 8,
        ],
        compiler_params=pltpu.CompilerParams(collective_id=0, has_side_effects=True, vmem_limit_bytes=VMEM_LIMIT),
        cost_estimate=pl.CostEstimate(flops=2 * 15 * t * d * ff, bytes_accessed=100 * d * ff, transcendentals=2 * t * ff),
        name="backward",
    )(a1, a0, h1, dy, wg, wu, wd)


HALVES = ((1, 0), (1, 1), (2, 0), (2, 1), (0, 0), (0, 1))


def adamw_kernel(rounds, first, n_old, *refs):
    arrays = {1: refs[0:3], 2: refs[3:6], 0: refs[6:9]}
    g_hbm = refs[9]
    outs = refs[10 + n_old :][:9]
    outs = {1: outs[0:3], 2: outs[3:6], 0: outs[6:9]}
    wt, mt, vt, gt, wd, md, vd, gd, wt_out, mt_out, vt_out, wd_out, md_out, vd_out, turned, in_sem, out_sem = refs[10 + n_old + 9 :]
    d, f = wt.shape[1] * 2, wt.shape[2]

    def place(b, half):
        which, s = HALVES[half]
        layer, j, q = 1 - b // BLOCKS, b % BLOCKS, 3 * b + which - first
        if which:
            cols = pl.ds(pl.multiple_of(j * f, f), f)
            return which, lambda ref: ref.at[layer, pl.ds(s * (d // 2), d // 2), cols], g_hbm.at[q, :, pl.ds(s * (d // 2), d // 2)]
        rows = pl.ds(pl.multiple_of(j * f + s * (f // 2), f // 2), f // 2)
        return which, lambda ref: ref.at[layer, rows, :], g_hbm.at[q, pl.ds(s * (f // 2), f // 2), :]

    def buffers(half):
        if HALVES[half][0]:
            return [x.at[half] for x in (wt, mt, vt, gt)], [x.at[half] for x in (wt_out, mt_out, vt_out)]
        return [x.at[half - 4] for x in (wd, md, vd, gd)], [x.at[half - 4] for x in (wd_out, md_out, vd_out)]

    def loads(b, half):
        which, at, g = place(b, half)
        sources = [at(x) for x in arrays[which]] + [g]
        return [pltpu.make_async_copy(x, y, in_sem.at[half, i]) for i, (x, y) in enumerate(zip(sources, buffers(half)[0], strict=True))]

    def stores(b, half):
        which, at, _ = place(b, half)
        return [pltpu.make_async_copy(x, at(y), out_sem.at[half, i]) for i, (x, y) in enumerate(zip(buffers(half)[1], outs[which], strict=True))]

    def take(half):
        (w_in, m_in, v_in, g_in), (w_out, m_out, v_out) = buffers(half)
        if HALVES[half][0]:
            turned[...] = g_in[...].T
            g_in = turned

        def body(i, _):
            at = pl.ds(pl.multiple_of(i * 16, 16), 16)
            g = g_in[at, :].astype(F32)
            m = 0.9 * m_in[at, :] + 0.1 * g
            v = 0.95 * v_in[at, :] + 0.05 * g * g
            w = w_in[at, :].astype(F32)
            w_out[at, :] = (w - 0.02 * (m * lax.rsqrt(v + 1e-8) + 0.1 * w)).astype(BF16)
            m_out[at, :] = m
            v_out[at, :] = v
            return 0

        lax.fori_loop(0, w_in.shape[0] // 16, body, 0, unroll=2)

    def start(copies):
        for c in copies:
            c.start()

    def wait(copies):
        for c in copies:
            c.wait()

    starts = {}
    for blocks, halves in rounds:
        for half in halves:
            if half not in starts:
                starts[half] = True
                start(loads(blocks[0], half))
    before = {}
    for n, (blocks, halves) in enumerate(rounds):
        low, high = blocks

        def next_of(half, n=n):
            return next((bs[0] for bs, hs in rounds[n + 1 :] if half in hs), None)

        def one(b, half, low=low, high=high, next_of=next_of):
            wait(loads(b, half))
            if half in before:
                wait(stores(before[half], half))
            elif high - low > 1:

                @pl.when(b > low)
                def _():
                    wait(stores(b - 1, half))

            take(half)
            start(stores(b, half))
            if high - low > 1:

                @pl.when(b + 1 < high)
                def _():
                    start(loads(b + 1, half))

            after = next_of(half)
            if after is not None:
                if high - low > 1:

                    @pl.when(b + 1 == high)
                    def _():
                        start(loads(after, half))

                else:
                    start(loads(after, half))

        def turn(b, _, halves=halves):
            for half in halves:
                one(b, half)
            return 0

        if high - low > 1:
            lax.fori_loop(low, high, turn, 0)
        else:
            turn(low, 0)
        for half in halves:
            before[half] = high - 1
    for half, b in before.items():
        wait(stores(b, half))


def adamw(pieces, first, g, w, m, v, old=()):
    low, high = pieces
    d, ff = w[0].shape[1:]
    f = ff // BLOCKS
    rounds = []
    for b in range(2 * BLOCKS):
        halves = tuple(h for h, (which, _) in enumerate(HALVES) if low <= 3 * b + which < high)
        if not halves:
            continue
        if len(rounds) == 1 and rounds[0][1] == halves:
            rounds[-1] = ((rounds[-1][0][0], b + 1), halves)
        else:
            rounds.append(((b, b + 1), halves))
    anywhere = pl.BlockSpec(memory_space=pl.ANY)
    operands = [x for i in range(3) for x in (w[i], m[i], v[i])]
    n = (high - low) * d * f
    return pl.pallas_call(
        functools.partial(adamw_kernel, tuple(rounds), first, len(old)),
        out_shape=[jax.ShapeDtypeStruct(x.shape, x.dtype) for x in operands],
        in_specs=[anywhere] * (10 + len(old)),
        out_specs=[anywhere] * 9,
        scratch_shapes=[
            pltpu.VMEM((4, d // 2, f), BF16),
            pltpu.VMEM((4, d // 2, f), F32),
            pltpu.VMEM((4, d // 2, f), F32),
            pltpu.VMEM((4, f, d // 2), BF16),
            pltpu.VMEM((2, f // 2, d), BF16),
            pltpu.VMEM((2, f // 2, d), F32),
            pltpu.VMEM((2, f // 2, d), F32),
            pltpu.VMEM((2, f // 2, d), BF16),
            pltpu.VMEM((4, d // 2, f), BF16),
            pltpu.VMEM((4, d // 2, f), F32),
            pltpu.VMEM((4, d // 2, f), F32),
            pltpu.VMEM((2, f // 2, d), BF16),
            pltpu.VMEM((2, f // 2, d), F32),
            pltpu.VMEM((2, f // 2, d), F32),
            pltpu.VMEM((d // 2, f), BF16),
            pltpu.SemaphoreType.DMA((6, 4)),
            pltpu.SemaphoreType.DMA((6, 3)),
        ],
        input_output_aliases={10 + i: i for i in range(len(old))},
        compiler_params=pltpu.CompilerParams(vmem_limit_bytes=VMEM_LIMIT),
        cost_estimate=pl.CostEstimate(flops=2000 * n, bytes_accessed=22 * n, transcendentals=n),
        name="adamw",
    )(*operands, g, *old)


def solution(mesh):
    def step(x, dy, *arrays):
        w, m, v = (arrays[i : i + 3] for i in (0, 3, 6))
        wg, wu, wd = w
        a0, h1, a1 = forward(x[0], wg, wu, wd)
        g, left, _, _ = backward(a1, a0, h1, dy[0], wg, wu, wd)
        left = lax.psum(left, "dp")
        done = adamw((0, SUMMED), 0, g, w, m, v)
        done = adamw((SUMMED, ALL), SUMMED, left, w, m, v, done)
        return tuple(done[3 * i + kind] for kind in range(3) for i in range(3))

    return jax.shard_map(
        step,
        mesh=mesh,
        in_specs=(P(("rep", "dp"), None, None),) * 2 + (P(None, None, None),) * 9,
        out_specs=(P("rep", None, None),) * 9,
        check_vma=False,
    )
```

```python
import functools

import jax
import jax.numpy as jnp
from jax import lax
from jax.experimental import pallas as pl
from jax.experimental.pallas import tpu as pltpu
from jax.sharding import PartitionSpec as P

BF16, F32 = jnp.bfloat16, jnp.float32
MESH = pl.DeviceIdType.MESH
VMEM_LIMIT = 66_000_000
BLOCKS = 5
ALL = 6 * BLOCKS
SUMMED = 26
UNITS = 2
FINE, PIECES = 2, 5
FIRST = 5
SLOTS, SEND_SLOTS, LOAD_SLOTS = 12, 6, 4
NN = (((1,), (0,)), ((), ()))
NT = (((1,), (1,)), ((), ()))


def dot(a, b, dims=NN):
    return lax.dot_general(a, b, dims, preferred_element_type=F32)


def scale_of(wide):
    return lax.rsqrt(jnp.mean(wide * wide, -1, keepdims=True) + 1e-6)


def cuts(n, width):
    starts = list(range(0, n - width + 1, width))
    return [(s, (starts[i + 1] if i + 1 < len(starts) else n) - s) for i, s in enumerate(starts)]


def forward_kernel(width, x_ref, wg_hbm, wu_hbm, wd_hbm, a0_ref, h1_ref, a1_ref, wg, wu, wd, p, sems):
    first = pl.program_id(0) == 0
    pieces = cuts(wg.shape[1], width)

    def loads(i):
        s, n = pieces[i]
        return (
            pltpu.make_async_copy(wg_hbm.at[0, :, pl.ds(s, n)], wg.at[:, pl.ds(s, n)], sems.at[0, i]),
            pltpu.make_async_copy(wu_hbm.at[0, :, pl.ds(s, n)], wu.at[:, pl.ds(s, n)], sems.at[1, i]),
            pltpu.make_async_copy(wd_hbm.at[0, pl.ds(s, n), :], wd.at[pl.ds(s, n), :], sems.at[2, i]),
        )

    @pl.when(first)
    def _():
        for i in range(len(pieces)):
            for c in loads(i)[:2]:
                c.start()
        for i in range(len(pieces)):
            loads(i)[2].start()

    wide = x_ref[...].astype(F32)
    a = (wide * scale_of(wide)).astype(BF16)
    a0_ref[...] = a
    for i, (s, n) in enumerate(pieces):

        @pl.when(first)
        def _(i=i):
            for c in loads(i)[:2]:
                c.wait()

        gate = dot(a, wg[:, s : s + n])
        up = dot(a, wu[:, s : s + n])
        p[:, s : s + n] = (gate * (0.5 * jnp.tanh(0.5 * gate) + 0.5) * up).astype(BF16)

    @pl.when(first)
    def _():
        for i in range(len(pieces)):
            loads(i)[2].wait()

    h1 = (wide + dot(p[...], wd[...]).astype(BF16).astype(F32)).astype(BF16)
    h1_ref[...] = h1
    wide1 = h1.astype(F32)
    a1_ref[...] = (wide1 * scale_of(wide1)).astype(BF16)


def forward(x, wg, wu, wd):
    t, d = x.shape
    ff = wg.shape[2]
    tile = min(t, 1024)
    width = min(ff, 768)
    rows = pl.BlockSpec((tile, d), lambda i: (i, 0))
    anywhere = pl.BlockSpec(memory_space=pl.ANY)
    return pl.pallas_call(
        functools.partial(forward_kernel, width),
        grid=(t // tile,),
        out_shape=[jax.ShapeDtypeStruct((t, d), BF16)] * 3,
        in_specs=[rows, anywhere, anywhere, anywhere],
        out_specs=[rows] * 3,
        scratch_shapes=[
            pltpu.VMEM((d, ff), BF16),
            pltpu.VMEM((d, ff), BF16),
            pltpu.VMEM((ff, d), BF16),
            pltpu.VMEM((tile, ff), BF16),
            pltpu.SemaphoreType.DMA((3, len(cuts(ff, width)))),
        ],
        compiler_params=pltpu.CompilerParams(vmem_limit_bytes=VMEM_LIMIT, dimension_semantics=("arbitrary",)),
        cost_estimate=pl.CostEstimate(flops=6 * t * d * ff, bytes_accessed=6 * d * ff + 8 * t * d, transcendentals=t * ff),
        name="forward",
    )(x, wg, wu, wd)


HALF_STEPS, DA_STEPS, TILES = 4, 2, 4
BLOCK_STEPS, LOW_STEPS = 2 * HALF_STEPS + DA_STEPS, 2 * HALF_STEPS
TURN = BLOCKS * BLOCK_STEPS
STEPS = 1 + TURN + DA_STEPS + BLOCKS * LOW_STEPS


def step_of(s):
    p = jnp.where(s <= 3, s, s - 1)
    low = p - (TURN + DA_STEPS)
    block = jnp.where(p < TURN, p // BLOCK_STEPS, jnp.where(low < 0, BLOCKS, BLOCKS + low // LOW_STEPS))
    place = jnp.where(p < TURN, p % BLOCK_STEPS, jnp.where(low < 0, BLOCK_STEPS + p - TURN, low % LOW_STEPS))
    half = jnp.where(place < LOW_STEPS, place // HALF_STEPS, 0)
    kind = jnp.where(place < LOW_STEPS, place % HALF_STEPS, place - 2)
    return block, half, jnp.where(s == 3, 4, jnp.where(s == 4, 5, kind))


def made_in(kind):
    low = jnp.where((kind == 3) | (kind == 4), 1, jnp.where(kind == 5, 2, 0))
    high = jnp.where((kind == 3) | (kind == 5), 3, jnp.where(kind == 4, 2, jnp.where(kind == 2, 1, 0)))
    return low, high


def summed_piece(c):
    full, rest = SUMMED // 3, max(SUMMED % 3, 1)
    late = c - 6 * full
    return tuple(
        jnp.where(late < 0, early, other) for early, other in ((c // 6, full), (c % 6 // 3, late // rest), (c % 3, late % rest))
    )


def place_of(block, half, which):
    full, rest = SUMMED // 3, SUMMED % 3
    return jnp.where(block < full, 6 * block + 3 * half + which, 6 * full + rest * half + which)


def backward_kernel(
    a1_hbm, a0_hbm, h1_hbm, dy_hbm, wg_hbm, wu_hbm, wd_hbm,
    g_hbm, left_hbm, mine_hbm, theirs_hbm,
    ad, pgu, wgb, wub, wdb, wgt, wut, dat, stage, mb, xb, sb, ra, rb, tot, fsb, fra, frb, ftot,
    in_sem, w_sem, own_sem, give_sem, get_sem, left_sem, load_sem, s_sem, ra_sem, rb_sem, tot_sem, down_sem, up_sem, keep_sem, pass_sem, partner_sem,
    fs_sem, fra_sem, frb_sem, ftot_sem, fdown_sem, fup_sem, fkeep_sem, fpass_sem,
):
    me = lax.axis_index("dp")
    z, core = me // 2, me % 2
    partner = me + 1 - 2 * core
    t, d = ad.shape[1:]
    f, fs = wgt.shape[0], stage.shape[1]
    part, r = fs // 2, fs // 2 // UNITS
    units = 2 * SUMMED * UNITS
    coarse = units - FINE
    sub = dat.shape[2]

    def remote(src, dst, send, recv, device):
        return pltpu.make_async_remote_copy(src_ref=src, dst_ref=dst, send_sem=send, recv_sem=recv, device_id={"dp": device}, device_id_type=MESH)

    def weights(block):
        layer, j, slot = 1 - block // BLOCKS, block % BLOCKS, block % 2
        at = pl.ds(pl.multiple_of(j * f, f), f)
        return (
            pltpu.make_async_copy(wg_hbm.at[layer, :, at], wgb.at[slot], w_sem.at[slot, 0]),
            pltpu.make_async_copy(wu_hbm.at[layer, :, at], wub.at[slot], w_sem.at[slot, 1]),
            pltpu.make_async_copy(wd_hbm.at[layer, at, :], wdb.at[slot], w_sem.at[slot, 2]),
        )

    load_dy = pltpu.make_async_copy(dy_hbm, ad.at[0], in_sem.at[0])
    load_a1 = pltpu.make_async_copy(a1_hbm, ad.at[1], in_sem.at[1])
    load_h1 = pltpu.make_async_copy(h1_hbm, ad.at[1], in_sem.at[2])
    load_a0 = pltpu.make_async_copy(a0_hbm, ad.at[1], in_sem.at[3])

    load_a1.start()
    for c in weights(0):
        c.start()
    load_dy.start()
    dat[...] = jnp.zeros_like(dat)

    barrier = pltpu.get_barrier_semaphore()
    pl.semaphore_signal(barrier, inc=1, device_id={"dp": partner}, device_id_type=MESH)

    @pl.when(z > 0)
    def _():
        pl.semaphore_signal(barrier, inc=1, device_id={"dp": me - 2}, device_id_type=MESH)

    @pl.when(z < 3)
    def _():
        pl.semaphore_signal(barrier, inc=1, device_id={"dp": me + 2}, device_id_type=MESH)

    pl.semaphore_wait(barrier, 3 - z // 3 - (3 - z) // 3)

    def at_half(half):
        return pl.ds(pl.multiple_of(half * fs, fs), fs)

    def hidden(block, half, tokens):
        slot = block % 2

        @pl.when((half == 0) & (tokens == 0))
        def _():
            @pl.when(block == 0)
            def _():
                load_a1.wait()
                load_dy.wait()

            @pl.when(block == BLOCKS)
            def _():
                load_a0.wait()

            for c in weights(block):
                c.wait()

            @pl.when(block + 1 < 2 * BLOCKS)
            def _():
                for c in weights(block + 1):
                    c.start()

            wgt[...] = wgb[slot].T
            wut[...] = wub[slot].T

        units_at = at_half(half)
        for i in range(TILES // 2):
            at = pl.ds(pl.multiple_of((tokens * (TILES // 2) + i) * sub, sub), sub)
            gate = dot(wgt[units_at, :], ad[1, at, :], NT)
            up = dot(wut[units_at, :], ad[1, at, :], NT)
            dp = dot(wdb[slot, units_at, :], ad[0, at, :], NT).astype(BF16).astype(F32)
            sig = 0.5 * jnp.tanh(0.5 * gate) + 0.5
            silu = gate * sig
            pgu[0, units_at, at] = (silu * up).astype(BF16)
            pgu[1, units_at, at] = (dp * up * (sig + silu * (1.0 - sig))).astype(BF16)
            pgu[2, units_at, at] = (dp * silu).astype(BF16)

    def gradients(half, kind):
        def body(which, _):
            stage[which] = dot(pgu[which, at_half(half), :], ad[jnp.minimum(which, 1)]).astype(BF16)
            return 0

        lax.fori_loop(*made_in(kind), body, 0)

    def to_input(block, step):
        slot = block % 2

        @pl.when((block == BLOCKS - 1) & (step == 0))
        def _():
            load_h1.start()

        for i in range(TILES // DA_STEPS):
            tile = step * (TILES // DA_STEPS) + i
            at = pl.ds(pl.multiple_of(tile * sub, sub), sub)
            dat[tile] += dot(wgb[slot], pgu[1, :, at]) + dot(wub[slot], pgu[2, :, at])

    def turn(step):
        @pl.when(step == 0)
        def _():
            load_h1.wait()

        def body(i, _):
            tile = step * (TILES // DA_STEPS) + i
            at = pl.ds(pl.multiple_of(tile * sub, sub), sub)
            da = dat[tile].T.astype(BF16).astype(F32)
            wide = ad[1, at, :].astype(F32)
            scale = scale_of(wide)
            inner = jnp.sum(da * wide, -1, keepdims=True) * (scale * scale * scale) * (1.0 / d)
            through = (da * scale - wide * inner).astype(BF16).astype(F32)
            ad[0, at, :] = (ad[0, at, :].astype(F32) + through).astype(BF16)
            return 0

        lax.fori_loop(0, TILES // DA_STEPS, body, 0)

        @pl.when(step == DA_STEPS - 1)
        def _():
            load_a0.start()

    def rows(slot, c):
        return stage.at[slot, pl.ds(pl.multiple_of(c * part, part), part), :]

    def give_copy(slot, c):
        return remote(rows(slot, 1 - core), theirs_hbm.at[c], give_sem.at[slot], get_sem.at[c], partner)

    def own_copy(slot, c):
        return pltpu.make_async_copy(rows(slot, core), mine_hbm.at[c], own_sem.at[slot])

    def left_copy(slot, block, half, which):
        return pltpu.make_async_copy(stage.at[slot], left_hbm.at[3 * block + which - SUMMED, at_half(half), :], left_sem.at[slot])

    def stage_copies(block, half, which, go):
        slot, here = which, 3 * block + which < SUMMED

        @pl.when(here)
        def _():
            c = place_of(block, half, which)
            if go:
                own_copy(slot, c).start()
                give_copy(slot, c).start()
            else:
                own_copy(slot, c).wait()
                give_copy(slot, c).wait_send()

        @pl.when(jnp.logical_not(here))
        def _():
            copy = left_copy(slot, block, half, which)
            if go:
                copy.start()
            else:
                copy.wait()

    is0, is1, is2, is3 = z == 0, z == 1, z == 2, z == 3
    sum_lag = jnp.where(is1, 2, jnp.where(is2, 1, 0))
    tot_lag = jnp.where(is1, 2, jnp.where(is3, 9, jnp.where(is2, 5, 6)))
    free_lag = tot_lag + jnp.where(is3, 2, 3)

    def load_copies(k):
        q, at, slot = k // UNITS, pl.ds(pl.multiple_of((k % UNITS) * r, r), r), k % LOAD_SLOTS
        return (
            pltpu.make_async_copy(mine_hbm.at[q, at, :], mb.at[slot], load_sem.at[slot, 0]),
            pltpu.make_async_copy(theirs_hbm.at[q, at, :], xb.at[slot], load_sem.at[slot, 1]),
        )

    def s_copy_edge(k):
        return remote(sb.at[k % SEND_SLOTS], ra.at[k % SLOTS], s_sem.at[k % SEND_SLOTS], ra_sem.at[k % SLOTS], me + 2 - 4 * (z // 3))

    def s_copy_inner(k):
        return remote(sb.at[k % SEND_SLOTS], rb.at[k % SLOTS], s_sem.at[k % SEND_SLOTS], rb_sem.at[k % SLOTS], me - 2)

    def tot_down(k):
        return remote(tot.at[k % SLOTS], tot.at[k % SLOTS], down_sem.at[k % SLOTS], tot_sem.at[k % SLOTS], me - 2)

    def tot_up(k):
        return remote(tot.at[k % SLOTS], tot.at[k % SLOTS], up_sem.at[k % SLOTS], tot_sem.at[k % SLOTS], me + 2)

    def out_copies(k):
        block, half, which = summed_piece(k // UNITS)
        q, at, slot = 3 * block + which, pl.ds(pl.multiple_of(half * fs + core * part + (k % UNITS) * r, r), r), k % SLOTS
        return (
            pltpu.make_async_copy(tot.at[slot], g_hbm.at[q, at, :], keep_sem.at[slot]),
            remote(tot.at[slot], g_hbm.at[q, at, :], pass_sem.at[slot], partner_sem, partner),
        )

    def inside(k):
        return (k >= 0) & (k < coarse)

    def free(k):
        @pl.when(inside(k))
        def _():
            keep, give = out_copies(k)
            keep.wait()
            give.wait_send()

            @pl.when(is1)
            def _():
                tot_down(k).wait_send()

            @pl.when(is1 | is2)
            def _():
                tot_up(k).wait_send()

    def add(k):
        @pl.when(inside(k))
        def _():
            for c in load_copies(k):
                c.wait()
            slot = k % LOAD_SLOTS
            both = mb[slot].astype(F32) + xb[slot].astype(F32)

            @pl.when((is0 | is3) & (k >= SEND_SLOTS))
            def _():
                s_copy_edge(k - SEND_SLOTS).wait_send()

            @pl.when(is2 & (k >= SEND_SLOTS))
            def _():
                s_copy_inner(k - SEND_SLOTS).wait_send()

            @pl.when(is0 | is3)
            def _():
                sb[k % SEND_SLOTS] = both.astype(BF16)

            @pl.when(is2)
            def _():
                s_copy_edge(k).wait_recv()
                sb[k % SEND_SLOTS] = (both + ra[k % SLOTS].astype(F32)).astype(BF16)

            @pl.when(is1)
            def _():
                s_copy_edge(k).wait_recv()
                s_copy_inner(k).wait_recv()
                tot[k % SLOTS] = (both + ra[k % SLOTS].astype(F32) + rb[k % SLOTS].astype(F32)).astype(BF16)

    def arrive(k):
        @pl.when(inside(k) & (z != 1))
        def _():
            tot_down(k).wait_recv()

    def send(k_sum, k_tot):
        @pl.when(inside(k_sum) & (is0 | is3))
        def _():
            s_copy_edge(k_sum).start()

        @pl.when(inside(k_sum) & is2)
        def _():
            s_copy_inner(k_sum).start()

        @pl.when(inside(k_tot))
        def _():
            @pl.when(is1)
            def _():
                tot_down(k_tot).start()

            @pl.when(is1 | is2)
            def _():
                tot_up(k_tot).start()

            for c in out_copies(k_tot):
                c.start()

    def fine_edge(j):
        return remote(fsb.at[j], fra.at[j], fs_sem.at[j], fra_sem.at[j], me + 2 - 4 * (z // 3))

    def fine_inner(j):
        return remote(fsb.at[j], frb.at[j], fs_sem.at[j], frb_sem.at[j], me - 2)

    def fine_down(j):
        return remote(ftot.at[j], ftot.at[j], fdown_sem.at[j], ftot_sem.at[j], me - 2)

    def fine_up(j):
        return remote(ftot.at[j], ftot.at[j], fup_sem.at[j], ftot_sem.at[j], me + 2)

    def fine_out(j):
        fr = r // PIECES
        k = coarse + j // PIECES
        block, half, which = summed_piece(k // UNITS)
        row = half * fs + core * part + (k % UNITS) * r + (j % PIECES) * fr
        q, at = 3 * block + which, pl.ds(pl.multiple_of(row, fr), fr)
        return (
            pltpu.make_async_copy(ftot.at[j], g_hbm.at[q, at, :], fkeep_sem.at[j]),
            remote(ftot.at[j], g_hbm.at[q, at, :], fpass_sem.at[j], partner_sem, partner),
        )

    def fine_send(j):
        @pl.when(is1)
        def _():
            fine_up(j).start()
            fine_down(j).start()

        @pl.when(is2)
        def _():
            fine_up(j).start()

        for c in fine_out(j):
            c.start()

    def fine_add(k):
        @pl.when((k >= coarse) & (k < units))
        def _():
            for c in load_copies(k):
                c.wait()
            fr, slot = r // PIECES, k % LOAD_SLOTS

            def body(i, _):
                j = (k - coarse) * PIECES + i
                at = pl.ds(pl.multiple_of(i * fr, fr), fr)
                both = mb[slot, at, :].astype(F32) + xb[slot, at, :].astype(F32)

                @pl.when(is0 | is3)
                def _():
                    fsb[j] = both.astype(BF16)
                    fine_edge(j).start()

                @pl.when(is2)
                def _():
                    fine_edge(j).wait_recv()
                    fsb[j] = (both + fra[j].astype(F32)).astype(BF16)
                    fine_inner(j).start()

                @pl.when(is1)
                def _():
                    fine_edge(j).wait_recv()
                    fine_inner(j).wait_recv()
                    ftot[j] = (both + fra[j].astype(F32) + frb[j].astype(F32)).astype(BF16)
                    fine_send(j)

                return 0

            lax.fori_loop(0, PIECES, body, 0)

    def fine_arrive(k):
        @pl.when((k >= coarse) & (k < units) & (z != 1))
        def _():
            def body(i, _):
                j = (k - coarse) * PIECES + i
                fine_down(j).wait_recv()
                fine_send(j)
                return 0

            lax.fori_loop(0, PIECES, body, 0)

    def fine_end():
        def body(j, _):
            keep, give = fine_out(j)
            keep.wait()
            give.wait_send()

            @pl.when(is0 | is3)
            def _():
                fine_edge(j).wait_send()

            @pl.when(is2)
            def _():
                fine_inner(j).wait_send()

            @pl.when(is1)
            def _():
                fine_down(j).wait_send()

            @pl.when(is1 | is2)
            def _():
                fine_up(j).wait_send()

            return 0

        lax.fori_loop(0, FINE * PIECES, body, 0)

    def load(k):
        @pl.when((k >= 0) & (k < units))
        def _():
            @pl.when(k % UNITS == 0)
            def _():
                give_copy(0, k // UNITS).wait_recv()

            for c in load_copies(k):
                c.start()


    def stage_of(s, go):
        @pl.when((s >= 0) & (s < STEPS))
        def _():
            block, half, kind = step_of(s)

            def body(which, _):
                stage_copies(block, half, which, go)
                return 0

            lax.fori_loop(*made_in(kind), body, 0)

    def tick(i, _):
        stage_of(i - 2, False)
        stage_of(i - 1, True)
        now = i - FIRST
        free(now - free_lag)
        add(now - sum_lag)
        arrive(now - tot_lag)
        send(now - sum_lag, now - tot_lag)
        fine_add(now - sum_lag)
        fine_arrive(now - tot_lag)
        load(now - sum_lag + 1)

        @pl.when(i < STEPS)
        def _():
            block, half, kind = step_of(i)

            @pl.when(kind < 2)
            def _():
                hidden(block, half, kind)

            @pl.when((kind >= 2) & (kind <= 5))
            def _():
                gradients(half, kind)

            @pl.when((kind == 6) | (kind == 7))
            def _():
                to_input(block, kind - 6)

            @pl.when(kind >= 8)
            def _():
                turn(kind - 8)

        return 0

    lax.fori_loop(0, max(FIRST + units + 12, STEPS + 2), tick, 0)

    for k in range(coarse - SEND_SLOTS, coarse):

        @pl.when(is0 | is3)
        def _(k=k):
            s_copy_edge(k).wait_send()

        @pl.when(is2)
        def _(k=k):
            s_copy_inner(k).wait_send()

    fine_end()
    pltpu.make_async_copy(theirs_hbm, theirs_hbm, partner_sem).wait()


def backward(a1, a0, h1, dy, wg, wu, wd):
    t, d = a1.shape
    ff = wg.shape[2]
    f = ff // BLOCKS
    fs = f // 2
    r = fs // 2 // UNITS
    sub = t // TILES
    anywhere = pl.BlockSpec(memory_space=pl.ANY)
    dma = pltpu.SemaphoreType.DMA
    return pl.pallas_call(
        backward_kernel,
        out_shape=[
            jax.ShapeDtypeStruct((SUMMED, f, d), BF16),
            jax.ShapeDtypeStruct((ALL - SUMMED, f, d), BF16),
            jax.ShapeDtypeStruct((2 * SUMMED, fs // 2, d), BF16),
            jax.ShapeDtypeStruct((2 * SUMMED, fs // 2, d), BF16),
        ],
        in_specs=[anywhere] * 7,
        out_specs=[anywhere] * 4,
        scratch_shapes=[
            pltpu.VMEM((2, t, d), BF16),
            pltpu.VMEM((3, f, t), BF16),
            pltpu.VMEM((2, d, f), BF16),
            pltpu.VMEM((2, d, f), BF16),
            pltpu.VMEM((2, f, d), BF16),
            pltpu.VMEM((f, d), BF16),
            pltpu.VMEM((f, d), BF16),
            pltpu.VMEM((TILES, d, sub), F32),
            pltpu.VMEM((3, fs, d), BF16),
            pltpu.VMEM((LOAD_SLOTS, r, d), BF16),
            pltpu.VMEM((LOAD_SLOTS, r, d), BF16),
            pltpu.VMEM((SEND_SLOTS, r, d), BF16),
            pltpu.VMEM((SLOTS, r, d), BF16),
            pltpu.VMEM((SLOTS, r, d), BF16),
            pltpu.VMEM((SLOTS, r, d), BF16),
            *[pltpu.VMEM((FINE * PIECES, r // PIECES, d), BF16)] * 4,
            dma((4,)),
            dma((2, 3)),
            dma((3,)),
            dma((3,)),
            dma((2 * SUMMED,)),
            dma((3,)),
            dma((LOAD_SLOTS, 2)),
            dma((SEND_SLOTS,)),
            dma((SLOTS,)),
            dma((SLOTS,)),
            dma((SLOTS,)),
            dma((SLOTS,)),
            dma((SLOTS,)),
            dma((SLOTS,)),
            dma((SLOTS,)),
            dma,
            *[dma((FINE * PIECES,))] * 8,
        ],
        compiler_params=pltpu.CompilerParams(collective_id=0, has_side_effects=True, vmem_limit_bytes=VMEM_LIMIT),
        cost_estimate=pl.CostEstimate(flops=2 * 15 * t * d * ff, bytes_accessed=100 * d * ff, transcendentals=2 * t * ff),
        name="backward",
    )(a1, a0, h1, dy, wg, wu, wd)


HALVES = ((1, 0), (1, 1), (2, 0), (2, 1), (0, 0), (0, 1))


def adamw_kernel(rounds, first, n_old, *refs):
    arrays = {1: refs[0:3], 2: refs[3:6], 0: refs[6:9]}
    g_hbm = refs[9]
    outs = refs[10 + n_old :][:9]
    outs = {1: outs[0:3], 2: outs[3:6], 0: outs[6:9]}
    wt, mt, vt, gt, wd, md, vd, gd, wt_out, mt_out, vt_out, wd_out, md_out, vd_out, turned, in_sem, out_sem = refs[10 + n_old + 9 :]
    d, f = wt.shape[1] * 2, wt.shape[2]

    def place(b, half):
        which, s = HALVES[half]
        layer, j, q = 1 - b // BLOCKS, b % BLOCKS, 3 * b + which - first
        if which:
            cols = pl.ds(pl.multiple_of(j * f, f), f)
            return which, lambda ref: ref.at[layer, pl.ds(s * (d // 2), d // 2), cols], g_hbm.at[q, :, pl.ds(s * (d // 2), d // 2)]
        rows = pl.ds(pl.multiple_of(j * f + s * (f // 2), f // 2), f // 2)
        return which, lambda ref: ref.at[layer, rows, :], g_hbm.at[q, pl.ds(s * (f // 2), f // 2), :]

    def buffers(half):
        if HALVES[half][0]:
            return [x.at[half] for x in (wt, mt, vt, gt)], [x.at[half] for x in (wt_out, mt_out, vt_out)]
        return [x.at[half - 4] for x in (wd, md, vd, gd)], [x.at[half - 4] for x in (wd_out, md_out, vd_out)]

    def loads(b, half):
        which, at, g = place(b, half)
        sources = [at(x) for x in arrays[which]] + [g]
        return [pltpu.make_async_copy(x, y, in_sem.at[half, i]) for i, (x, y) in enumerate(zip(sources, buffers(half)[0], strict=True))]

    def stores(b, half):
        which, at, _ = place(b, half)
        return [pltpu.make_async_copy(x, at(y), out_sem.at[half, i]) for i, (x, y) in enumerate(zip(buffers(half)[1], outs[which], strict=True))]

    def take(half):
        (w_in, m_in, v_in, g_in), (w_out, m_out, v_out) = buffers(half)
        if HALVES[half][0]:
            turned[...] = g_in[...].T
            g_in = turned

        def body(i, _):
            at = pl.ds(pl.multiple_of(i * 16, 16), 16)
            g = g_in[at, :].astype(F32)
            m = 0.9 * m_in[at, :] + 0.1 * g
            v = 0.95 * v_in[at, :] + 0.05 * g * g
            w = w_in[at, :].astype(F32)
            w_out[at, :] = (w - 0.02 * (m * lax.rsqrt(v + 1e-8) + 0.1 * w)).astype(BF16)
            m_out[at, :] = m
            v_out[at, :] = v
            return 0

        lax.fori_loop(0, w_in.shape[0] // 16, body, 0, unroll=2)

    def start(copies):
        for c in copies:
            c.start()

    def wait(copies):
        for c in copies:
            c.wait()

    starts = {}
    for blocks, halves in rounds:
        for half in halves:
            if half not in starts:
                starts[half] = True
                start(loads(blocks[0], half))
    before = {}
    for n, (blocks, halves) in enumerate(rounds):
        low, high = blocks

        def next_of(half, n=n):
            return next((bs[0] for bs, hs in rounds[n + 1 :] if half in hs), None)

        def one(b, half, low=low, high=high, next_of=next_of):
            wait(loads(b, half))
            if half in before:
                wait(stores(before[half], half))
            elif high - low > 1:

                @pl.when(b > low)
                def _():
                    wait(stores(b - 1, half))

            take(half)
            start(stores(b, half))
            if high - low > 1:

                @pl.when(b + 1 < high)
                def _():
                    start(loads(b + 1, half))

            after = next_of(half)
            if after is not None:
                if high - low > 1:

                    @pl.when(b + 1 == high)
                    def _():
                        start(loads(after, half))

                else:
                    start(loads(after, half))

        def turn(b, _, halves=halves):
            for half in halves:
                one(b, half)
            return 0

        if high - low > 1:
            lax.fori_loop(low, high, turn, 0)
        else:
            turn(low, 0)
        for half in halves:
            before[half] = high - 1
    for half, b in before.items():
        wait(stores(b, half))


def adamw(pieces, first, g, w, m, v, old=()):
    low, high = pieces
    d, ff = w[0].shape[1:]
    f = ff // BLOCKS
    rounds = []
    for b in range(2 * BLOCKS):
        halves = tuple(h for h, (which, _) in enumerate(HALVES) if low <= 3 * b + which < high)
        if not halves:
            continue
        if len(rounds) == 1 and rounds[0][1] == halves:
            rounds[-1] = ((rounds[-1][0][0], b + 1), halves)
        else:
            rounds.append(((b, b + 1), halves))
    anywhere = pl.BlockSpec(memory_space=pl.ANY)
    operands = [x for i in range(3) for x in (w[i], m[i], v[i])]
    n = (high - low) * d * f
    return pl.pallas_call(
        functools.partial(adamw_kernel, tuple(rounds), first, len(old)),
        out_shape=[jax.ShapeDtypeStruct(x.shape, x.dtype) for x in operands],
        in_specs=[anywhere] * (10 + len(old)),
        out_specs=[anywhere] * 9,
        scratch_shapes=[
            pltpu.VMEM((4, d // 2, f), BF16),
            pltpu.VMEM((4, d // 2, f), F32),
            pltpu.VMEM((4, d // 2, f), F32),
            pltpu.VMEM((4, f, d // 2), BF16),
            pltpu.VMEM((2, f // 2, d), BF16),
            pltpu.VMEM((2, f // 2, d), F32),
            pltpu.VMEM((2, f // 2, d), F32),
            pltpu.VMEM((2, f // 2, d), BF16),
            pltpu.VMEM((4, d // 2, f), BF16),
            pltpu.VMEM((4, d // 2, f), F32),
            pltpu.VMEM((4, d // 2, f), F32),
            pltpu.VMEM((2, f // 2, d), BF16),
            pltpu.VMEM((2, f // 2, d), F32),
            pltpu.VMEM((2, f // 2, d), F32),
            pltpu.VMEM((d // 2, f), BF16),
            pltpu.SemaphoreType.DMA((6, 4)),
            pltpu.SemaphoreType.DMA((6, 3)),
        ],
        input_output_aliases={10 + i: i for i in range(len(old))},
        compiler_params=pltpu.CompilerParams(vmem_limit_bytes=VMEM_LIMIT),
        cost_estimate=pl.CostEstimate(flops=2000 * n, bytes_accessed=22 * n, transcendentals=n),
        name="adamw",
    )(*operands, g, *old)


def solution(mesh):
    def step(x, dy, *arrays):
        w, m, v = (arrays[i : i + 3] for i in (0, 3, 6))
        wg, wu, wd = w
        a0, h1, a1 = forward(x[0], wg, wu, wd)
        g, left, _, _ = backward(a1, a0, h1, dy[0], wg, wu, wd)
        left = lax.psum(left, "dp")
        done = adamw((0, SUMMED), 0, g, w, m, v)
        done = adamw((SUMMED, ALL), SUMMED, left, w, m, v, done)
        return tuple(done[3 * i + kind] for kind in range(3) for i in range(3))

    return jax.shard_map(
        step,
        mesh=mesh,
        in_specs=(P(("rep", "dp"), None, None),) * 2 + (P(None, None, None),) * 9,
        out_specs=(P("rep", None, None),) * 9,
        check_vma=False,
    )
```

```python
import functools

import jax
import jax.numpy as jnp
from jax import lax
from jax.experimental import pallas as pl
from jax.experimental.pallas import tpu as pltpu
from jax.sharding import PartitionSpec as P


BF16, F32 = jnp.bfloat16, jnp.float32
MESH = pl.DeviceIdType.MESH
VMEM_LIMIT = 66_000_000
BLOCKS = 5
ALL = 6 * BLOCKS
SUMMED = 26
UNITS = 2
FINE, PIECES = 2, 5
FIRST = 5
SLOTS, SEND_SLOTS, LOAD_SLOTS = 12, 6, 4
NN = (((1,), (0,)), ((), ()))
NT = (((1,), (1,)), ((), ()))


def dot(a, b, dims=NN):
    return lax.dot_general(a, b, dims, preferred_element_type=F32)


def scale_of(wide):
    return lax.rsqrt(jnp.mean(wide * wide, -1, keepdims=True) + 1e-6)


def groups_of(ff):
    width = min(ff, 512)
    starts = list(range(0, ff - width + 1, width))
    pieces = [(s, (starts[i + 1] if i + 1 < len(starts) else ff) - s) for i, s in enumerate(starts)]
    return [g for g in (pieces[:1], pieces[1:3], pieces[3:]) if g]


def forward_kernel(groups, x_ref, wg_hbm, wu_hbm, wd_hbm, a0_ref, h1_ref, a1_ref, wg, wu, wd, p, sems):
    first = pl.program_id(0) == 0

    def loads(i):
        at = pl.ds(groups[i][0][0], sum(n for _, n in groups[i]))
        return (
            pltpu.make_async_copy(wg_hbm.at[0, :, at], wg.at[:, at], sems.at[0, i]),
            pltpu.make_async_copy(wu_hbm.at[0, :, at], wu.at[:, at], sems.at[1, i]),
            pltpu.make_async_copy(wd_hbm.at[0, at, :], wd.at[at, :], sems.at[2, i]),
        )

    everything = range(len(groups))

    @pl.when(first)
    def _():
        for i in everything:
            for c in loads(i)[:2]:
                c.start()
        for i in everything:
            loads(i)[2].start()

    wide = x_ref[...].astype(F32)
    a = (wide * scale_of(wide)).astype(BF16)
    a0_ref[...] = a
    for i in everything:

        @pl.when(first)
        def _(i=i):
            for c in loads(i)[:2]:
                c.wait()
            if i + 1 == len(groups):
                for j in everything:
                    loads(j)[2].wait()

        for s, n in groups[i]:
            gate = dot(a, wg[:, s : s + n])
            up = dot(a, wu[:, s : s + n])
            p[:, s : s + n] = (gate * (0.5 * jnp.tanh(0.5 * gate) + 0.5) * up).astype(BF16)

    h1 = (x_ref[...].astype(F32) + dot(p[...], wd[...]).astype(BF16).astype(F32)).astype(BF16)
    h1_ref[...] = h1
    wide1 = h1.astype(F32)
    a1_ref[...] = (wide1 * scale_of(wide1)).astype(BF16)


def forward(x, wg, wu, wd):
    t, d = x.shape
    ff = wg.shape[2]
    tile = min(t, 1024)
    groups = groups_of(ff)
    rows = pl.BlockSpec((tile, d), lambda i: (i, 0))
    anywhere = pl.BlockSpec(memory_space=pl.ANY)
    return pl.pallas_call(
        functools.partial(forward_kernel, groups),
        grid=(t // tile,),
        out_shape=[jax.ShapeDtypeStruct((t, d), BF16)] * 3,
        in_specs=[rows, anywhere, anywhere, anywhere],
        out_specs=[rows] * 3,
        scratch_shapes=[
            pltpu.VMEM((d, ff), BF16),
            pltpu.VMEM((d, ff), BF16),
            pltpu.VMEM((ff, d), BF16),
            pltpu.VMEM((tile, ff), BF16),
            pltpu.SemaphoreType.DMA((3, len(groups))),
        ],
        compiler_params=pltpu.CompilerParams(vmem_limit_bytes=VMEM_LIMIT, dimension_semantics=("arbitrary",)),
        cost_estimate=pl.CostEstimate(flops=6 * t * d * ff, bytes_accessed=6 * d * ff + 8 * t * d, transcendentals=t * ff),
        name="forward",
    )(x, wg, wu, wd)


HALF_STEPS, DA_STEPS, TILES = 4, 2, 4
BLOCK_STEPS, LOW_STEPS = 2 * HALF_STEPS + DA_STEPS, 2 * HALF_STEPS
TURN = BLOCKS * BLOCK_STEPS
STEPS = 1 + TURN + DA_STEPS + BLOCKS * LOW_STEPS


def step_of(s):
    p = jnp.where(s <= 3, s, s - 1)
    low = p - (TURN + DA_STEPS)
    block = jnp.where(p < TURN, p // BLOCK_STEPS, jnp.where(low < 0, BLOCKS, BLOCKS + low // LOW_STEPS))
    place = jnp.where(p < TURN, p % BLOCK_STEPS, jnp.where(low < 0, BLOCK_STEPS + p - TURN, low % LOW_STEPS))
    half = jnp.where(place < LOW_STEPS, place // HALF_STEPS, 0)
    kind = jnp.where(place < LOW_STEPS, place % HALF_STEPS, place - 2)
    return block, half, jnp.where(s == 3, 4, jnp.where(s == 4, 5, kind))


def made_in(kind):
    low = jnp.where((kind == 3) | (kind == 4), 1, jnp.where(kind == 5, 2, 0))
    high = jnp.where((kind == 3) | (kind == 5), 3, jnp.where(kind == 4, 2, jnp.where(kind == 2, 1, 0)))
    return low, high


def summed_piece(c):
    full, rest = SUMMED // 3, max(SUMMED % 3, 1)
    late = c - 6 * full
    return tuple(
        jnp.where(late < 0, early, other) for early, other in ((c // 6, full), (c % 6 // 3, late // rest), (c % 3, late % rest))
    )


def place_of(block, half, which):
    full, rest = SUMMED // 3, SUMMED % 3
    return jnp.where(block < full, 6 * block + 3 * half + which, 6 * full + rest * half + which)


def backward_kernel(
    a1_hbm, a0_hbm, h1_hbm, dy_hbm, wg_hbm, wu_hbm, wd_hbm,
    g_hbm, left_hbm, mine_hbm, theirs_hbm,
    ad, pgu, wgb, wub, wdb, wgt, wut, dat, stage, mb, xb, sb, ra, rb, tot, fsb, fra, frb, ftot,
    in_sem, w_sem, own_sem, give_sem, get_sem, left_sem, load_sem, s_sem, ra_sem, rb_sem, tot_sem, down_sem, up_sem, keep_sem, pass_sem, partner_sem,
    fs_sem, fra_sem, frb_sem, ftot_sem, fdown_sem, fup_sem, fkeep_sem, fpass_sem,
):
    me = lax.axis_index("dp")
    z, core = me // 2, me % 2
    partner = me + 1 - 2 * core
    t, d = ad.shape[1:]
    f, fs = wgt.shape[0], stage.shape[1]
    part, r = fs // 2, fs // 2 // UNITS
    units = 2 * SUMMED * UNITS
    coarse = units - FINE
    sub = dat.shape[2]

    def remote(src, dst, send, recv, device):
        return pltpu.make_async_remote_copy(src_ref=src, dst_ref=dst, send_sem=send, recv_sem=recv, device_id={"dp": device}, device_id_type=MESH)

    def weights(block):
        layer, j, slot = 1 - block // BLOCKS, block % BLOCKS, block % 2
        at = pl.ds(pl.multiple_of(j * f, f), f)
        return (
            pltpu.make_async_copy(wg_hbm.at[layer, :, at], wgb.at[slot], w_sem.at[slot, 0]),
            pltpu.make_async_copy(wu_hbm.at[layer, :, at], wub.at[slot], w_sem.at[slot, 1]),
            pltpu.make_async_copy(wd_hbm.at[layer, at, :], wdb.at[slot], w_sem.at[slot, 2]),
        )

    def load_tokens(which):
        at = pl.ds(which * (t // 2), t // 2)
        return (
            pltpu.make_async_copy(a1_hbm.at[at, :], ad.at[1, at, :], in_sem.at[0, which]),
            pltpu.make_async_copy(dy_hbm.at[at, :], ad.at[0, at, :], in_sem.at[1, which]),
        )

    load_h1 = pltpu.make_async_copy(h1_hbm, ad.at[1], in_sem.at[2, 0])
    load_a0 = pltpu.make_async_copy(a0_hbm, ad.at[1], in_sem.at[3, 0])

    for a, b in zip(weights(0), (*load_tokens(0), None)):
        a.start()
        if b is not None:
            b.start()
    for c in load_tokens(1):
        c.start()
    dat[...] = jnp.zeros_like(dat)

    barrier = pltpu.get_barrier_semaphore()
    pl.semaphore_signal(barrier, inc=1, device_id={"dp": partner}, device_id_type=MESH)

    @pl.when(z > 0)
    def _():
        pl.semaphore_signal(barrier, inc=1, device_id={"dp": me - 2}, device_id_type=MESH)

    @pl.when(z < 3)
    def _():
        pl.semaphore_signal(barrier, inc=1, device_id={"dp": me + 2}, device_id_type=MESH)

    pl.semaphore_wait(barrier, 3 - z // 3 - (3 - z) // 3)

    def at_half(half):
        return pl.ds(pl.multiple_of(half * fs, fs), fs)

    def hidden(block, half, tokens):
        slot = block % 2

        for which in range(2):

            @pl.when((block == 0) & (half == 0) & (tokens == which))
            def _(which=which):
                for c in load_tokens(which):
                    c.wait()

        @pl.when((half == 0) & (tokens == 0))
        def _():
            @pl.when(block == BLOCKS)
            def _():
                load_a0.wait()

            for c in weights(block):
                c.wait()

            @pl.when(block + 1 < 2 * BLOCKS)
            def _():
                for c in weights(block + 1):
                    c.start()

            wgt[...] = wgb[slot].T
            wut[...] = wub[slot].T

        units_at = at_half(half)
        for i in range(TILES // 2):
            at = pl.ds(pl.multiple_of((tokens * (TILES // 2) + i) * sub, sub), sub)
            gate = dot(wgt[units_at, :], ad[1, at, :], NT)
            up = dot(wut[units_at, :], ad[1, at, :], NT)
            dp = dot(wdb[slot, units_at, :], ad[0, at, :], NT).astype(BF16).astype(F32)
            sig = 0.5 * jnp.tanh(0.5 * gate) + 0.5
            silu = gate * sig
            pgu[0, units_at, at] = (silu * up).astype(BF16)
            pgu[1, units_at, at] = (dp * up * (sig + silu * (1.0 - sig))).astype(BF16)
            pgu[2, units_at, at] = (dp * silu).astype(BF16)

    def gradients(half, kind):
        def body(which, _):
            stage[which] = dot(pgu[which, at_half(half), :], ad[jnp.minimum(which, 1)]).astype(BF16)
            return 0

        lax.fori_loop(*made_in(kind), body, 0)

    def to_input(block, step):
        slot = block % 2

        @pl.when((block == BLOCKS - 1) & (step == 0))
        def _():
            load_h1.start()

        for i in range(TILES // DA_STEPS):
            tile = step * (TILES // DA_STEPS) + i
            at = pl.ds(pl.multiple_of(tile * sub, sub), sub)
            dat[tile] += dot(wgb[slot], pgu[1, :, at]) + dot(wub[slot], pgu[2, :, at])

    def turn(step):
        @pl.when(step == 0)
        def _():
            load_h1.wait()

        def body(i, _):
            tile = step * (TILES // DA_STEPS) + i
            at = pl.ds(pl.multiple_of(tile * sub, sub), sub)
            da = dat[tile].T.astype(BF16).astype(F32)
            wide = ad[1, at, :].astype(F32)
            scale = scale_of(wide)
            inner = jnp.sum(da * wide, -1, keepdims=True) * (scale * scale * scale) * (1.0 / d)
            through = (da * scale - wide * inner).astype(BF16).astype(F32)
            ad[0, at, :] = (ad[0, at, :].astype(F32) + through).astype(BF16)
            return 0

        lax.fori_loop(0, TILES // DA_STEPS, body, 0)

        @pl.when(step == DA_STEPS - 1)
        def _():
            load_a0.start()

    def rows(slot, c):
        return stage.at[slot, pl.ds(pl.multiple_of(c * part, part), part), :]

    def give_copy(slot, c):
        return remote(rows(slot, 1 - core), theirs_hbm.at[c], give_sem.at[slot], get_sem.at[c], partner)

    def own_copy(slot, c):
        return pltpu.make_async_copy(rows(slot, core), mine_hbm.at[c], own_sem.at[slot])

    def left_copy(slot, block, half, which):
        return pltpu.make_async_copy(stage.at[slot], left_hbm.at[3 * block + which - SUMMED, at_half(half), :], left_sem.at[slot])

    def stage_copies(block, half, which, go):
        slot, here = which, 3 * block + which < SUMMED

        @pl.when(here)
        def _():
            c = place_of(block, half, which)
            if go:
                own_copy(slot, c).start()
                give_copy(slot, c).start()
            else:
                own_copy(slot, c).wait()
                give_copy(slot, c).wait_send()

        @pl.when(jnp.logical_not(here))
        def _():
            copy = left_copy(slot, block, half, which)
            if go:
                copy.start()
            else:
                copy.wait()

    is0, is1, is2, is3 = z == 0, z == 1, z == 2, z == 3
    sum_lag = jnp.where(is1, 2, jnp.where(is2, 1, 0))
    tot_lag = jnp.where(is1, 2, jnp.where(is3, 9, jnp.where(is2, 5, 6)))
    free_lag = tot_lag + jnp.where(is3, 2, 3)

    def load_copies(k):
        q, at, slot = k // UNITS, pl.ds(pl.multiple_of((k % UNITS) * r, r), r), k % LOAD_SLOTS
        return (
            pltpu.make_async_copy(mine_hbm.at[q, at, :], mb.at[slot], load_sem.at[slot, 0]),
            pltpu.make_async_copy(theirs_hbm.at[q, at, :], xb.at[slot], load_sem.at[slot, 1]),
        )

    def s_copy_edge(k):
        return remote(sb.at[k % SEND_SLOTS], ra.at[k % SLOTS], s_sem.at[k % SEND_SLOTS], ra_sem.at[k % SLOTS], me + 2 - 4 * (z // 3))

    def s_copy_inner(k):
        return remote(sb.at[k % SEND_SLOTS], rb.at[k % SLOTS], s_sem.at[k % SEND_SLOTS], rb_sem.at[k % SLOTS], me - 2)

    def tot_down(k):
        return remote(tot.at[k % SLOTS], tot.at[k % SLOTS], down_sem.at[k % SLOTS], tot_sem.at[k % SLOTS], me - 2)

    def tot_up(k):
        return remote(tot.at[k % SLOTS], tot.at[k % SLOTS], up_sem.at[k % SLOTS], tot_sem.at[k % SLOTS], me + 2)

    def out_copies(k):
        block, half, which = summed_piece(k // UNITS)
        q, at, slot = 3 * block + which, pl.ds(pl.multiple_of(half * fs + core * part + (k % UNITS) * r, r), r), k % SLOTS
        return (
            pltpu.make_async_copy(tot.at[slot], g_hbm.at[q, at, :], keep_sem.at[slot]),
            remote(tot.at[slot], g_hbm.at[q, at, :], pass_sem.at[slot], partner_sem, partner),
        )

    def inside(k):
        return (k >= 0) & (k < coarse)

    def free(k):
        @pl.when(inside(k))
        def _():
            keep, give = out_copies(k)
            keep.wait()
            give.wait_send()

            @pl.when(is1)
            def _():
                tot_down(k).wait_send()

            @pl.when(is1 | is2)
            def _():
                tot_up(k).wait_send()

    def add(k):
        @pl.when(inside(k))
        def _():
            for c in load_copies(k):
                c.wait()
            slot = k % LOAD_SLOTS
            both = mb[slot].astype(F32) + xb[slot].astype(F32)

            @pl.when((is0 | is3) & (k >= SEND_SLOTS))
            def _():
                s_copy_edge(k - SEND_SLOTS).wait_send()

            @pl.when(is2 & (k >= SEND_SLOTS))
            def _():
                s_copy_inner(k - SEND_SLOTS).wait_send()

            @pl.when(is0 | is3)
            def _():
                sb[k % SEND_SLOTS] = both.astype(BF16)

            @pl.when(is2)
            def _():
                s_copy_edge(k).wait_recv()
                sb[k % SEND_SLOTS] = (both + ra[k % SLOTS].astype(F32)).astype(BF16)

            @pl.when(is1)
            def _():
                s_copy_edge(k).wait_recv()
                s_copy_inner(k).wait_recv()
                tot[k % SLOTS] = (both + ra[k % SLOTS].astype(F32) + rb[k % SLOTS].astype(F32)).astype(BF16)

    def arrive(k):
        @pl.when(inside(k) & (z != 1))
        def _():
            tot_down(k).wait_recv()

    def send(k_sum, k_tot):
        @pl.when(inside(k_sum) & (is0 | is3))
        def _():
            s_copy_edge(k_sum).start()

        @pl.when(inside(k_sum) & is2)
        def _():
            s_copy_inner(k_sum).start()

        @pl.when(inside(k_tot))
        def _():
            @pl.when(is1)
            def _():
                tot_down(k_tot).start()

            @pl.when(is1 | is2)
            def _():
                tot_up(k_tot).start()

            for c in out_copies(k_tot):
                c.start()

    def fine_edge(j):
        return remote(fsb.at[j], fra.at[j], fs_sem.at[j], fra_sem.at[j], me + 2 - 4 * (z // 3))

    def fine_inner(j):
        return remote(fsb.at[j], frb.at[j], fs_sem.at[j], frb_sem.at[j], me - 2)

    def fine_down(j):
        return remote(ftot.at[j], ftot.at[j], fdown_sem.at[j], ftot_sem.at[j], me - 2)

    def fine_up(j):
        return remote(ftot.at[j], ftot.at[j], fup_sem.at[j], ftot_sem.at[j], me + 2)

    def fine_out(j):
        fr = r // PIECES
        k = coarse + j // PIECES
        block, half, which = summed_piece(k // UNITS)
        row = half * fs + core * part + (k % UNITS) * r + (j % PIECES) * fr
        q, at = 3 * block + which, pl.ds(pl.multiple_of(row, fr), fr)
        return (
            pltpu.make_async_copy(ftot.at[j], g_hbm.at[q, at, :], fkeep_sem.at[j]),
            remote(ftot.at[j], g_hbm.at[q, at, :], fpass_sem.at[j], partner_sem, partner),
        )

    def fine_send(j):
        @pl.when(is1)
        def _():
            fine_up(j).start()
            fine_down(j).start()

        @pl.when(is2)
        def _():
            fine_up(j).start()

        for c in fine_out(j):
            c.start()

    def fine_add(k):
        @pl.when((k >= coarse) & (k < units))
        def _():
            for c in load_copies(k):
                c.wait()
            fr, slot = r // PIECES, k % LOAD_SLOTS

            def body(i, _):
                j = (k - coarse) * PIECES + i
                at = pl.ds(pl.multiple_of(i * fr, fr), fr)
                both = mb[slot, at, :].astype(F32) + xb[slot, at, :].astype(F32)

                @pl.when(is0 | is3)
                def _():
                    fsb[j] = both.astype(BF16)
                    fine_edge(j).start()

                @pl.when(is2)
                def _():
                    fine_edge(j).wait_recv()
                    fsb[j] = (both + fra[j].astype(F32)).astype(BF16)
                    fine_inner(j).start()

                @pl.when(is1)
                def _():
                    fine_edge(j).wait_recv()
                    fine_inner(j).wait_recv()
                    ftot[j] = (both + fra[j].astype(F32) + frb[j].astype(F32)).astype(BF16)
                    fine_send(j)

                return 0

            lax.fori_loop(0, PIECES, body, 0)

    def fine_arrive(k):
        @pl.when((k >= coarse) & (k < units) & (z != 1))
        def _():
            def body(i, _):
                j = (k - coarse) * PIECES + i
                fine_down(j).wait_recv()
                fine_send(j)
                return 0

            lax.fori_loop(0, PIECES, body, 0)

    def fine_end():
        def body(j, _):
            keep, give = fine_out(j)
            keep.wait()
            give.wait_send()

            @pl.when(is0 | is3)
            def _():
                fine_edge(j).wait_send()

            @pl.when(is2)
            def _():
                fine_inner(j).wait_send()

            @pl.when(is1)
            def _():
                fine_down(j).wait_send()

            @pl.when(is1 | is2)
            def _():
                fine_up(j).wait_send()

            return 0

        lax.fori_loop(0, FINE * PIECES, body, 0)

    def load(k):
        @pl.when((k >= 0) & (k < units))
        def _():
            @pl.when(k % UNITS == 0)
            def _():
                give_copy(0, k // UNITS).wait_recv()

            for c in load_copies(k):
                c.start()


    def stage_of(s, go):
        @pl.when((s >= 0) & (s < STEPS))
        def _():
            block, half, kind = step_of(s)

            def body(which, _):
                stage_copies(block, half, which, go)
                return 0

            lax.fori_loop(*made_in(kind), body, 0)

    def tick(i, _):
        stage_of(i - 2, False)
        stage_of(i - 1, True)
        now = i - FIRST
        free(now - free_lag)
        add(now - sum_lag)
        arrive(now - tot_lag)
        send(now - sum_lag, now - tot_lag)
        fine_add(now - sum_lag)
        fine_arrive(now - tot_lag)
        load(now - sum_lag + 1)

        @pl.when(i < STEPS)
        def _():
            block, half, kind = step_of(i)

            @pl.when(kind < 2)
            def _():
                hidden(block, half, kind)

            @pl.when((kind >= 2) & (kind <= 5))
            def _():
                gradients(half, kind)

            @pl.when((kind == 6) | (kind == 7))
            def _():
                to_input(block, kind - 6)

            @pl.when(kind >= 8)
            def _():
                turn(kind - 8)

        return 0

    lax.fori_loop(0, max(FIRST + units + 12, STEPS + 2), tick, 0)

    for k in range(coarse - SEND_SLOTS, coarse):

        @pl.when(is0 | is3)
        def _(k=k):
            s_copy_edge(k).wait_send()

        @pl.when(is2)
        def _(k=k):
            s_copy_inner(k).wait_send()

    fine_end()
    pltpu.make_async_copy(theirs_hbm, theirs_hbm, partner_sem).wait()


def backward(a1, a0, h1, dy, wg, wu, wd):
    t, d = a1.shape
    ff = wg.shape[2]
    f = ff // BLOCKS
    fs = f // 2
    r = fs // 2 // UNITS
    sub = t // TILES
    anywhere = pl.BlockSpec(memory_space=pl.ANY)
    dma = pltpu.SemaphoreType.DMA
    return pl.pallas_call(
        backward_kernel,
        out_shape=[
            jax.ShapeDtypeStruct((SUMMED, f, d), BF16),
            jax.ShapeDtypeStruct((ALL - SUMMED, f, d), BF16),
            jax.ShapeDtypeStruct((2 * SUMMED, fs // 2, d), BF16),
            jax.ShapeDtypeStruct((2 * SUMMED, fs // 2, d), BF16),
        ],
        in_specs=[anywhere] * 7,
        out_specs=[anywhere] * 4,
        scratch_shapes=[
            pltpu.VMEM((2, t, d), BF16),
            pltpu.VMEM((3, f, t), BF16),
            pltpu.VMEM((2, d, f), BF16),
            pltpu.VMEM((2, d, f), BF16),
            pltpu.VMEM((2, f, d), BF16),
            pltpu.VMEM((f, d), BF16),
            pltpu.VMEM((f, d), BF16),
            pltpu.VMEM((TILES, d, sub), F32),
            pltpu.VMEM((3, fs, d), BF16),
            pltpu.VMEM((LOAD_SLOTS, r, d), BF16),
            pltpu.VMEM((LOAD_SLOTS, r, d), BF16),
            pltpu.VMEM((SEND_SLOTS, r, d), BF16),
            pltpu.VMEM((SLOTS, r, d), BF16),
            pltpu.VMEM((SLOTS, r, d), BF16),
            pltpu.VMEM((SLOTS, r, d), BF16),
            *[pltpu.VMEM((FINE * PIECES, r // PIECES, d), BF16)] * 4,
            dma((4, 2)),
            dma((2, 3)),
            dma((3,)),
            dma((3,)),
            dma((2 * SUMMED,)),
            dma((3,)),
            dma((LOAD_SLOTS, 2)),
            dma((SEND_SLOTS,)),
            dma((SLOTS,)),
            dma((SLOTS,)),
            dma((SLOTS,)),
            dma((SLOTS,)),
            dma((SLOTS,)),
            dma((SLOTS,)),
            dma((SLOTS,)),
            dma,
            *[dma((FINE * PIECES,))] * 8,
        ],
        compiler_params=pltpu.CompilerParams(collective_id=0, has_side_effects=True, vmem_limit_bytes=VMEM_LIMIT),
        cost_estimate=pl.CostEstimate(flops=2 * 15 * t * d * ff, bytes_accessed=100 * d * ff, transcendentals=2 * t * ff),
        name="backward",
    )(a1, a0, h1, dy, wg, wu, wd)


HALVES = ((1, 0), (1, 1), (2, 0), (2, 1), (0, 0), (0, 1))


def adamw_kernel(rounds, first, n_old, *refs):
    arrays = {1: refs[0:3], 2: refs[3:6], 0: refs[6:9]}
    g_hbm = refs[9]
    outs = refs[10 + n_old :][:9]
    outs = {1: outs[0:3], 2: outs[3:6], 0: outs[6:9]}
    wt, mt, vt, gt, wd, md, vd, gd, wt_out, mt_out, vt_out, wd_out, md_out, vd_out, turned, in_sem, out_sem = refs[10 + n_old + 9 :]
    d, f = wt.shape[1] * 2, wt.shape[2]

    def place(b, half):
        which, s = HALVES[half]
        layer, j, q = 1 - b // BLOCKS, b % BLOCKS, 3 * b + which - first
        if which:
            cols = pl.ds(pl.multiple_of(j * f, f), f)
            return which, lambda ref: ref.at[layer, pl.ds(s * (d // 2), d // 2), cols], g_hbm.at[q, :, pl.ds(s * (d // 2), d // 2)]
        rows = pl.ds(pl.multiple_of(j * f + s * (f // 2), f // 2), f // 2)
        return which, lambda ref: ref.at[layer, rows, :], g_hbm.at[q, pl.ds(s * (f // 2), f // 2), :]

    def buffers(half):
        if HALVES[half][0]:
            return [x.at[half] for x in (wt, mt, vt, gt)], [x.at[half] for x in (wt_out, mt_out, vt_out)]
        return [x.at[half - 4] for x in (wd, md, vd, gd)], [x.at[half - 4] for x in (wd_out, md_out, vd_out)]

    def loads(b, half):
        which, at, g = place(b, half)
        sources = [at(x) for x in arrays[which]] + [g]
        return [pltpu.make_async_copy(x, y, in_sem.at[half, i]) for i, (x, y) in enumerate(zip(sources, buffers(half)[0], strict=True))]

    def stores(b, half):
        which, at, _ = place(b, half)
        return [pltpu.make_async_copy(x, at(y), out_sem.at[half, i]) for i, (x, y) in enumerate(zip(buffers(half)[1], outs[which], strict=True))]

    def take(half):
        (w_in, m_in, v_in, g_in), (w_out, m_out, v_out) = buffers(half)
        if HALVES[half][0]:
            turned[...] = g_in[...].T
            g_in = turned

        def body(i, _):
            at = pl.ds(pl.multiple_of(i * 16, 16), 16)
            g = g_in[at, :].astype(F32)
            m = 0.9 * m_in[at, :] + 0.1 * g
            v = 0.95 * v_in[at, :] + 0.05 * g * g
            w = w_in[at, :].astype(F32)
            w_out[at, :] = (w - 0.02 * (m * lax.rsqrt(v + 1e-8) + 0.1 * w)).astype(BF16)
            m_out[at, :] = m
            v_out[at, :] = v
            return 0

        lax.fori_loop(0, w_in.shape[0] // 16, body, 0, unroll=2)

    def start(copies):
        for c in copies:
            c.start()

    def wait(copies):
        for c in copies:
            c.wait()

    starts = {}
    for blocks, halves in rounds:
        for half in halves:
            if half not in starts:
                starts[half] = True
                start(loads(blocks[0], half))
    before = {}
    for n, (blocks, halves) in enumerate(rounds):
        low, high = blocks

        def next_of(half, n=n):
            return next((bs[0] for bs, hs in rounds[n + 1 :] if half in hs), None)

        def one(b, half, low=low, high=high, next_of=next_of):
            wait(loads(b, half))
            if half in before:
                wait(stores(before[half], half))
            elif high - low > 1:

                @pl.when(b > low)
                def _():
                    wait(stores(b - 1, half))

            take(half)
            start(stores(b, half))
            if high - low > 1:

                @pl.when(b + 1 < high)
                def _():
                    start(loads(b + 1, half))

            after = next_of(half)
            if after is not None:
                if high - low > 1:

                    @pl.when(b + 1 == high)
                    def _():
                        start(loads(after, half))

                else:
                    start(loads(after, half))

        def turn(b, _, halves=halves):
            for half in halves:
                one(b, half)
            return 0

        if high - low > 1:
            lax.fori_loop(low, high, turn, 0)
        else:
            turn(low, 0)
        for half in halves:
            before[half] = high - 1
    for half, b in before.items():
        wait(stores(b, half))


def adamw(pieces, first, g, w, m, v, old=()):
    low, high = pieces
    d, ff = w[0].shape[1:]
    f = ff // BLOCKS
    rounds = []
    for b in range(2 * BLOCKS):
        halves = tuple(h for h, (which, _) in enumerate(HALVES) if low <= 3 * b + which < high)
        if not halves:
            continue
        if len(rounds) == 1 and rounds[0][1] == halves:
            rounds[-1] = ((rounds[-1][0][0], b + 1), halves)
        else:
            rounds.append(((b, b + 1), halves))
    anywhere = pl.BlockSpec(memory_space=pl.ANY)
    operands = [x for i in range(3) for x in (w[i], m[i], v[i])]
    n = (high - low) * d * f
    return pl.pallas_call(
        functools.partial(adamw_kernel, tuple(rounds), first, len(old)),
        out_shape=[jax.ShapeDtypeStruct(x.shape, x.dtype) for x in operands],
        in_specs=[anywhere] * (10 + len(old)),
        out_specs=[anywhere] * 9,
        scratch_shapes=[
            pltpu.VMEM((4, d // 2, f), BF16),
            pltpu.VMEM((4, d // 2, f), F32),
            pltpu.VMEM((4, d // 2, f), F32),
            pltpu.VMEM((4, f, d // 2), BF16),
            pltpu.VMEM((2, f // 2, d), BF16),
            pltpu.VMEM((2, f // 2, d), F32),
            pltpu.VMEM((2, f // 2, d), F32),
            pltpu.VMEM((2, f // 2, d), BF16),
            pltpu.VMEM((4, d // 2, f), BF16),
            pltpu.VMEM((4, d // 2, f), F32),
            pltpu.VMEM((4, d // 2, f), F32),
            pltpu.VMEM((2, f // 2, d), BF16),
            pltpu.VMEM((2, f // 2, d), F32),
            pltpu.VMEM((2, f // 2, d), F32),
            pltpu.VMEM((d // 2, f), BF16),
            pltpu.SemaphoreType.DMA((6, 4)),
            pltpu.SemaphoreType.DMA((6, 3)),
        ],
        input_output_aliases={10 + i: i for i in range(len(old))},
        compiler_params=pltpu.CompilerParams(vmem_limit_bytes=VMEM_LIMIT),
        cost_estimate=pl.CostEstimate(flops=2000 * n, bytes_accessed=22 * n, transcendentals=n),
        name="adamw",
    )(*operands, g, *old)


def solution(mesh):
    def step(x, dy, *arrays):
        w, m, v = (arrays[i : i + 3] for i in (0, 3, 6))
        wg, wu, wd = w
        a0, h1, a1 = forward(x[0], wg, wu, wd)
        g, left, _, _ = backward(a1, a0, h1, dy[0], wg, wu, wd)
        left = lax.psum(left, "dp")
        done = adamw((0, SUMMED), 0, g, w, m, v)
        done = adamw((SUMMED, ALL), SUMMED, left, w, m, v, done)
        return tuple(done[3 * i + kind] for kind in range(3) for i in range(3))

    return jax.shard_map(
        step,
        mesh=mesh,
        in_specs=(P(("rep", "dp"), None, None),) * 2 + (P(None, None, None),) * 9,
        out_specs=(P("rep", None, None),) * 9,
        check_vma=False,
    )
```

```python
import functools

import jax
import jax.numpy as jnp
from jax import lax
from jax.experimental import pallas as pl
from jax.experimental.pallas import tpu as pltpu
from jax.sharding import PartitionSpec as P

BF16, F32 = jnp.bfloat16, jnp.float32
MESH = pl.DeviceIdType.MESH
VMEM_LIMIT = 66_000_000
BLOCKS = 5
ALL = 6 * BLOCKS
SUMMED = 26
UNITS = 2
FINE, PIECES = 2, 5
FIRST = 5
SLOTS, SEND_SLOTS, LOAD_SLOTS = 12, 6, 4
NN = (((1,), (0,)), ((), ()))
NT = (((1,), (1,)), ((), ()))


def dot(a, b, dims=NN):
    return lax.dot_general(a, b, dims, preferred_element_type=F32)


def scale_of(wide):
    return lax.rsqrt(jnp.mean(wide * wide, -1, keepdims=True) + 1e-6)


def groups_of(ff):
    shared = ff - 128 if ff % 512 == 128 and ff > 512 else None
    end = ff if shared is None else shared
    width = min(end, 512)
    starts = list(range(0, end - width + 1, width))
    pieces = [(s, (starts[i + 1] if i + 1 < len(starts) else end) - s) for i, s in enumerate(starts)]
    return [g for g in (pieces[:2], pieces[2:]) if g], shared


def forward_kernel(groups, shared, x_hbm, wg_hbm, wu_hbm, wd_hbm, a0_ref, h1_ref, a1_ref, x, wg, wu, both, wd, p, sems, x_sem):
    tile, tiles = a0_ref.shape[0], x.shape[0]
    now = pl.program_id(0)
    first = now == 0

    def load_x(i):
        return pltpu.make_async_copy(x_hbm.at[pl.ds(i * tile, tile), :], x.at[i], x_sem.at[i])

    def loads(i):
        at = pl.ds(groups[i][0][0], sum(n for _, n in groups[i]))
        copies = [
            pltpu.make_async_copy(wg_hbm.at[0, :, at], wg.at[:, at], sems.at[0, i]),
            pltpu.make_async_copy(wu_hbm.at[0, :, at], wu.at[:, at], sems.at[1, i]),
        ]
        if shared is not None and i + 1 == len(groups):
            for k, w_hbm in enumerate((wg_hbm, wu_hbm)):
                half = both.at[:, pl.ds(k * 128, 128)]
                copies.append(pltpu.make_async_copy(w_hbm.at[0, :, pl.ds(shared, 128)], half, sems.at[2, k]))
        return copies

    load_down = pltpu.make_async_copy(wd_hbm.at[0], wd, sems.at[3, 0])

    @pl.when(first)
    def _():
        load_x(0).start()
        for i in range(len(groups)):
            for c in loads(i):
                c.start()
        load_down.start()
        for i in range(1, tiles):
            load_x(i).start()

    load_x(now).wait()
    wide = x[now].astype(F32)
    a = (wide * scale_of(wide)).astype(BF16)
    a0_ref[...] = a

    def product(gate, up):
        return (gate * (0.5 * jnp.tanh(0.5 * gate) + 0.5) * up).astype(BF16)

    for i in range(len(groups)):

        @pl.when(first)
        def _(i=i):
            for c in loads(i):
                c.wait()
            if i + 1 == len(groups):
                load_down.wait()

        for s, n in groups[i]:
            p[:, s : s + n] = product(dot(a, wg[:, s : s + n]), dot(a, wu[:, s : s + n]))
    if shared is not None:
        gate_up = dot(a, both[...])
        p[:, shared:] = product(gate_up[:, :128], gate_up[:, 128:])

    h1 = (x[now].astype(F32) + dot(p[...], wd[...]).astype(BF16).astype(F32)).astype(BF16)
    h1_ref[...] = h1
    wide1 = h1.astype(F32)
    a1_ref[...] = (wide1 * scale_of(wide1)).astype(BF16)


def forward(x, wg, wu, wd):
    t, d = x.shape
    ff = wg.shape[2]
    tile = min(t, 1024)
    groups, shared = groups_of(ff)
    anywhere = pl.BlockSpec(memory_space=pl.ANY)
    return pl.pallas_call(
        functools.partial(forward_kernel, groups, shared),
        grid=(t // tile,),
        out_shape=[jax.ShapeDtypeStruct((t, d), BF16)] * 3,
        in_specs=[anywhere] * 4,
        out_specs=[pl.BlockSpec((tile, d), lambda i: (i, 0))] * 3,
        scratch_shapes=[
            pltpu.VMEM((t // tile, tile, d), BF16),
            pltpu.VMEM((d, ff), BF16),
            pltpu.VMEM((d, ff), BF16),
            pltpu.VMEM((d, 256), BF16),
            pltpu.VMEM((ff, d), BF16),
            pltpu.VMEM((tile, ff), BF16),
            pltpu.SemaphoreType.DMA((4, 2)),
            pltpu.SemaphoreType.DMA((t // tile,)),
        ],
        compiler_params=pltpu.CompilerParams(vmem_limit_bytes=VMEM_LIMIT, dimension_semantics=("arbitrary",)),
        cost_estimate=pl.CostEstimate(flops=6 * t * d * ff, bytes_accessed=6 * d * ff + 8 * t * d, transcendentals=t * ff),
        name="forward",
    )(x, wg, wu, wd)


HALF_STEPS, DA_STEPS, TILES = 4, 2, 4
BLOCK_STEPS, LOW_STEPS = 2 * HALF_STEPS + DA_STEPS, 2 * HALF_STEPS
TURN = BLOCKS * BLOCK_STEPS
STEPS = 1 + TURN + DA_STEPS + BLOCKS * LOW_STEPS


def step_of(s):
    p = jnp.where(s <= 3, s, s - 1)
    low = p - (TURN + DA_STEPS)
    block = jnp.where(p < TURN, p // BLOCK_STEPS, jnp.where(low < 0, BLOCKS, BLOCKS + low // LOW_STEPS))
    place = jnp.where(p < TURN, p % BLOCK_STEPS, jnp.where(low < 0, BLOCK_STEPS + p - TURN, low % LOW_STEPS))
    half = jnp.where(place < LOW_STEPS, place // HALF_STEPS, 0)
    kind = jnp.where(place < LOW_STEPS, place % HALF_STEPS, place - 2)
    return block, half, jnp.where(s == 3, 4, jnp.where(s == 4, 5, kind))


def made_in(kind):
    low = jnp.where((kind == 3) | (kind == 4), 1, jnp.where(kind == 5, 2, 0))
    high = jnp.where((kind == 3) | (kind == 5), 3, jnp.where(kind == 4, 2, jnp.where(kind == 2, 1, 0)))
    return low, high


def summed_piece(c):
    full, rest = SUMMED // 3, max(SUMMED % 3, 1)
    late = c - 6 * full
    return tuple(
        jnp.where(late < 0, early, other) for early, other in ((c // 6, full), (c % 6 // 3, late // rest), (c % 3, late % rest))
    )


def place_of(block, half, which):
    full, rest = SUMMED // 3, SUMMED % 3
    return jnp.where(block < full, 6 * block + 3 * half + which, 6 * full + rest * half + which)


def backward_kernel(
    a1_hbm, a0_hbm, h1_hbm, dy_hbm, wg_hbm, wu_hbm, wd_hbm,
    g_hbm, left_hbm, mine_hbm, theirs_hbm,
    ad, pgu, wgb, wub, wdb, wgt, wut, dat, stage, mb, xb, sb, ra, rb, tot, fsb, fra, frb, ftot,
    in_sem, w_sem, own_sem, give_sem, get_sem, left_sem, load_sem, s_sem, ra_sem, rb_sem, tot_sem, down_sem, up_sem, keep_sem, pass_sem, partner_sem,
    fs_sem, fra_sem, frb_sem, ftot_sem, fdown_sem, fup_sem, fkeep_sem, fpass_sem,
):
    me = lax.axis_index("dp")
    z, core = me // 2, me % 2
    partner = me + 1 - 2 * core
    t, d = ad.shape[1:]
    f, fs = wgt.shape[0], stage.shape[1]
    part, r = fs // 2, fs // 2 // UNITS
    units = 2 * SUMMED * UNITS
    coarse = units - FINE
    sub = dat.shape[2]

    def remote(src, dst, send, recv, device):
        return pltpu.make_async_remote_copy(src_ref=src, dst_ref=dst, send_sem=send, recv_sem=recv, device_id={"dp": device}, device_id_type=MESH)

    def weights(block):
        layer, j, slot = 1 - block // BLOCKS, block % BLOCKS, block % 2
        at = pl.ds(pl.multiple_of(j * f, f), f)
        return (
            pltpu.make_async_copy(wg_hbm.at[layer, :, at], wgb.at[slot], w_sem.at[slot, 0]),
            pltpu.make_async_copy(wu_hbm.at[layer, :, at], wub.at[slot], w_sem.at[slot, 1]),
            pltpu.make_async_copy(wd_hbm.at[layer, at, :], wdb.at[slot], w_sem.at[slot, 2]),
        )

    def load_tokens(which):
        at = pl.ds(which * (t // 2), t // 2)
        return (
            pltpu.make_async_copy(a1_hbm.at[at, :], ad.at[1, at, :], in_sem.at[0, which]),
            pltpu.make_async_copy(dy_hbm.at[at, :], ad.at[0, at, :], in_sem.at[1, which]),
        )

    load_h1 = pltpu.make_async_copy(h1_hbm, ad.at[1], in_sem.at[2, 0])
    load_a0 = pltpu.make_async_copy(a0_hbm, ad.at[1], in_sem.at[3, 0])

    for a, b in zip(weights(0), (*load_tokens(0), None)):
        a.start()
        if b is not None:
            b.start()
    for c in load_tokens(1):
        c.start()
    dat[...] = jnp.zeros_like(dat)

    barrier = pltpu.get_barrier_semaphore()
    pl.semaphore_signal(barrier, inc=1, device_id={"dp": partner}, device_id_type=MESH)

    @pl.when(z > 0)
    def _():
        pl.semaphore_signal(barrier, inc=1, device_id={"dp": me - 2}, device_id_type=MESH)

    @pl.when(z < 3)
    def _():
        pl.semaphore_signal(barrier, inc=1, device_id={"dp": me + 2}, device_id_type=MESH)

    pl.semaphore_wait(barrier, 3 - z // 3 - (3 - z) // 3)

    def at_half(half):
        return pl.ds(pl.multiple_of(half * fs, fs), fs)

    def hidden(block, half, tokens):
        slot = block % 2

        for which in range(2):

            @pl.when((block == 0) & (half == 0) & (tokens == which))
            def _(which=which):
                for c in load_tokens(which):
                    c.wait()

        @pl.when((half == 0) & (tokens == 0))
        def _():
            @pl.when(block == BLOCKS)
            def _():
                load_a0.wait()

            for c in weights(block):
                c.wait()

            @pl.when(block + 1 < 2 * BLOCKS)
            def _():
                for c in weights(block + 1):
                    c.start()

        cut = -(-fs // 128) * 128
        for which, at in ((0, slice(0, cut)), (1, slice(cut, f))):

            @pl.when((half == which) & (tokens == 0))
            def _(at=at):
                wgt[at, :] = wgb[slot, :, at].T
                wut[at, :] = wub[slot, :, at].T

        units_at = at_half(half)
        for i in range(TILES // 2):
            at = pl.ds(pl.multiple_of((tokens * (TILES // 2) + i) * sub, sub), sub)
            gate = dot(wgt[units_at, :], ad[1, at, :], NT)
            up = dot(wut[units_at, :], ad[1, at, :], NT)
            dp = dot(wdb[slot, units_at, :], ad[0, at, :], NT).astype(BF16).astype(F32)
            sig = 0.5 * jnp.tanh(0.5 * gate) + 0.5
            silu = gate * sig
            pgu[0, units_at, at] = (silu * up).astype(BF16)
            pgu[1, units_at, at] = (dp * up * (sig + silu * (1.0 - sig))).astype(BF16)
            pgu[2, units_at, at] = (dp * silu).astype(BF16)

    def gradients(half, kind):
        def body(which, _):
            stage[which] = dot(pgu[which, at_half(half), :], ad[jnp.minimum(which, 1)]).astype(BF16)
            return 0

        lax.fori_loop(*made_in(kind), body, 0)

    def to_input(block, step):
        slot = block % 2

        @pl.when((block == BLOCKS - 1) & (step == 0))
        def _():
            load_h1.start()

        for i in range(TILES // DA_STEPS):
            tile = step * (TILES // DA_STEPS) + i
            at = pl.ds(pl.multiple_of(tile * sub, sub), sub)
            dat[tile] += dot(wgb[slot], pgu[1, :, at]) + dot(wub[slot], pgu[2, :, at])

    def turn(step):
        @pl.when(step == 0)
        def _():
            load_h1.wait()

        def body(i, _):
            tile = step * (TILES // DA_STEPS) + i
            at = pl.ds(pl.multiple_of(tile * sub, sub), sub)
            da = dat[tile].T.astype(BF16).astype(F32)
            wide = ad[1, at, :].astype(F32)
            scale = scale_of(wide)
            inner = jnp.sum(da * wide, -1, keepdims=True) * (scale * scale * scale) * (1.0 / d)
            through = (da * scale - wide * inner).astype(BF16).astype(F32)
            ad[0, at, :] = (ad[0, at, :].astype(F32) + through).astype(BF16)
            return 0

        lax.fori_loop(0, TILES // DA_STEPS, body, 0)

        @pl.when(step == DA_STEPS - 1)
        def _():
            load_a0.start()

    def rows(slot, c):
        return stage.at[slot, pl.ds(pl.multiple_of(c * part, part), part), :]

    def give_copy(slot, c):
        return remote(rows(slot, 1 - core), theirs_hbm.at[c], give_sem.at[slot], get_sem.at[c], partner)

    def own_copy(slot, c):
        return pltpu.make_async_copy(rows(slot, core), mine_hbm.at[c], own_sem.at[slot])

    def left_copy(slot, block, half, which):
        return pltpu.make_async_copy(stage.at[slot], left_hbm.at[3 * block + which - SUMMED, at_half(half), :], left_sem.at[slot])

    def stage_copies(block, half, which, go):
        slot, here = which, 3 * block + which < SUMMED

        @pl.when(here)
        def _():
            c = place_of(block, half, which)
            if go:
                own_copy(slot, c).start()
                give_copy(slot, c).start()
            else:
                own_copy(slot, c).wait()
                give_copy(slot, c).wait_send()

        @pl.when(jnp.logical_not(here))
        def _():
            copy = left_copy(slot, block, half, which)
            if go:
                copy.start()
            else:
                copy.wait()

    is0, is1, is2, is3 = z == 0, z == 1, z == 2, z == 3
    sum_lag = jnp.where(is1, 2, jnp.where(is2, 1, 0))
    tot_lag = jnp.where(is1, 2, jnp.where(is3, 9, jnp.where(is2, 5, 6)))
    free_lag = tot_lag + jnp.where(is3, 2, 3)

    def load_copies(k):
        q, at, slot = k // UNITS, pl.ds(pl.multiple_of((k % UNITS) * r, r), r), k % LOAD_SLOTS
        return (
            pltpu.make_async_copy(mine_hbm.at[q, at, :], mb.at[slot], load_sem.at[slot, 0]),
            pltpu.make_async_copy(theirs_hbm.at[q, at, :], xb.at[slot], load_sem.at[slot, 1]),
        )

    def s_copy_edge(k):
        return remote(sb.at[k % SEND_SLOTS], ra.at[k % SLOTS], s_sem.at[k % SEND_SLOTS], ra_sem.at[k % SLOTS], me + 2 - 4 * (z // 3))

    def s_copy_inner(k):
        return remote(sb.at[k % SEND_SLOTS], rb.at[k % SLOTS], s_sem.at[k % SEND_SLOTS], rb_sem.at[k % SLOTS], me - 2)

    def tot_down(k):
        return remote(tot.at[k % SLOTS], tot.at[k % SLOTS], down_sem.at[k % SLOTS], tot_sem.at[k % SLOTS], me - 2)

    def tot_up(k):
        return remote(tot.at[k % SLOTS], tot.at[k % SLOTS], up_sem.at[k % SLOTS], tot_sem.at[k % SLOTS], me + 2)

    def out_copies(k):
        block, half, which = summed_piece(k // UNITS)
        q, at, slot = 3 * block + which, pl.ds(pl.multiple_of(half * fs + core * part + (k % UNITS) * r, r), r), k % SLOTS
        return (
            pltpu.make_async_copy(tot.at[slot], g_hbm.at[q, at, :], keep_sem.at[slot]),
            remote(tot.at[slot], g_hbm.at[q, at, :], pass_sem.at[slot], partner_sem, partner),
        )

    def inside(k):
        return (k >= 0) & (k < coarse)

    def free(k):
        @pl.when(inside(k))
        def _():
            keep, give = out_copies(k)
            keep.wait()
            give.wait_send()

            @pl.when(is1)
            def _():
                tot_down(k).wait_send()

            @pl.when(is1 | is2)
            def _():
                tot_up(k).wait_send()

    def add(k):
        @pl.when(inside(k))
        def _():
            for c in load_copies(k):
                c.wait()
            slot = k % LOAD_SLOTS
            both = mb[slot].astype(F32) + xb[slot].astype(F32)

            @pl.when((is0 | is3) & (k >= SEND_SLOTS))
            def _():
                s_copy_edge(k - SEND_SLOTS).wait_send()

            @pl.when(is2 & (k >= SEND_SLOTS))
            def _():
                s_copy_inner(k - SEND_SLOTS).wait_send()

            @pl.when(is0 | is3)
            def _():
                sb[k % SEND_SLOTS] = both.astype(BF16)

            @pl.when(is2)
            def _():
                s_copy_edge(k).wait_recv()
                sb[k % SEND_SLOTS] = (both + ra[k % SLOTS].astype(F32)).astype(BF16)

            @pl.when(is1)
            def _():
                s_copy_edge(k).wait_recv()
                s_copy_inner(k).wait_recv()
                tot[k % SLOTS] = (both + ra[k % SLOTS].astype(F32) + rb[k % SLOTS].astype(F32)).astype(BF16)

    def arrive(k):
        @pl.when(inside(k) & (z != 1))
        def _():
            tot_down(k).wait_recv()

    def send(k_sum, k_tot):
        @pl.when(inside(k_sum) & (is0 | is3))
        def _():
            s_copy_edge(k_sum).start()

        @pl.when(inside(k_sum) & is2)
        def _():
            s_copy_inner(k_sum).start()

        @pl.when(inside(k_tot))
        def _():
            @pl.when(is1)
            def _():
                tot_down(k_tot).start()

            @pl.when(is1 | is2)
            def _():
                tot_up(k_tot).start()

            for c in out_copies(k_tot):
                c.start()

    def fine_edge(j):
        return remote(fsb.at[j], fra.at[j], fs_sem.at[j], fra_sem.at[j], me + 2 - 4 * (z // 3))

    def fine_inner(j):
        return remote(fsb.at[j], frb.at[j], fs_sem.at[j], frb_sem.at[j], me - 2)

    def fine_down(j):
        return remote(ftot.at[j], ftot.at[j], fdown_sem.at[j], ftot_sem.at[j], me - 2)

    def fine_up(j):
        return remote(ftot.at[j], ftot.at[j], fup_sem.at[j], ftot_sem.at[j], me + 2)

    def fine_out(j):
        fr = r // PIECES
        k = coarse + j // PIECES
        block, half, which = summed_piece(k // UNITS)
        row = half * fs + core * part + (k % UNITS) * r + (j % PIECES) * fr
        q, at = 3 * block + which, pl.ds(pl.multiple_of(row, fr), fr)
        return (
            pltpu.make_async_copy(ftot.at[j], g_hbm.at[q, at, :], fkeep_sem.at[j]),
            remote(ftot.at[j], g_hbm.at[q, at, :], fpass_sem.at[j], partner_sem, partner),
        )

    def fine_send(j):
        @pl.when(is1)
        def _():
            fine_up(j).start()
            fine_down(j).start()

        @pl.when(is2)
        def _():
            fine_up(j).start()

        for c in fine_out(j):
            c.start()

    def fine_add(k):
        @pl.when((k >= coarse) & (k < units))
        def _():
            for c in load_copies(k):
                c.wait()
            fr, slot = r // PIECES, k % LOAD_SLOTS

            def body(i, _):
                j = (k - coarse) * PIECES + i
                at = pl.ds(pl.multiple_of(i * fr, fr), fr)
                both = mb[slot, at, :].astype(F32) + xb[slot, at, :].astype(F32)

                @pl.when(is0 | is3)
                def _():
                    fsb[j] = both.astype(BF16)
                    fine_edge(j).start()

                @pl.when(is2)
                def _():
                    fine_edge(j).wait_recv()
                    fsb[j] = (both + fra[j].astype(F32)).astype(BF16)
                    fine_inner(j).start()

                @pl.when(is1)
                def _():
                    fine_edge(j).wait_recv()
                    fine_inner(j).wait_recv()
                    ftot[j] = (both + fra[j].astype(F32) + frb[j].astype(F32)).astype(BF16)
                    fine_send(j)

                return 0

            lax.fori_loop(0, PIECES, body, 0)

    def fine_arrive(k):
        @pl.when((k >= coarse) & (k < units) & (z != 1))
        def _():
            def body(i, _):
                j = (k - coarse) * PIECES + i
                fine_down(j).wait_recv()
                fine_send(j)
                return 0

            lax.fori_loop(0, PIECES, body, 0)

    def fine_end():
        def body(j, _):
            keep, give = fine_out(j)
            keep.wait()
            give.wait_send()

            @pl.when(is0 | is3)
            def _():
                fine_edge(j).wait_send()

            @pl.when(is2)
            def _():
                fine_inner(j).wait_send()

            @pl.when(is1)
            def _():
                fine_down(j).wait_send()

            @pl.when(is1 | is2)
            def _():
                fine_up(j).wait_send()

            return 0

        lax.fori_loop(0, FINE * PIECES, body, 0)

    def load(k):
        @pl.when((k >= 0) & (k < units))
        def _():
            @pl.when(k % UNITS == 0)
            def _():
                give_copy(0, k // UNITS).wait_recv()

            for c in load_copies(k):
                c.start()


    def stage_of(s, go):
        @pl.when((s >= 0) & (s < STEPS))
        def _():
            block, half, kind = step_of(s)

            def body(which, _):
                stage_copies(block, half, which, go)
                return 0

            lax.fori_loop(*made_in(kind), body, 0)

    def tick(i, _):
        stage_of(i - 2, False)
        stage_of(i - 1, True)
        now = i - FIRST
        free(now - free_lag)
        add(now - sum_lag)
        arrive(now - tot_lag)
        send(now - sum_lag, now - tot_lag)
        fine_add(now - sum_lag)
        fine_arrive(now - tot_lag)
        load(now - sum_lag + 1)

        @pl.when(i < STEPS)
        def _():
            block, half, kind = step_of(i)

            @pl.when(kind < 2)
            def _():
                hidden(block, half, kind)

            @pl.when((kind >= 2) & (kind <= 5))
            def _():
                gradients(half, kind)

            @pl.when((kind == 6) | (kind == 7))
            def _():
                to_input(block, kind - 6)

            @pl.when(kind >= 8)
            def _():
                turn(kind - 8)

        return 0

    lax.fori_loop(0, max(FIRST + units + 12, STEPS + 2), tick, 0)

    for k in range(coarse - SEND_SLOTS, coarse):

        @pl.when(is0 | is3)
        def _(k=k):
            s_copy_edge(k).wait_send()

        @pl.when(is2)
        def _(k=k):
            s_copy_inner(k).wait_send()

    fine_end()
    pltpu.make_async_copy(theirs_hbm, theirs_hbm, partner_sem).wait()


def backward(a1, a0, h1, dy, wg, wu, wd):
    t, d = a1.shape
    ff = wg.shape[2]
    f = ff // BLOCKS
    fs = f // 2
    r = fs // 2 // UNITS
    sub = t // TILES
    anywhere = pl.BlockSpec(memory_space=pl.ANY)
    dma = pltpu.SemaphoreType.DMA
    return pl.pallas_call(
        backward_kernel,
        out_shape=[
            jax.ShapeDtypeStruct((SUMMED, f, d), BF16),
            jax.ShapeDtypeStruct((ALL - SUMMED, f, d), BF16),
            jax.ShapeDtypeStruct((2 * SUMMED, fs // 2, d), BF16),
            jax.ShapeDtypeStruct((2 * SUMMED, fs // 2, d), BF16),
        ],
        in_specs=[anywhere] * 7,
        out_specs=[anywhere] * 4,
        scratch_shapes=[
            pltpu.VMEM((2, t, d), BF16),
            pltpu.VMEM((3, f, t), BF16),
            pltpu.VMEM((2, d, f), BF16),
            pltpu.VMEM((2, d, f), BF16),
            pltpu.VMEM((2, f, d), BF16),
            pltpu.VMEM((f, d), BF16),
            pltpu.VMEM((f, d), BF16),
            pltpu.VMEM((TILES, d, sub), F32),
            pltpu.VMEM((3, fs, d), BF16),
            pltpu.VMEM((LOAD_SLOTS, r, d), BF16),
            pltpu.VMEM((LOAD_SLOTS, r, d), BF16),
            pltpu.VMEM((SEND_SLOTS, r, d), BF16),
            pltpu.VMEM((SLOTS, r, d), BF16),
            pltpu.VMEM((SLOTS, r, d), BF16),
            pltpu.VMEM((SLOTS, r, d), BF16),
            *[pltpu.VMEM((FINE * PIECES, r // PIECES, d), BF16)] * 4,
            dma((4, 2)),
            dma((2, 3)),
            dma((3,)),
            dma((3,)),
            dma((2 * SUMMED,)),
            dma((3,)),
            dma((LOAD_SLOTS, 2)),
            dma((SEND_SLOTS,)),
            dma((SLOTS,)),
            dma((SLOTS,)),
            dma((SLOTS,)),
            dma((SLOTS,)),
            dma((SLOTS,)),
            dma((SLOTS,)),
            dma((SLOTS,)),
            dma,
            *[dma((FINE * PIECES,))] * 8,
        ],
        compiler_params=pltpu.CompilerParams(collective_id=0, has_side_effects=True, vmem_limit_bytes=VMEM_LIMIT),
        cost_estimate=pl.CostEstimate(flops=2 * 15 * t * d * ff, bytes_accessed=100 * d * ff, transcendentals=2 * t * ff),
        name="backward",
    )(a1, a0, h1, dy, wg, wu, wd)


HALVES = ((1, 0), (1, 1), (2, 0), (2, 1), (0, 0), (0, 1))


def adamw_kernel(rounds, first, n_old, *refs):
    arrays = {1: refs[0:3], 2: refs[3:6], 0: refs[6:9]}
    g_hbm = refs[9]
    outs = refs[10 + n_old :][:9]
    outs = {1: outs[0:3], 2: outs[3:6], 0: outs[6:9]}
    wt, mt, vt, gt, wd, md, vd, gd, wt_out, mt_out, vt_out, wd_out, md_out, vd_out, turned, in_sem, out_sem = refs[10 + n_old + 9 :]
    d, f = wt.shape[1] * 2, wt.shape[2]

    def place(b, half):
        which, s = HALVES[half]
        layer, j, q = 1 - b // BLOCKS, b % BLOCKS, 3 * b + which - first
        if which:
            cols = pl.ds(pl.multiple_of(j * f, f), f)
            return which, lambda ref: ref.at[layer, pl.ds(s * (d // 2), d // 2), cols], g_hbm.at[q, :, pl.ds(s * (d // 2), d // 2)]
        rows = pl.ds(pl.multiple_of(j * f + s * (f // 2), f // 2), f // 2)
        return which, lambda ref: ref.at[layer, rows, :], g_hbm.at[q, pl.ds(s * (f // 2), f // 2), :]

    def buffers(half):
        if HALVES[half][0]:
            return [x.at[half] for x in (wt, mt, vt, gt)], [x.at[half] for x in (wt_out, mt_out, vt_out)]
        return [x.at[half - 4] for x in (wd, md, vd, gd)], [x.at[half - 4] for x in (wd_out, md_out, vd_out)]

    def loads(b, half):
        which, at, g = place(b, half)
        sources = [at(x) for x in arrays[which]] + [g]
        return [pltpu.make_async_copy(x, y, in_sem.at[half, i]) for i, (x, y) in enumerate(zip(sources, buffers(half)[0], strict=True))]

    def stores(b, half):
        which, at, _ = place(b, half)
        return [pltpu.make_async_copy(x, at(y), out_sem.at[half, i]) for i, (x, y) in enumerate(zip(buffers(half)[1], outs[which], strict=True))]

    def take(half):
        (w_in, m_in, v_in, g_in), (w_out, m_out, v_out) = buffers(half)
        if HALVES[half][0]:
            turned[...] = g_in[...].T
            g_in = turned

        def body(i, _):
            at = pl.ds(pl.multiple_of(i * 16, 16), 16)
            g = g_in[at, :].astype(F32)
            m = 0.9 * m_in[at, :] + 0.1 * g
            v = 0.95 * v_in[at, :] + 0.05 * g * g
            w = w_in[at, :].astype(F32)
            w_out[at, :] = (w - 0.02 * (m * lax.rsqrt(v + 1e-8) + 0.1 * w)).astype(BF16)
            m_out[at, :] = m
            v_out[at, :] = v
            return 0

        lax.fori_loop(0, w_in.shape[0] // 16, body, 0, unroll=2)

    def start(copies):
        for c in copies:
            c.start()

    def wait(copies):
        for c in copies:
            c.wait()

    starts = {}
    for blocks, halves in rounds:
        for half in halves:
            if half not in starts:
                starts[half] = True
                start(loads(blocks[0], half))
    before = {}
    for n, (blocks, halves) in enumerate(rounds):
        low, high = blocks

        def next_of(half, n=n):
            return next((bs[0] for bs, hs in rounds[n + 1 :] if half in hs), None)

        def one(b, half, low=low, high=high, next_of=next_of):
            wait(loads(b, half))
            if half in before:
                wait(stores(before[half], half))
            elif high - low > 1:

                @pl.when(b > low)
                def _():
                    wait(stores(b - 1, half))

            take(half)
            start(stores(b, half))
            if high - low > 1:

                @pl.when(b + 1 < high)
                def _():
                    start(loads(b + 1, half))

            after = next_of(half)
            if after is not None:
                if high - low > 1:

                    @pl.when(b + 1 == high)
                    def _():
                        start(loads(after, half))

                else:
                    start(loads(after, half))

        def turn(b, _, halves=halves):
            for half in halves:
                one(b, half)
            return 0

        if high - low > 1:
            lax.fori_loop(low, high, turn, 0)
        else:
            turn(low, 0)
        for half in halves:
            before[half] = high - 1
    for half, b in before.items():
        wait(stores(b, half))


def adamw(pieces, first, g, w, m, v, old=()):
    low, high = pieces
    d, ff = w[0].shape[1:]
    f = ff // BLOCKS
    rounds = []
    for b in range(2 * BLOCKS):
        halves = tuple(h for h, (which, _) in enumerate(HALVES) if low <= 3 * b + which < high)
        if not halves:
            continue
        if len(rounds) == 1 and rounds[0][1] == halves:
            rounds[-1] = ((rounds[-1][0][0], b + 1), halves)
        else:
            rounds.append(((b, b + 1), halves))
    anywhere = pl.BlockSpec(memory_space=pl.ANY)
    operands = [x for i in range(3) for x in (w[i], m[i], v[i])]
    n = (high - low) * d * f
    return pl.pallas_call(
        functools.partial(adamw_kernel, tuple(rounds), first, len(old)),
        out_shape=[jax.ShapeDtypeStruct(x.shape, x.dtype) for x in operands],
        in_specs=[anywhere] * (10 + len(old)),
        out_specs=[anywhere] * 9,
        scratch_shapes=[
            pltpu.VMEM((4, d // 2, f), BF16),
            pltpu.VMEM((4, d // 2, f), F32),
            pltpu.VMEM((4, d // 2, f), F32),
            pltpu.VMEM((4, f, d // 2), BF16),
            pltpu.VMEM((2, f // 2, d), BF16),
            pltpu.VMEM((2, f // 2, d), F32),
            pltpu.VMEM((2, f // 2, d), F32),
            pltpu.VMEM((2, f // 2, d), BF16),
            pltpu.VMEM((4, d // 2, f), BF16),
            pltpu.VMEM((4, d // 2, f), F32),
            pltpu.VMEM((4, d // 2, f), F32),
            pltpu.VMEM((2, f // 2, d), BF16),
            pltpu.VMEM((2, f // 2, d), F32),
            pltpu.VMEM((2, f // 2, d), F32),
            pltpu.VMEM((d // 2, f), BF16),
            pltpu.SemaphoreType.DMA((6, 4)),
            pltpu.SemaphoreType.DMA((6, 3)),
        ],
        input_output_aliases={10 + i: i for i in range(len(old))},
        compiler_params=pltpu.CompilerParams(vmem_limit_bytes=VMEM_LIMIT),
        cost_estimate=pl.CostEstimate(flops=2000 * n, bytes_accessed=22 * n, transcendentals=n),
        name="adamw",
    )(*operands, g, *old)


def solution(mesh):
    def step(x, dy, *arrays):
        w, m, v = (arrays[i : i + 3] for i in (0, 3, 6))
        wg, wu, wd = w
        a0, h1, a1 = forward(x[0], wg, wu, wd)
        g, left, _, _ = backward(a1, a0, h1, dy[0], wg, wu, wd)
        left = lax.psum(left, "dp")
        done = adamw((0, SUMMED), 0, g, w, m, v)
        done = adamw((SUMMED, ALL), SUMMED, left, w, m, v, done)
        return tuple(done[3 * i + kind] for kind in range(3) for i in range(3))

    return jax.shard_map(
        step,
        mesh=mesh,
        in_specs=(P(("rep", "dp"), None, None),) * 2 + (P(None, None, None),) * 9,
        out_specs=(P("rep", None, None),) * 9,
        check_vma=False,
    )
```

```python
import functools

import jax
import jax.numpy as jnp
from jax import lax
from jax.experimental import pallas as pl
from jax.experimental.pallas import tpu as pltpu
from jax.sharding import PartitionSpec as P

BF16, F32 = jnp.bfloat16, jnp.float32
MESH = pl.DeviceIdType.MESH
VMEM_LIMIT = 66_000_000
BLOCKS = 5
ALL = 6 * BLOCKS
SUMMED = 26
UNITS = 2
FINE, PIECES = 2, 5
FIRST = 5
SLOTS, SEND_SLOTS, LOAD_SLOTS = 12, 6, 4
NN = (((1,), (0,)), ((), ()))
NT = (((1,), (1,)), ((), ()))


def dot(a, b, dims=NN):
    return lax.dot_general(a, b, dims, preferred_element_type=F32)


def scale_of(wide):
    return lax.rsqrt(jnp.mean(wide * wide, -1, keepdims=True) + 1e-6)


def groups_of(ff):
    width = min(ff, 512)
    starts = list(range(0, ff - width + 1, width))
    pieces = [(s, (starts[i + 1] if i + 1 < len(starts) else ff) - s) for i, s in enumerate(starts)]
    return [g for g in (pieces[:1], pieces[1:3], pieces[3:]) if g]


def forward_kernel(groups, x_ref, wg_hbm, wu_hbm, wd_hbm, a0_ref, h1_ref, a1_ref, wg, wu, wd, p, sems):
    first = pl.program_id(0) == 0

    def loads(i):
        at = pl.ds(groups[i][0][0], sum(n for _, n in groups[i]))
        return (
            pltpu.make_async_copy(wg_hbm.at[0, :, at], wg.at[:, at], sems.at[0, i]),
            pltpu.make_async_copy(wu_hbm.at[0, :, at], wu.at[:, at], sems.at[1, i]),
            pltpu.make_async_copy(wd_hbm.at[0, at, :], wd.at[at, :], sems.at[2, i]),
        )

    everything = range(len(groups))

    @pl.when(first)
    def _():
        for c in loads(0)[:2]:
            c.start()

    wide = x_ref[...].astype(F32)
    a = (wide * scale_of(wide)).astype(BF16)
    a0_ref[...] = a
    for i in everything:

        @pl.when(first)
        def _(i=i):
            for c in loads(i)[:2]:
                c.wait()
            if i + 1 < len(groups):
                for c in loads(i + 1)[:2]:
                    c.start()
            if i + 2 >= len(groups):
                for j in everything:
                    if i + 2 == len(groups) or len(groups) == 1:
                        loads(j)[2].start()
                    if i + 1 == len(groups):
                        loads(j)[2].wait()

        for s, n in groups[i]:
            gate = dot(a, wg[:, s : s + n])
            up = dot(a, wu[:, s : s + n])
            p[:, s : s + n] = (gate * (0.5 * jnp.tanh(0.5 * gate) + 0.5) * up).astype(BF16)

    h1 = (x_ref[...].astype(F32) + dot(p[...], wd[...]).astype(BF16).astype(F32)).astype(BF16)
    h1_ref[...] = h1
    wide1 = h1.astype(F32)
    a1_ref[...] = (wide1 * scale_of(wide1)).astype(BF16)


def forward(x, wg, wu, wd):
    t, d = x.shape
    ff = wg.shape[2]
    tile = min(t, 1024)
    groups = groups_of(ff)
    rows = pl.BlockSpec((tile, d), lambda i: (i, 0))
    anywhere = pl.BlockSpec(memory_space=pl.ANY)
    return pl.pallas_call(
        functools.partial(forward_kernel, groups),
        grid=(t // tile,),
        out_shape=[jax.ShapeDtypeStruct((t, d), BF16)] * 3,
        in_specs=[rows, anywhere, anywhere, anywhere],
        out_specs=[rows] * 3,
        scratch_shapes=[
            pltpu.VMEM((d, ff), BF16),
            pltpu.VMEM((d, ff), BF16),
            pltpu.VMEM((ff, d), BF16),
            pltpu.VMEM((tile, ff), BF16),
            pltpu.SemaphoreType.DMA((3, len(groups))),
        ],
        compiler_params=pltpu.CompilerParams(vmem_limit_bytes=VMEM_LIMIT, dimension_semantics=("arbitrary",)),
        cost_estimate=pl.CostEstimate(flops=6 * t * d * ff, bytes_accessed=6 * d * ff + 8 * t * d, transcendentals=t * ff),
        name="forward",
    )(x, wg, wu, wd)


HALF_STEPS, DA_STEPS, TILES = 4, 2, 4
BLOCK_STEPS, LOW_STEPS = 2 * HALF_STEPS + DA_STEPS, 2 * HALF_STEPS
TURN = BLOCKS * BLOCK_STEPS
STEPS = 1 + TURN + DA_STEPS + BLOCKS * LOW_STEPS


def step_of(s):
    p = jnp.where(s <= 3, s, s - 1)
    low = p - (TURN + DA_STEPS)
    block = jnp.where(p < TURN, p // BLOCK_STEPS, jnp.where(low < 0, BLOCKS, BLOCKS + low // LOW_STEPS))
    place = jnp.where(p < TURN, p % BLOCK_STEPS, jnp.where(low < 0, BLOCK_STEPS + p - TURN, low % LOW_STEPS))
    half = jnp.where(place < LOW_STEPS, place // HALF_STEPS, 0)
    kind = jnp.where(place < LOW_STEPS, place % HALF_STEPS, place - 2)
    return block, half, jnp.where(s == 3, 4, jnp.where(s == 4, 5, kind))


def made_in(kind):
    low = jnp.where((kind == 3) | (kind == 4), 1, jnp.where(kind == 5, 2, 0))
    high = jnp.where((kind == 3) | (kind == 5), 3, jnp.where(kind == 4, 2, jnp.where(kind == 2, 1, 0)))
    return low, high


def summed_piece(c):
    full, rest = SUMMED // 3, max(SUMMED % 3, 1)
    late = c - 6 * full
    return tuple(
        jnp.where(late < 0, early, other) for early, other in ((c // 6, full), (c % 6 // 3, late // rest), (c % 3, late % rest))
    )


def place_of(block, half, which):
    full, rest = SUMMED // 3, SUMMED % 3
    return jnp.where(block < full, 6 * block + 3 * half + which, 6 * full + rest * half + which)


def backward_kernel(
    a1_hbm, a0_hbm, h1_hbm, dy_hbm, wg_hbm, wu_hbm, wd_hbm,
    g_hbm, left_hbm, mine_hbm, theirs_hbm,
    ad, pgu, wgb, wub, wdb, wgt, wut, dat, stage, mb, xb, sb, ra, rb, tot, fsb, fra, frb, ftot,
    in_sem, w_sem, own_sem, give_sem, get_sem, left_sem, load_sem, s_sem, ra_sem, rb_sem, tot_sem, down_sem, up_sem, keep_sem, pass_sem, partner_sem,
    fs_sem, fra_sem, frb_sem, ftot_sem, fdown_sem, fup_sem, fkeep_sem, fpass_sem,
):
    me = lax.axis_index("dp")
    z, core = me // 2, me % 2
    partner = me + 1 - 2 * core
    t, d = ad.shape[1:]
    f, fs = wgt.shape[0], stage.shape[1]
    part, r = fs // 2, fs // 2 // UNITS
    units = 2 * SUMMED * UNITS
    coarse = units - FINE
    sub = dat.shape[2]

    def remote(src, dst, send, recv, device):
        return pltpu.make_async_remote_copy(src_ref=src, dst_ref=dst, send_sem=send, recv_sem=recv, device_id={"dp": device}, device_id_type=MESH)

    def weights(block):
        layer, j, slot = 1 - block // BLOCKS, block % BLOCKS, block % 2
        at = pl.ds(pl.multiple_of(j * f, f), f)
        return (
            pltpu.make_async_copy(wg_hbm.at[layer, :, at], wgb.at[slot], w_sem.at[slot, 0]),
            pltpu.make_async_copy(wu_hbm.at[layer, :, at], wub.at[slot], w_sem.at[slot, 1]),
            pltpu.make_async_copy(wd_hbm.at[layer, at, :], wdb.at[slot], w_sem.at[slot, 2]),
        )

    def load_tokens(which):
        at = pl.ds(which * (t // 2), t // 2)
        return (
            pltpu.make_async_copy(a1_hbm.at[at, :], ad.at[1, at, :], in_sem.at[0, which]),
            pltpu.make_async_copy(dy_hbm.at[at, :], ad.at[0, at, :], in_sem.at[1, which]),
        )

    load_h1 = pltpu.make_async_copy(h1_hbm, ad.at[1], in_sem.at[2, 0])
    load_a0 = pltpu.make_async_copy(a0_hbm, ad.at[1], in_sem.at[3, 0])

    for a, b in zip(weights(0), (*load_tokens(0), None)):
        a.start()
        if b is not None:
            b.start()
    dat[...] = jnp.zeros_like(dat)

    barrier = pltpu.get_barrier_semaphore()
    pl.semaphore_signal(barrier, inc=1, device_id={"dp": partner}, device_id_type=MESH)

    @pl.when(z > 0)
    def _():
        pl.semaphore_signal(barrier, inc=1, device_id={"dp": me - 2}, device_id_type=MESH)

    @pl.when(z < 3)
    def _():
        pl.semaphore_signal(barrier, inc=1, device_id={"dp": me + 2}, device_id_type=MESH)

    pl.semaphore_wait(barrier, 3 - z // 3 - (3 - z) // 3)

    def at_half(half):
        return pl.ds(pl.multiple_of(half * fs, fs), fs)

    def hidden(block, half, tokens):
        slot = block % 2

        for which in range(2):

            @pl.when((block == 0) & (half == 0) & (tokens == which))
            def _(which=which):
                for c in load_tokens(which):
                    c.wait()

        @pl.when((half == 0) & (tokens == 0))
        def _():
            @pl.when(block == BLOCKS)
            def _():
                load_a0.wait()

            for c in weights(block):
                c.wait()

            @pl.when(block == 0)
            def _():
                for c in load_tokens(1):
                    c.start()

            @pl.when(block + 1 < 2 * BLOCKS)
            def _():
                for c in weights(block + 1):
                    c.start()

        cut = -(-fs // 128) * 128
        for which, at in ((0, slice(0, cut)), (1, slice(cut, f))):

            @pl.when((half == which) & (tokens == 0))
            def _(at=at):
                wgt[at, :] = wgb[slot, :, at].T
                wut[at, :] = wub[slot, :, at].T

        units_at = at_half(half)
        for i in range(TILES // 2):
            at = pl.ds(pl.multiple_of((tokens * (TILES // 2) + i) * sub, sub), sub)
            gate = dot(wgt[units_at, :], ad[1, at, :], NT)
            up = dot(wut[units_at, :], ad[1, at, :], NT)
            dp = dot(wdb[slot, units_at, :], ad[0, at, :], NT).astype(BF16).astype(F32)
            sig = 0.5 * jnp.tanh(0.5 * gate) + 0.5
            silu = gate * sig
            pgu[0, units_at, at] = (silu * up).astype(BF16)
            pgu[1, units_at, at] = (dp * up * (sig + silu * (1.0 - sig))).astype(BF16)
            pgu[2, units_at, at] = (dp * silu).astype(BF16)

    def gradients(half, kind):
        def body(which, _):
            stage[which] = dot(pgu[which, at_half(half), :], ad[jnp.minimum(which, 1)]).astype(BF16)
            return 0

        lax.fori_loop(*made_in(kind), body, 0)

    def to_input(block, step):
        slot = block % 2

        @pl.when((block == BLOCKS - 1) & (step == 0))
        def _():
            load_h1.start()

        for i in range(TILES // DA_STEPS):
            tile = step * (TILES // DA_STEPS) + i
            at = pl.ds(pl.multiple_of(tile * sub, sub), sub)
            dat[tile] += dot(wgb[slot], pgu[1, :, at]) + dot(wub[slot], pgu[2, :, at])

    def turn(step):
        @pl.when(step == 0)
        def _():
            load_h1.wait()

        def body(i, _):
            tile = step * (TILES // DA_STEPS) + i
            at = pl.ds(pl.multiple_of(tile * sub, sub), sub)
            da = dat[tile].T.astype(BF16).astype(F32)
            wide = ad[1, at, :].astype(F32)
            scale = scale_of(wide)
            inner = jnp.sum(da * wide, -1, keepdims=True) * (scale * scale * scale) * (1.0 / d)
            through = (da * scale - wide * inner).astype(BF16).astype(F32)
            ad[0, at, :] = (ad[0, at, :].astype(F32) + through).astype(BF16)
            return 0

        lax.fori_loop(0, TILES // DA_STEPS, body, 0)

        @pl.when(step == DA_STEPS - 1)
        def _():
            load_a0.start()

    def rows(slot, c):
        return stage.at[slot, pl.ds(pl.multiple_of(c * part, part), part), :]

    def give_copy(slot, c):
        return remote(rows(slot, 1 - core), theirs_hbm.at[c], give_sem.at[slot], get_sem.at[c], partner)

    def own_copy(slot, c):
        return pltpu.make_async_copy(rows(slot, core), mine_hbm.at[c], own_sem.at[slot])

    def left_copy(slot, block, half, which):
        return pltpu.make_async_copy(stage.at[slot], left_hbm.at[3 * block + which - SUMMED, at_half(half), :], left_sem.at[slot])

    def stage_copies(block, half, which, go):
        slot, here = which, 3 * block + which < SUMMED

        @pl.when(here)
        def _():
            c = place_of(block, half, which)
            if go:
                own_copy(slot, c).start()
                give_copy(slot, c).start()
            else:
                own_copy(slot, c).wait()
                give_copy(slot, c).wait_send()

        @pl.when(jnp.logical_not(here))
        def _():
            copy = left_copy(slot, block, half, which)
            if go:
                copy.start()
            else:
                copy.wait()

    is0, is1, is2, is3 = z == 0, z == 1, z == 2, z == 3
    sum_lag = jnp.where(is1, 2, jnp.where(is2, 1, 0))
    tot_lag = jnp.where(is1, 2, jnp.where(is3, 9, jnp.where(is2, 5, 6)))
    free_lag = tot_lag + jnp.where(is3, 2, 3)

    def load_copies(k):
        q, at, slot = k // UNITS, pl.ds(pl.multiple_of((k % UNITS) * r, r), r), k % LOAD_SLOTS
        return (
            pltpu.make_async_copy(mine_hbm.at[q, at, :], mb.at[slot], load_sem.at[slot, 0]),
            pltpu.make_async_copy(theirs_hbm.at[q, at, :], xb.at[slot], load_sem.at[slot, 1]),
        )

    def s_copy_edge(k):
        return remote(sb.at[k % SEND_SLOTS], ra.at[k % SLOTS], s_sem.at[k % SEND_SLOTS], ra_sem.at[k % SLOTS], me + 2 - 4 * (z // 3))

    def s_copy_inner(k):
        return remote(sb.at[k % SEND_SLOTS], rb.at[k % SLOTS], s_sem.at[k % SEND_SLOTS], rb_sem.at[k % SLOTS], me - 2)

    def tot_down(k):
        return remote(tot.at[k % SLOTS], tot.at[k % SLOTS], down_sem.at[k % SLOTS], tot_sem.at[k % SLOTS], me - 2)

    def tot_up(k):
        return remote(tot.at[k % SLOTS], tot.at[k % SLOTS], up_sem.at[k % SLOTS], tot_sem.at[k % SLOTS], me + 2)

    def out_copies(k):
        block, half, which = summed_piece(k // UNITS)
        q, at, slot = 3 * block + which, pl.ds(pl.multiple_of(half * fs + core * part + (k % UNITS) * r, r), r), k % SLOTS
        return (
            pltpu.make_async_copy(tot.at[slot], g_hbm.at[q, at, :], keep_sem.at[slot]),
            remote(tot.at[slot], g_hbm.at[q, at, :], pass_sem.at[slot], partner_sem, partner),
        )

    def inside(k):
        return (k >= 0) & (k < coarse)

    def free(k):
        @pl.when(inside(k))
        def _():
            keep, give = out_copies(k)
            keep.wait()
            give.wait_send()

            @pl.when(is1)
            def _():
                tot_down(k).wait_send()

            @pl.when(is1 | is2)
            def _():
                tot_up(k).wait_send()

    def add(k):
        @pl.when(inside(k))
        def _():
            for c in load_copies(k):
                c.wait()
            slot = k % LOAD_SLOTS
            both = mb[slot].astype(F32) + xb[slot].astype(F32)

            @pl.when((is0 | is3) & (k >= SEND_SLOTS))
            def _():
                s_copy_edge(k - SEND_SLOTS).wait_send()

            @pl.when(is2 & (k >= SEND_SLOTS))
            def _():
                s_copy_inner(k - SEND_SLOTS).wait_send()

            @pl.when(is0 | is3)
            def _():
                sb[k % SEND_SLOTS] = both.astype(BF16)

            @pl.when(is2)
            def _():
                s_copy_edge(k).wait_recv()
                sb[k % SEND_SLOTS] = (both + ra[k % SLOTS].astype(F32)).astype(BF16)

            @pl.when(is1)
            def _():
                s_copy_edge(k).wait_recv()
                s_copy_inner(k).wait_recv()
                tot[k % SLOTS] = (both + ra[k % SLOTS].astype(F32) + rb[k % SLOTS].astype(F32)).astype(BF16)

    def arrive(k):
        @pl.when(inside(k) & (z != 1))
        def _():
            tot_down(k).wait_recv()

    def send(k_sum, k_tot):
        @pl.when(inside(k_sum) & (is0 | is3))
        def _():
            s_copy_edge(k_sum).start()

        @pl.when(inside(k_sum) & is2)
        def _():
            s_copy_inner(k_sum).start()

        @pl.when(inside(k_tot))
        def _():
            @pl.when(is1)
            def _():
                tot_down(k_tot).start()

            @pl.when(is1 | is2)
            def _():
                tot_up(k_tot).start()

            for c in out_copies(k_tot):
                c.start()

    def fine_edge(j):
        return remote(fsb.at[j], fra.at[j], fs_sem.at[j], fra_sem.at[j], me + 2 - 4 * (z // 3))

    def fine_inner(j):
        return remote(fsb.at[j], frb.at[j], fs_sem.at[j], frb_sem.at[j], me - 2)

    def fine_down(j):
        return remote(ftot.at[j], ftot.at[j], fdown_sem.at[j], ftot_sem.at[j], me - 2)

    def fine_up(j):
        return remote(ftot.at[j], ftot.at[j], fup_sem.at[j], ftot_sem.at[j], me + 2)

    def fine_out(j):
        fr = r // PIECES
        k = coarse + j // PIECES
        block, half, which = summed_piece(k // UNITS)
        row = half * fs + core * part + (k % UNITS) * r + (j % PIECES) * fr
        q, at = 3 * block + which, pl.ds(pl.multiple_of(row, fr), fr)
        return (
            pltpu.make_async_copy(ftot.at[j], g_hbm.at[q, at, :], fkeep_sem.at[j]),
            remote(ftot.at[j], g_hbm.at[q, at, :], fpass_sem.at[j], partner_sem, partner),
        )

    def fine_send(j):
        @pl.when(is1)
        def _():
            fine_up(j).start()
            fine_down(j).start()

        @pl.when(is2)
        def _():
            fine_up(j).start()

        for c in fine_out(j):
            c.start()

    def fine_add(k):
        @pl.when((k >= coarse) & (k < units))
        def _():
            for c in load_copies(k):
                c.wait()
            fr, slot = r // PIECES, k % LOAD_SLOTS

            def body(i, _):
                j = (k - coarse) * PIECES + i
                at = pl.ds(pl.multiple_of(i * fr, fr), fr)
                both = mb[slot, at, :].astype(F32) + xb[slot, at, :].astype(F32)

                @pl.when(is0 | is3)
                def _():
                    fsb[j] = both.astype(BF16)
                    fine_edge(j).start()

                @pl.when(is2)
                def _():
                    fine_edge(j).wait_recv()
                    fsb[j] = (both + fra[j].astype(F32)).astype(BF16)
                    fine_inner(j).start()

                @pl.when(is1)
                def _():
                    fine_edge(j).wait_recv()
                    fine_inner(j).wait_recv()
                    ftot[j] = (both + fra[j].astype(F32) + frb[j].astype(F32)).astype(BF16)
                    fine_send(j)

                return 0

            lax.fori_loop(0, PIECES, body, 0)

    def fine_arrive(k):
        @pl.when((k >= coarse) & (k < units) & (z != 1))
        def _():
            def body(i, _):
                j = (k - coarse) * PIECES + i
                fine_down(j).wait_recv()
                fine_send(j)
                return 0

            lax.fori_loop(0, PIECES, body, 0)

    def fine_end():
        def body(j, _):
            keep, give = fine_out(j)
            keep.wait()
            give.wait_send()

            @pl.when(is0 | is3)
            def _():
                fine_edge(j).wait_send()

            @pl.when(is2)
            def _():
                fine_inner(j).wait_send()

            @pl.when(is1)
            def _():
                fine_down(j).wait_send()

            @pl.when(is1 | is2)
            def _():
                fine_up(j).wait_send()

            return 0

        lax.fori_loop(0, FINE * PIECES, body, 0)

    def load(k):
        @pl.when((k >= 0) & (k < units))
        def _():
            @pl.when(k % UNITS == 0)
            def _():
                give_copy(0, k // UNITS).wait_recv()

            for c in load_copies(k):
                c.start()


    def stage_of(s, go):
        @pl.when((s >= 0) & (s < STEPS))
        def _():
            block, half, kind = step_of(s)

            def body(which, _):
                stage_copies(block, half, which, go)
                return 0

            lax.fori_loop(*made_in(kind), body, 0)

    def tick(i, _):
        stage_of(i - 2, False)
        stage_of(i - 1, True)
        now = i - FIRST
        free(now - free_lag)
        add(now - sum_lag)
        arrive(now - tot_lag)
        send(now - sum_lag, now - tot_lag)
        fine_add(now - sum_lag)
        fine_arrive(now - tot_lag)
        load(now - sum_lag + 1)

        @pl.when(i < STEPS)
        def _():
            block, half, kind = step_of(i)

            @pl.when(kind < 2)
            def _():
                hidden(block, half, kind)

            @pl.when((kind >= 2) & (kind <= 5))
            def _():
                gradients(half, kind)

            @pl.when((kind == 6) | (kind == 7))
            def _():
                to_input(block, kind - 6)

            @pl.when(kind >= 8)
            def _():
                turn(kind - 8)

        return 0

    lax.fori_loop(0, max(FIRST + units + 12, STEPS + 2), tick, 0)

    for k in range(coarse - SEND_SLOTS, coarse):

        @pl.when(is0 | is3)
        def _(k=k):
            s_copy_edge(k).wait_send()

        @pl.when(is2)
        def _(k=k):
            s_copy_inner(k).wait_send()

    fine_end()
    pltpu.make_async_copy(theirs_hbm, theirs_hbm, partner_sem).wait()


def backward(a1, a0, h1, dy, wg, wu, wd):
    t, d = a1.shape
    ff = wg.shape[2]
    f = ff // BLOCKS
    fs = f // 2
    r = fs // 2 // UNITS
    sub = t // TILES
    anywhere = pl.BlockSpec(memory_space=pl.ANY)
    dma = pltpu.SemaphoreType.DMA
    return pl.pallas_call(
        backward_kernel,
        out_shape=[
            jax.ShapeDtypeStruct((SUMMED, f, d), BF16),
            jax.ShapeDtypeStruct((ALL - SUMMED, f, d), BF16),
            jax.ShapeDtypeStruct((2 * SUMMED, fs // 2, d), BF16),
            jax.ShapeDtypeStruct((2 * SUMMED, fs // 2, d), BF16),
        ],
        in_specs=[anywhere] * 7,
        out_specs=[anywhere] * 4,
        scratch_shapes=[
            pltpu.VMEM((2, t, d), BF16),
            pltpu.VMEM((3, f, t), BF16),
            pltpu.VMEM((2, d, f), BF16),
            pltpu.VMEM((2, d, f), BF16),
            pltpu.VMEM((2, f, d), BF16),
            pltpu.VMEM((f, d), BF16),
            pltpu.VMEM((f, d), BF16),
            pltpu.VMEM((TILES, d, sub), F32),
            pltpu.VMEM((3, fs, d), BF16),
            pltpu.VMEM((LOAD_SLOTS, r, d), BF16),
            pltpu.VMEM((LOAD_SLOTS, r, d), BF16),
            pltpu.VMEM((SEND_SLOTS, r, d), BF16),
            pltpu.VMEM((SLOTS, r, d), BF16),
            pltpu.VMEM((SLOTS, r, d), BF16),
            pltpu.VMEM((SLOTS, r, d), BF16),
            *[pltpu.VMEM((FINE * PIECES, r // PIECES, d), BF16)] * 4,
            dma((4, 2)),
            dma((2, 3)),
            dma((3,)),
            dma((3,)),
            dma((2 * SUMMED,)),
            dma((3,)),
            dma((LOAD_SLOTS, 2)),
            dma((SEND_SLOTS,)),
            dma((SLOTS,)),
            dma((SLOTS,)),
            dma((SLOTS,)),
            dma((SLOTS,)),
            dma((SLOTS,)),
            dma((SLOTS,)),
            dma((SLOTS,)),
            dma,
            *[dma((FINE * PIECES,))] * 8,
        ],
        compiler_params=pltpu.CompilerParams(collective_id=0, has_side_effects=True, vmem_limit_bytes=VMEM_LIMIT),
        cost_estimate=pl.CostEstimate(flops=2 * 15 * t * d * ff, bytes_accessed=100 * d * ff, transcendentals=2 * t * ff),
        name="backward",
    )(a1, a0, h1, dy, wg, wu, wd)


HALVES = ((1, 0), (1, 1), (2, 0), (2, 1), (0, 0), (0, 1))


def adamw_kernel(rounds, first, n_old, *refs):
    arrays = {1: refs[0:3], 2: refs[3:6], 0: refs[6:9]}
    g_hbm = refs[9]
    outs = refs[10 + n_old :][:9]
    outs = {1: outs[0:3], 2: outs[3:6], 0: outs[6:9]}
    wt, mt, vt, gt, wd, md, vd, gd, wt_out, mt_out, vt_out, wd_out, md_out, vd_out, turned, in_sem, out_sem = refs[10 + n_old + 9 :]
    d, f = wt.shape[1] * 2, wt.shape[2]

    def place(b, half):
        which, s = HALVES[half]
        layer, j, q = 1 - b // BLOCKS, b % BLOCKS, 3 * b + which - first
        if which:
            cols = pl.ds(pl.multiple_of(j * f, f), f)
            return which, lambda ref: ref.at[layer, pl.ds(s * (d // 2), d // 2), cols], g_hbm.at[q, :, pl.ds(s * (d // 2), d // 2)]
        rows = pl.ds(pl.multiple_of(j * f + s * (f // 2), f // 2), f // 2)
        return which, lambda ref: ref.at[layer, rows, :], g_hbm.at[q, pl.ds(s * (f // 2), f // 2), :]

    def buffers(half):
        if HALVES[half][0]:
            return [x.at[half] for x in (wt, mt, vt, gt)], [x.at[half] for x in (wt_out, mt_out, vt_out)]
        return [x.at[half - 4] for x in (wd, md, vd, gd)], [x.at[half - 4] for x in (wd_out, md_out, vd_out)]

    def loads(b, half):
        which, at, g = place(b, half)
        sources = [at(x) for x in arrays[which]] + [g]
        return [pltpu.make_async_copy(x, y, in_sem.at[half, i]) for i, (x, y) in enumerate(zip(sources, buffers(half)[0], strict=True))]

    def stores(b, half):
        which, at, _ = place(b, half)
        return [pltpu.make_async_copy(x, at(y), out_sem.at[half, i]) for i, (x, y) in enumerate(zip(buffers(half)[1], outs[which], strict=True))]

    def take(half):
        (w_in, m_in, v_in, g_in), (w_out, m_out, v_out) = buffers(half)
        if HALVES[half][0]:
            turned[...] = g_in[...].T
            g_in = turned

        def body(i, _):
            at = pl.ds(pl.multiple_of(i * 16, 16), 16)
            g = g_in[at, :].astype(F32)
            m = 0.9 * m_in[at, :] + 0.1 * g
            v = 0.95 * v_in[at, :] + 0.05 * g * g
            w = w_in[at, :].astype(F32)
            w_out[at, :] = (w - 0.02 * (m * lax.rsqrt(v + 1e-8) + 0.1 * w)).astype(BF16)
            m_out[at, :] = m
            v_out[at, :] = v
            return 0

        lax.fori_loop(0, w_in.shape[0] // 16, body, 0, unroll=2)

    def start(copies):
        for c in copies:
            c.start()

    def wait(copies):
        for c in copies:
            c.wait()

    starts = {}
    for blocks, halves in rounds:
        for half in halves:
            if half not in starts:
                starts[half] = True
                start(loads(blocks[0], half))
    before = {}
    for n, (blocks, halves) in enumerate(rounds):
        low, high = blocks

        def next_of(half, n=n):
            return next((bs[0] for bs, hs in rounds[n + 1 :] if half in hs), None)

        def one(b, half, low=low, high=high, next_of=next_of):
            wait(loads(b, half))
            if half in before:
                wait(stores(before[half], half))
            elif high - low > 1:

                @pl.when(b > low)
                def _():
                    wait(stores(b - 1, half))

            take(half)
            start(stores(b, half))
            if high - low > 1:

                @pl.when(b + 1 < high)
                def _():
                    start(loads(b + 1, half))

            after = next_of(half)
            if after is not None:
                if high - low > 1:

                    @pl.when(b + 1 == high)
                    def _():
                        start(loads(after, half))

                else:
                    start(loads(after, half))

        def turn(b, _, halves=halves):
            for half in halves:
                one(b, half)
            return 0

        if high - low > 1:
            lax.fori_loop(low, high, turn, 0)
        else:
            turn(low, 0)
        for half in halves:
            before[half] = high - 1
    for half, b in before.items():
        wait(stores(b, half))


def adamw(pieces, first, g, w, m, v, old=()):
    low, high = pieces
    d, ff = w[0].shape[1:]
    f = ff // BLOCKS
    rounds = []
    for b in range(2 * BLOCKS):
        halves = tuple(h for h, (which, _) in enumerate(HALVES) if low <= 3 * b + which < high)
        if not halves:
            continue
        if len(rounds) == 1 and rounds[0][1] == halves:
            rounds[-1] = ((rounds[-1][0][0], b + 1), halves)
        else:
            rounds.append(((b, b + 1), halves))
    anywhere = pl.BlockSpec(memory_space=pl.ANY)
    operands = [x for i in range(3) for x in (w[i], m[i], v[i])]
    n = (high - low) * d * f
    return pl.pallas_call(
        functools.partial(adamw_kernel, tuple(rounds), first, len(old)),
        out_shape=[jax.ShapeDtypeStruct(x.shape, x.dtype) for x in operands],
        in_specs=[anywhere] * (10 + len(old)),
        out_specs=[anywhere] * 9,
        scratch_shapes=[
            pltpu.VMEM((4, d // 2, f), BF16),
            pltpu.VMEM((4, d // 2, f), F32),
            pltpu.VMEM((4, d // 2, f), F32),
            pltpu.VMEM((4, f, d // 2), BF16),
            pltpu.VMEM((2, f // 2, d), BF16),
            pltpu.VMEM((2, f // 2, d), F32),
            pltpu.VMEM((2, f // 2, d), F32),
            pltpu.VMEM((2, f // 2, d), BF16),
            pltpu.VMEM((4, d // 2, f), BF16),
            pltpu.VMEM((4, d // 2, f), F32),
            pltpu.VMEM((4, d // 2, f), F32),
            pltpu.VMEM((2, f // 2, d), BF16),
            pltpu.VMEM((2, f // 2, d), F32),
            pltpu.VMEM((2, f // 2, d), F32),
            pltpu.VMEM((d // 2, f), BF16),
            pltpu.SemaphoreType.DMA((6, 4)),
            pltpu.SemaphoreType.DMA((6, 3)),
        ],
        input_output_aliases={10 + i: i for i in range(len(old))},
        compiler_params=pltpu.CompilerParams(vmem_limit_bytes=VMEM_LIMIT),
        cost_estimate=pl.CostEstimate(flops=2000 * n, bytes_accessed=22 * n, transcendentals=n),
        name="adamw",
    )(*operands, g, *old)


def solution(mesh):
    def step(x, dy, *arrays):
        w, m, v = (arrays[i : i + 3] for i in (0, 3, 6))
        wg, wu, wd = w
        a0, h1, a1 = forward(x[0], wg, wu, wd)
        g, left, _, _ = backward(a1, a0, h1, dy[0], wg, wu, wd)
        left = lax.psum(left, "dp")
        done = adamw((0, SUMMED), 0, g, w, m, v)
        done = adamw((SUMMED, ALL), SUMMED, left, w, m, v, done)
        return tuple(done[3 * i + kind] for kind in range(3) for i in range(3))

    return jax.shard_map(
        step,
        mesh=mesh,
        in_specs=(P(("rep", "dp"), None, None),) * 2 + (P(None, None, None),) * 9,
        out_specs=(P("rep", None, None),) * 9,
        check_vma=False,
    )
```
